256 devices in a mesh: rep: 1, dp: 256 (over x, y, z, core).
Axes of the slice: x: 4, y: 4, z: 8, core: 2. Of those that a mesh axis runs over, the one named last changes fastest.
Arguments:
- x: bfloat16 [256, 1024, 768], P(('rep', 'dp'))
- dy: bfloat16 [256, 1024, 768], P(('rep', 'dp'))
- wq: bfloat16 [1, 768, 768], replicated
- wk: bfloat16 [1, 768, 128], replicated
- wv: bfloat16 [1, 768, 128], replicated
- wo: bfloat16 [1, 768, 768], replicated
- w_gate: bfloat16 [1, 768, 2048], replicated
- w_up: bfloat16 [1, 768, 2048], replicated
- w_down: bfloat16 [1, 2048, 768], replicated
- m_wq: float32 [1, 768, 768], P(None, 'dp')
- m_wk: float32 [1, 768, 128], P(None, 'dp')
- m_wv: float32 [1, 768, 128], P(None, 'dp')
- m_wo: float32 [1, 768, 768], P(None, 'dp')
- m_w_gate: float32 [1, 768, 2048], P(None, 'dp')
- m_w_up: float32 [1, 768, 2048], P(None, 'dp')
- m_w_down: float32 [1, 2048, 768], P(None, 'dp')
- v_wq: float32 [1, 768, 768], P(None, 'dp')
- v_wk: float32 [1, 768, 128], P(None, 'dp')
- v_wv: float32 [1, 768, 128], P(None, 'dp')
- v_wo: float32 [1, 768, 768], P(None, 'dp')
- v_w_gate: float32 [1, 768, 2048], P(None, 'dp')
- v_w_up: float32 [1, 768, 2048], P(None, 'dp')
- v_w_down: float32 [1, 2048, 768], P(None, 'dp')
Outputs:
- output 1: bfloat16 [1, 768, 768], P('rep')
- output 2: bfloat16 [1, 768, 128], P('rep')
- output 3: bfloat16 [1, 768, 128], P('rep')
- output 4: bfloat16 [1, 768, 768], P('rep')
- output 5: bfloat16 [1, 768, 2048], P('rep')
- output 6: bfloat16 [1, 768, 2048], P('rep')
- output 7: bfloat16 [1, 2048, 768], P('rep')
- output 8: float32 [1, 768, 768], P('rep', 'dp')
- output 9: float32 [1, 768, 128], P('rep', 'dp')
- output 10: float32 [1, 768, 128], P('rep', 'dp')
- output 11: float32 [1, 768, 768], P('rep', 'dp')
- output 12: float32 [1, 768, 2048], P('rep', 'dp')
- output 13: float32 [1, 768, 2048], P('rep', 'dp')
- output 14: float32 [1, 2048, 768], P('rep', 'dp')
- output 15: float32 [1, 768, 768], P('rep', 'dp')
- output 16: float32 [1, 768, 128], P('rep', 'dp')
- output 17: float32 [1, 768, 128], P('rep', 'dp')
- output 18: float32 [1, 768, 768], P('rep', 'dp')
- output 19: float32 [1, 768, 2048], P('rep', 'dp')
- output 20: float32 [1, 768, 2048], P('rep', 'dp')
- output 21: float32 [1, 2048, 768], P('rep', 'dp')
All inputs are finite; a program needn't handle non-finite values.
Results may differ from the reference program's by a relative error of at most 0.024.
Values are sent between devices in bfloat16 or wider.
A program may use at most 768 MiB of HBM per device.

```python
import jax
import jax.numpy as jnp
from jax import lax

SEQUENCES = 256
TOKENS = 1024
D = 768
HEADS = 6
KV_HEADS = 1
HEAD = 128
FF = 2048
LAYERS = 1
THETA = 10000
NAMES = ("wq", "wk", "wv", "wo", "w_gate", "w_up", "w_down")
SHAPES = {
    "wq": (LAYERS, D, HEADS * HEAD),
    "wk": (LAYERS, D, KV_HEADS * HEAD),
    "wv": (LAYERS, D, KV_HEADS * HEAD),
    "wo": (LAYERS, HEADS * HEAD, D),
    "w_gate": (LAYERS, D, FF),
    "w_up": (LAYERS, D, FF),
    "w_down": (LAYERS, FF, D),
}


def bump(key, n, height):
    away = (jnp.arange(n, dtype=jnp.int32) - jax.random.randint(key, (), 0, n, jnp.int32)) % n
    return jnp.where(away < n // 8, height, 1.0)


def together(key, own, strength):
    shared = jax.random.normal(key, own.shape[1:], jnp.float32)
    return (own + strength * shared) * lax.rsqrt(1 + strength * strength)


def setup_inputs(seed: int = 0, part: int = 0) -> dict:
    kx, kdy, ka, kb, kz, kf, kh, kl, *keys = jax.random.split(jax.random.key(seed), 8 + 3 * len(NAMES))
    kx, kdy, ka, kb = (jax.random.fold_in(k, part) for k in (kx, kdy, ka, kb))
    kw, km, kv = (keys[i::3] for i in range(3))
    shape = (SEQUENCES, TOKENS, D)
    much_x, much_dy = jax.random.uniform(kz, (2,), jnp.float32, 0.0, 1.0)
    loud = 2.0 ** jax.random.uniform(jax.random.fold_in(kz, 1), (), jnp.float32, -1.0, 2.0)
    layers = 2.0 ** jax.random.uniform(kl, (LAYERS, 1, 1), jnp.float32, -1.0, 1.0)
    times = {"wq": 1.0, "wk": 1.0, "wv": 2.0, "wo": layers, "w_gate": 1.0, "w_up": bump(kh, FF, 4.0), "w_down": layers}
    x = together(ka, jax.random.normal(kx, shape, jnp.float32), much_x) * bump(kf, D, 4.0)
    dy = together(kb, jax.random.normal(kdy, shape, jnp.float32), much_dy)
    drawn = {"x": x.astype(jnp.bfloat16), "dy": (loud * dy * (SEQUENCES * TOKENS) ** -0.5).astype(jnp.bfloat16)}
    for key, name in zip(kw, NAMES, strict=True):
        drawn[name] = (jax.random.normal(key, SHAPES[name], jnp.float32) * SHAPES[name][1] ** -0.5 * times[name]).astype(jnp.bfloat16)
    for key, name in zip(km, NAMES, strict=True):
        drawn[f"m_{name}"] = 0.1 * jax.random.normal(key, SHAPES[name], jnp.float32)
    for key, name in zip(kv, NAMES, strict=True):
        drawn[f"v_{name}"] = loud * loud * jax.random.uniform(key, SHAPES[name], jnp.float32, 0.2, 0.6)
    return drawn


def matmul(a, w):
    return jnp.dot(a, w, preferred_element_type=jnp.float32).astype(jnp.bfloat16)


def normed(h):
    wide = h.astype(jnp.float32)
    scale = lax.rsqrt(jnp.mean(wide**2, -1, keepdims=True) + 1e-6)
    return (wide * scale).astype(jnp.bfloat16)


def turned(t, theta):
    half = t.shape[-1] // 2
    angle = jnp.arange(t.shape[0], dtype=jnp.float32)[:, None] * theta ** (-jnp.arange(half, dtype=jnp.float32) / half)
    cos, sin = jnp.cos(angle)[:, None], jnp.sin(angle)[:, None]
    a, b = t[..., :half].astype(jnp.float32), t[..., half:].astype(jnp.float32)
    return jnp.concatenate([a * cos - b * sin, b * cos + a * sin], -1).astype(jnp.bfloat16)


def seen_by(q, k, v):
    tokens, kv = q.shape[0], k.shape[1]
    q = q.reshape(tokens, kv, -1, q.shape[-1])
    scores = jnp.einsum("tgsd,ugd->gstu", q.astype(jnp.float32), k.astype(jnp.float32)) * q.shape[-1] ** -0.5
    place = jnp.arange(tokens)
    weights = jax.nn.softmax(jnp.where(place[:, None] >= place, scores, -jnp.inf), -1).astype(jnp.bfloat16)
    return jnp.einsum("gstu,ugd->tgsd", weights.astype(jnp.float32), v.astype(jnp.float32)).astype(jnp.bfloat16).reshape(tokens, -1)


def layer(h, w):
    a = normed(h)
    q, k = (turned(matmul(a, w[name]).reshape(h.shape[0], -1, HEAD), THETA) for name in ("wq", "wk"))
    h = h + matmul(seen_by(q, k, matmul(a, w["wv"]).reshape(h.shape[0], -1, HEAD)), w["wo"])
    b = normed(h)
    gate = jnp.dot(b, w["w_gate"], preferred_element_type=jnp.float32)
    up = jnp.dot(b, w["w_up"], preferred_element_type=jnp.float32)
    return h + matmul((jax.nn.silu(gate) * up).astype(jnp.bfloat16), w["w_down"])


def adamw(w, m, v, g):
    m = 0.9 * m + 0.1 * g
    v = 0.95 * v + 0.05 * g * g
    step = m * lax.rsqrt(v + 1e-8) + 0.1 * w
    return (w - 0.02 * step).astype(jnp.bfloat16), m, v


def stack(weights, h):
    return lax.scan(lambda h, w: (layer(h, w), None), h, weights)[0]


def reference(x, dy, wq, wk, wv, wo, w_gate, w_up, w_down, m_wq, m_wk, m_wv, m_wo, m_w_gate, m_w_up, m_w_down, v_wq, v_wk, v_wv, v_wo, v_w_gate, v_w_up, v_w_down):
    weights = dict(zip(NAMES, (wq, wk, wv, wo, w_gate, w_up, w_down), strict=True))

    def take(so_far, sequence):
        h, by_y = sequence
        _, back = jax.vjp(stack, weights, h)
        by_weights, by_h = back(by_y)
        return jax.tree.map(lambda total, term: total + term.astype(jnp.float32), so_far, by_weights), by_h

    none_yet = {name: jnp.zeros(w.shape, jnp.float32) for name, w in weights.items()}
    by_weights, by_x = lax.scan(take, none_yet, (x, dy))
    gradients = [by_weights[name].astype(jnp.bfloat16).astype(jnp.float32) for name in NAMES]
    first = (m_wq, m_wk, m_wv, m_wo, m_w_gate, m_w_up, m_w_down)
    second = (v_wq, v_wk, v_wv, v_wo, v_w_gate, v_w_up, v_w_down)
    new = [adamw(weights[name].astype(jnp.float32), m, v, g) for name, m, v, g in zip(NAMES, first, second, gradients, strict=True)]
    return tuple(one[which] for which in range(3) for one in new)
```

```python
import jax
import jax.numpy as jnp
from jax import lax
from jax.experimental import pallas as pl
from jax.experimental.pallas import tpu as pltpu
from jax.sharding import PartitionSpec as P

NAMES = ("wq", "wk", "wv", "wo", "w_gate", "w_up", "w_down")
F32, BF16 = jnp.float32, jnp.bfloat16
TOKENS, D, FF, HEAD, HEADS = 1024, 768, 2048, 128, 6
BLOCK = 256
BLOCKS = TOKENS // BLOCK
THETA = 10000
LOG2E = 1.4426950408889634
SCALE = HEAD**-0.5
POWER = SCALE * LOG2E
HIDDEN = -1e30
LANES, ROW3, ROW8 = 128, 48, 128
COLUMNS = 16


def dot(a, b, ca=1, cb=0):
    return lax.dot_general(a, b, (((ca,), (cb,)), ((), ())), preferred_element_type=F32)


def scale_of(wide):
    return lax.rsqrt(jnp.mean(wide * wide, -1, keepdims=True) + 1e-6)


def each(n, body):
    lax.fori_loop(0, n, lambda j, _: body(j), None)


def rope_tables(freq, near_s, far_s):
    place = lax.broadcasted_iota(jnp.int32, (32, LANES), 0).astype(F32)
    for ref, step in ((near_s, 1.0), (far_s, 32.0)):
        angle = place * step * freq
        ref[0] = jnp.cos(angle)
        ref[1] = jnp.sin(angle)


def rope_at(group, near_s, far_s):
    cn, sn, cf, sf = near_s[0], near_s[1], far_s[0, pl.ds(group, 1), :], far_s[1, pl.ds(group, 1), :]
    return cn * cf - sn * sf, sn * cf + cn * sf


def turn(t, cos, sin):
    return t * cos + pltpu.roll(t, HEAD // 2, 1) * sin


def forward(x_h, dy_h, wq_h, wk_h, wv_h, wo_h, wg_h, wu_h, wd_h, freq, g_h, q_h, k_h, v_h, o_h, a_h, dh_h, lse_h, cos_h, sin_h,
            x, dy, wq, wk, wv, wo, wg, wu, wd, g, q, k, v, o, a, dh, lse, cos_s, sin_s, near_s, far_s, vt, b, bt, act, dg, du, in_sem, out_sem):
    loads = [pltpu.make_async_copy(s, d, in_sem.at[n]) for n, (s, d) in enumerate(
        zip((x_h, wq_h, wk_h, wv_h, wo_h, wg_h, wu_h, wd_h, dy_h), (x, wq, wk, wv, wo, wg, wu, wd, dy)))]
    for load in loads:
        load.start()
    sends = []

    def send(src, dst):
        sends.append(pltpu.make_async_copy(src, dst, out_sem.at[len(sends)]))
        sends[-1].start()

    rope_tables(freq[...], near_s, far_s)
    minus = jnp.where(lax.broadcasted_iota(jnp.int32, (32, LANES), 1) < HEAD // 2, -1.0, 1.0)

    def places(i):
        cos, sin = rope_at(i, near_s, far_s)
        at = pl.ds(pl.multiple_of(i * 32, 32), 32)
        cos_s[at, :] = cos
        sin_s[at, :] = sin * minus
    each(TOKENS // 32, places)

    for load in loads[:4]:
        load.wait()

    def project(i):
        at = pl.ds(pl.multiple_of(i * BLOCK, BLOCK), BLOCK)
        wide = x[at, :].astype(F32)
        low = (wide * scale_of(wide)).astype(BF16)
        a[at, :] = low
        cos, sin = cos_s[at, :], sin_s[at, :]
        for h in range(HEADS):
            q[h, at, :] = turn(dot(low, wq[:, h * HEAD : (h + 1) * HEAD]).astype(BF16).astype(F32), cos, sin).astype(BF16)
        k[at, :] = turn(dot(low, wk[...]).astype(BF16).astype(F32), cos, sin).astype(BF16)
        v[at, :] = dot(low, wv[...]).astype(BF16)
    each(BLOCKS, project)
    vt[:HEAD, :] = v[...].T
    vt[HEAD:, :] = jnp.ones((8, TOKENS), BF16)
    send(a, a_h)
    send(q, q_h)
    send(k, k_h)
    send(v, v_h)
    send(cos_s, cos_h)
    send(sin_s, sin_h)

    seen = lax.broadcasted_iota(jnp.int32, (BLOCK, BLOCK), 0) <= lax.broadcasted_iota(jnp.int32, (BLOCK, BLOCK), 1)
    for i in range(BLOCKS):
        rows, past = slice(i * BLOCK, (i + 1) * BLOCK), i * BLOCK

        def heads(j):
            hs = [j * 3 + n for n in range(3)]
            diag = [jnp.where(seen, dot(k[rows, :], q[h, rows, :], 1, 1), HIDDEN) for h in hs]
            before = [dot(k[:past, :], q[h, rows, :], 1, 1) for h in hs] if i else []
            for n, h in enumerate(hs):
                top = diag[n].max(0, keepdims=True)
                if i:
                    top = jnp.maximum(top, before[n].max(0, keepdims=True))
                p = jnp.exp2((diag[n] - top) * POWER).astype(BF16)
                mix = dot(vt[:, rows], p)
                if i:
                    mix = mix + dot(vt[:, :past], jnp.exp2((before[n] - top) * POWER).astype(BF16))
                total = mix[HEAD : HEAD + 1, :]
                lse[h, :, rows] = top * POWER + jnp.log2(total)
                o[rows, pl.ds(pl.multiple_of(h * HEAD, HEAD), HEAD)] = (mix[:HEAD, :] * (1 / total)).T.astype(BF16)
        each(2, heads)
    send(o, o_h)
    send(lse, lse_h)

    for load in loads[4:]:
        load.wait()

    def rest(i):
        at = pl.ds(pl.multiple_of(i * BLOCK, BLOCK), BLOCK)
        h = (x[at, :].astype(F32) + dot(o[at, :], wo[...]).astype(BF16).astype(F32)).astype(BF16)
        wide = h.astype(F32)
        r = scale_of(wide)
        low = (wide * r).astype(BF16)
        b[at, :] = low
        d_out = dy[at, :]
        back = jnp.zeros((BLOCK, D), F32)
        for t in range(4):
            cols = slice(t * 512, (t + 1) * 512)
            gate, up = dot(low, wg[:, cols]), dot(low, wu[:, cols])
            d_act = dot(d_out, wd[cols, :], 1, 1).astype(BF16).astype(F32)
            sig = 1 / (1 + jnp.exp2(gate * -LOG2E))
            silu = gate * sig
            act[at, cols] = (silu * up).astype(BF16)
            d_gate = (d_act * up * (sig + silu * (1 - sig))).astype(BF16)
            d_up = (d_act * silu).astype(BF16)
            dg[at, cols] = d_gate
            du[at, cols] = d_up
            back = back + dot(d_gate, wg[:, cols], 1, 1) + dot(d_up, wu[:, cols], 1, 1)
        back = back.astype(BF16).astype(F32)
        slope = (back * wide).sum(-1, keepdims=True) * (r * r * r * (1 / D))
        dh[at, :] = (d_out.astype(F32) + (back * r - wide * slope).astype(BF16).astype(F32)).astype(BF16)
    each(BLOCKS, rest)
    send(dh, dh_h)

    def down(i):
        cols = pl.ds(pl.multiple_of(i * 512, 512), 512)
        term = dot(act[:, cols], dy[...], 0, 0).astype(BF16)
        for t in range(6):
            g[t // 3, pl.ds(i * 4, 4), 768 + t % 3 * ROW8 : 768 + (t % 3 + 1) * ROW8, :] = term[:, t * LANES : (t + 1) * LANES].reshape(4, ROW8, LANES)
    each(4, down)
    send(g.at[:, :, pl.ds(768, 384), :], g_h.at[:, :, pl.ds(768, 384), :])
    bt[...] = b[...].T
    for n, d in enumerate((dg, du)):
        def deep(i):
            term = dot(bt[...], d[:, pl.ds(pl.multiple_of(i * 512, 512), 512)]).astype(BF16)
            for t in range(4):
                g[n, :, pl.ds(pl.multiple_of(i * 192 + t * ROW3, ROW3), ROW3), :] = term[:, t * LANES : (t + 1) * LANES].reshape(COLUMNS, ROW3, LANES)
        each(4, deep)
        send(g.at[n, :, pl.ds(0, 768), :], g_h.at[n, :, pl.ds(0, 768), :])
    for one in sends:
        one.wait()


def run_forward(x, dy, w):
    half = HEAD // 2
    freq = THETA ** (-jnp.arange(half, dtype=F32) / half)
    freq = jnp.concatenate([freq, freq])[None]
    low = lambda *shape: (shape, BF16)
    io = [low(2, COLUMNS, 1152, LANES), low(HEADS, TOKENS, HEAD), low(TOKENS, HEAD), low(TOKENS, HEAD), low(TOKENS, D), low(TOKENS, D), low(TOKENS, D),
          ((HEADS, 1, TOKENS), F32), ((TOKENS, LANES), F32), ((TOKENS, LANES), F32)]
    ins = [x, *(w[n] for n in ("wq", "wk", "wv", "wo", "w_gate", "w_up", "w_down")), dy]
    tables = [((2, 32, LANES), F32)] * 2
    rest = [low(HEAD + 8, TOKENS), low(TOKENS, D), low(D, TOKENS), low(TOKENS, FF), low(TOKENS, FF), low(TOKENS, FF)]
    given = [x, dy, *(w[n] for n in ("wq", "wk", "wv", "wo", "w_gate", "w_up", "w_down"))]
    hbm = pl.BlockSpec(memory_space=pl.ANY)
    return pl.pallas_call(
        forward,
        out_shape=[jax.ShapeDtypeStruct(*one) for one in io],
        in_specs=[hbm] * 9 + [pl.BlockSpec(memory_space=pltpu.VMEM)],
        out_specs=[hbm] * len(io),
        scratch_shapes=[pltpu.VMEM(t.shape, BF16) for t in given] + [pltpu.VMEM(*one) for one in io + tables + rest]
        + [pltpu.SemaphoreType.DMA((9,)), pltpu.SemaphoreType.DMA((12,))],
        compiler_params=pltpu.CompilerParams(vmem_limit_bytes=63 * 2**20),
    )(*given, freq)

N, Z = 4, 8


SIX, EIGHT, SIXTEEN = 6, 8, 16


class Batch:
    def __init__(self, deep, wide, flat, cuts):
        self.deep, self.wide, self.flat, self.cuts = deep, wide, flat, cuts
        self.rows = deep * ROW3 + flat * ROW8
        self.space = wide * ROW3 + flat * ROW8
        self.part = wide * SIX + flat * SIXTEEN
        self.own = self.part // TWO
        self.halves = pl.ds(NONE, sum(cuts[:TWO])), pl.ds(sum(cuts[:TWO]), sum(cuts[TWO:]))

    def at(self, q):
        return pl.ds(sum(self.cuts[:q]), self.cuts[q])

    def flat_rows(self, t, z):
        return pl.ds(self.wide * ROW3 + t * ROW8 + z * SIXTEEN, SIXTEEN)

    def flat_share(self, t):
        return slice(self.wide * SIX + t * SIXTEEN, self.wide * SIX + (t + ONE) * SIXTEEN)

    def core_rows(self, core):
        deep = self.part - self.flat * SIXTEEN
        rows = [(slice(NONE, deep // TWO), slice(core * deep // TWO, (core + ONE) * deep // TWO))]
        for t in range(self.flat):
            own, share = deep // TWO + t * EIGHT, deep + t * SIXTEEN + core * EIGHT
            rows.append((slice(own, own + EIGHT), slice(share, share + EIGHT)))
        return rows


NONE, ONE, TWO = range(3)
MLP = Batch(16, 16, 3, (288, 288, 288, 288))
ATT = Batch(7, 8, 0, (80, 80, 80, 96))
RIGHT_SLOT, STRAIGHT, JOINED = range(3)
Q0, Q1, Q2, Q3 = range(4)
THREE = 3


class Axis:
    def __init__(self, i, device):
        self.i, self.right, self.opposite, self.left = i, *(lax.rem(i + k, N) for k in range(ONE, N))
        self.to_right, self.to_left = device(self.right), device(self.left)


class Place:
    def __init__(self):
        me = lax.axis_index("dp")
        self.c = lax.rem(me, TWO)
        self.o = ONE - self.c
        self.z = lax.rem(lax.div(me, TWO), Z)
        self.y = lax.rem(lax.div(me, TWO * Z), N)
        self.x = lax.div(me, TWO * Z * N)
        self.other = self.at(c=self.o)
        self.along_x, self.along_y = Axis(self.x, lambda x: self.at(x=x)), Axis(self.y, lambda y: self.at(y=y))
        self.zs = [lax.rem(self.z + k, Z) for k in range(ONE, Z)]

    def at(self, x=None, y=None, z=None, c=None):
        x, y, z, c = (mine if other is None else other for mine, other in ((self.x, x), (self.y, y), (self.z, z), (self.c, c)))
        return ((x * N + y) * Z + z) * TWO + c


class Copies:
    def __init__(self, send, recv):
        self.send, self.recv, self.n = send, recv, 0
        self.open = []

    def go(self, src, dst, device):
        copy = pltpu.make_async_remote_copy(src_ref=src, dst_ref=dst, send_sem=self.send.at[self.n], recv_sem=self.recv.at[self.n],
                                            device_id={"dp": device}, device_id_type=pl.DeviceIdType.MESH)
        self.n += 1
        copy.start()
        self.open.append(copy)
        return copy

    def finish(self):
        for copy in self.open:
            copy.wait_send()


def greet(p):
    barrier = pltpu.get_barrier_semaphore()
    others = [p.other, p.along_x.to_right, p.along_x.to_left, p.along_y.to_right, p.along_y.to_left] + [p.at(z=z) for z in p.zs]
    for other in others:
        pl.semaphore_signal(barrier, device_id={"dp": other}, device_id_type=pl.DeviceIdType.MESH)
    pl.semaphore_wait(barrier, len(others))


class Ring:
    def __init__(self, copies, axis, inner, quarters, load, keep, out, got, ready=lambda k: None):
        self.__dict__.update(locals())

    def put(self, n, slot, block, add=None):
        def one(j, _):
            term = self.load(block, j, self.quarters[n])
            self.out[n][slot, j] = (term if add is None else self.got[n][add, j].astype(F32) + term).astype(BF16)

        loop(self.inner, one)
        device = self.axis.to_right if (n == NONE) == (slot != STRAIGHT) else self.axis.to_left
        return self.copies.go(self.out[n].at[slot], self.got[n].at[slot], device)

    def start(self):
        at = self.axis
        self.ready(NONE)
        self.far = [self.put(n, RIGHT_SLOT, at.opposite) for n in range(TWO)]
        self.ready(ONE)
        straight = self.put(ONE, STRAIGHT, at.right)
        self.ready(TWO)
        self.straight = [self.put(NONE, STRAIGHT, at.left), straight]

    def middle(self):
        self.joined = []
        for n, block in enumerate((self.axis.right, self.axis.left)):
            self.far[n].wait_recv()
            self.joined.append(self.put(n, JOINED, block, RIGHT_SLOT))

    def end(self):
        self.ready(THREE)
        for n, q in enumerate(self.quarters):
            self.straight[n].wait_recv()
            self.joined[n].wait_recv()

            def one(j, _):
                self.keep(q, j, self.load(self.axis.i, j, q) + self.got[n][STRAIGHT, j].astype(F32) + self.got[n][JOINED, j].astype(F32))

            loop(self.inner, one)


def loop(n, body):
    if n == ONE:
        body(NONE, None)
    else:
        lax.fori_loop(NONE, n, lambda j, _: body(j, None), None)


class Sum:
    def __init__(self, b, copies, p, g, own, bufs):
        self.b, self.copies, self.p, self.g, self.own = b, copies, p, g, own
        self.__dict__.update(bufs)

    def pair(self):
        p, b = self.p, self.b
        self.pairs = []
        first, second = b.halves
        x, y = p.along_x, p.along_y
        for i, j in ((x.opposite, y.opposite), (x.right, y.right), (x.left, y.left), (x.i, y.i)):
            self.pairs.append((self.copies.go(self.g.at[p.o, i, :, first, :], self.other.at[i, :, first, :], p.other),
                               self.copies.go(self.g.at[p.o, :, j, second, :], self.other.at[:, j, second, :], p.other)))

    def rings(self, inner, quarters, load, keep, prefix, ready):
        p, b = self.p, self.b
        made = []
        for which, axis, qs in zip(range(TWO), (p.along_x, p.along_y), quarters):
            out, got = ([getattr(self, f"{prefix}{kind}{q}") for q in qs] for kind in ("out", "in"))
            made.append(Ring(self.copies, axis, inner, qs, lambda i, j, q, which=which: load(which, i, j, b.at(q)), keep, out, got,
                             lambda k, which=which: ready(k, which)))
        return made

    def first(self):
        b = self.b

        def load(which, i, j, rows):
            x, y = (j, i) if which else (i, j)
            return self.own[x, y, rows, :].astype(F32) + self.other[x, y, rows, :].astype(F32)

        def keep(q, j, value):
            self.half[j, b.at(q), :] = value

        self.now = self.rings(N, ((Q0, Q1), (Q2, Q3)), load, keep, "", lambda k, which: self.pairs[k][which].wait_recv())
        for ring in self.now:
            ring.start()

    def middle(self):
        for ring in self.now:
            ring.middle()

    def second(self):
        b = self.b

        def keep(q, j, value):
            self.block[b.at(q), :] = value

        for ring in self.now:
            ring.end()
        self.now = self.rings(ONE, ((Q2, Q3), (Q0, Q1)), lambda which, i, j, rows: self.half[i, rows, :], keep, "s", lambda k, which: None)
        for ring in self.now:
            ring.start()

    def third(self):
        p, b = self.p, self.b
        if b.deep < b.wide:
            self.block[b.deep * ROW3 : b.wide * ROW3, :] = jnp.zeros(((b.wide - b.deep) * ROW3, LANES), F32)
        for ring in self.now:
            ring.end()
        for z in range(Z):
            for q in range(SIX):
                self.shares[z, q * b.wide : (q + ONE) * b.wide, :] = self.block[pl.ds(z * SIX + q, b.wide, stride=ROW3), :]
            for t in range(b.flat):
                self.shares[z, b.flat_share(t), :] = self.block[b.flat_rows(t, z), :]
            self.low[z] = self.shares[z].astype(BF16)
        self.zs = [self.copies.go(self.low.at[z], self.got.at[k], p.at(z=z)) for k, z in enumerate(p.zs)]

    def last(self):
        p, b = self.p, self.b
        total = self.shares[p.z]
        for k, copy in enumerate(self.zs):
            copy.wait_recv()
            total = total + self.got[k].astype(F32)
        for core in range(TWO):
            for own, share in b.core_rows(core):
                self.swap[core, own, :] = total[share, :]
        self.fin = self.copies.go(self.swap.at[p.o], self.swapped, p.other)

    def gradient(self):
        p = self.p
        self.fin.wait_recv()
        self.mine[p.c] = self.swap[p.c]
        self.mine[p.o] = self.swapped[...]


def sum_buffers(b):
    low = lambda *shape: pltpu.VMEM((*shape, LANES), BF16)
    wide = lambda *shape: pltpu.VMEM((*shape, LANES), F32)
    o = {}
    for q, rows in enumerate(b.cuts):
        for kind in ("out", "in"):
            o[f"{kind}{q}"], o[f"s{kind}{q}"] = low(THREE, N, rows), low(THREE, ONE, rows)
    o |= {"other": low(N, N, b.rows), "half": wide(N, b.rows), "block": wide(b.space), "shares": wide(Z, b.part), "low": low(Z, b.part)}
    return o | {"got": low(Z, b.part), "swap": wide(TWO, b.own), "swapped": wide(b.own), "mine": wide(TWO, b.own)}


class Gather:
    def __init__(self, b, copies, p, new, full, bufs):
        self.b, self.copies, self.p, self.new, self.full = b, copies, p, new, full
        self.__dict__.update(bufs)

    def start(self):
        self.fin = self.copies.go(self.new.at[self.p.o], self.pal, self.p.other)

    def along_z(self):
        p, b = self.p, self.b
        self.fin.wait_recv()
        self.both[p.c] = self.new[p.c]
        self.both[p.o] = self.pal[...]
        for core in range(TWO):
            for own, share in b.core_rows(core):
                self.share[share, :] = self.both[core, own, :]
        self.wide_z[p.z] = self.share[...].astype(BF16)
        self.zs = [self.copies.go(self.wide_z.at[p.z], self.wide_z.at[p.z], p.at(z=z)) for z in p.zs]

    def first(self):
        p, b, full = self.p, self.b, self.full
        for copy in self.zs:
            copy.wait_recv()
        for z in range(Z):
            share = self.wide_z[z].astype(F32)
            for q in range(SIX):
                self.block[pl.ds(z * SIX + q, b.wide, stride=ROW3), :] = share[q * b.wide : (q + ONE) * b.wide, :]
            for t in range(b.flat):
                self.block[b.flat_rows(t, z), :] = share[b.flat_share(t), :]
        full[p.c, p.x, p.y] = self.block[: b.rows, :].astype(BF16)
        self.now = [Spread(self.copies, p.along_y, lambda i, q: full.at[p.c, p.x, i, b.at(q), :], (Q0, Q1)),
                    Spread(self.copies, p.along_x, lambda i, q: full.at[p.c, i, p.y, b.at(q), :], (Q2, Q3))]
        for one in self.now:
            one.start()

    def middle(self):
        for one in self.now:
            one.middle()

    def second(self):
        p, b, full = self.p, self.b, self.full
        for one in self.now:
            one.end()
        self.now = [Spread(self.copies, p.along_x, lambda i, q: full.at[p.c, i, :, b.at(q), :], (Q0, Q1)),
                    Spread(self.copies, p.along_y, lambda i, q: full.at[p.c, :, i, b.at(q), :], (Q2, Q3))]
        self.over = []
        for one in self.now:
            one.start()
        for one in self.now:
            for q in one.quarters:
                self.pass_on(one, one.axis.i, q)

    def pass_on(self, spread, i, q):
        ref = spread.ref(i, q)
        self.over.append(self.copies.go(ref, ref, self.p.other))

    def last_middle(self):
        for one in self.now:
            one.middle()
        for one in self.now:
            for i, q in zip((one.axis.left, one.axis.right), one.quarters):
                self.pass_on(one, i, q)

    def end(self):
        for one in self.now:
            one.end()
            a, b = one.quarters
            for i, q in ((one.axis.left, b), (one.axis.right, a), (one.axis.opposite, a), (one.axis.opposite, b)):
                self.pass_on(one, i, q)

    def finish(self):
        for copy in self.over:
            copy.wait_recv()


class Spread:
    def __init__(self, copies, axis, ref, quarters):
        self.__dict__.update(locals())

    def send(self, i, q, device):
        return self.copies.go(self.ref(i, q), self.ref(i, q), device)

    def start(self):
        at, (a, b) = self.axis, self.quarters
        self.turns = [self.send(at.i, a, at.to_right), self.send(at.i, b, at.to_left)]
        self.ends = [self.send(at.i, b, at.to_right), self.send(at.i, a, at.to_left)]

    def middle(self):
        at = self.axis
        for turn, i, q, device in zip(self.turns, (at.left, at.right), self.quarters, (at.to_right, at.to_left)):
            turn.wait_recv()
            self.ends.append(self.send(i, q, device))

    def end(self):
        for copy in self.ends:
            copy.wait_recv()


def gather_buffers(b):
    wide = lambda *shape: pltpu.VMEM((*shape, LANES), F32)
    return {"pal": wide(b.own), "both": wide(TWO, b.own), "share": wide(b.part), "wide_z": pltpu.VMEM((Z, b.part, LANES), BF16)}


DEEP = (("w_gate", 16), ("w_up", 16), ("wq", 6), ("wk", 1), ("wo", 6), ("wv", 1))
SPOT = {"w_gate": (MLP, 0, 0), "w_up": (MLP, 1, 0), "wq": (ATT, 0, 0), "wk": (ATT, 0, 6), "wo": (ATT, 1, 0), "wv": (ATT, 1, 6)}


class Adam:
    def __init__(self, b, p, w, m, v, moments, column32, bufs):
        self.b, self.p, self.w, self.m, self.v, self.moments, self.column32 = b, p, w, m, v, moments, column32
        self.__dict__.update(bufs)

    def fetch(self, sems, n):
        p, b = self.p, self.b
        column = p.x * N + p.y
        self.reads = []
        for name, (batch, _, _) in SPOT.items():
            if batch is b:
                self.reads.append(pltpu.make_async_copy(self.w[name].at[pl.ds(pl.multiple_of(column * 48, 48), 48), :], self.column[name], sems.at[n]))
                n += 1
        if b.flat:
            self.reads.append(pltpu.make_async_copy(self.w["w_down"].at[pl.ds(pl.multiple_of(column * 128, 128), 128), :], self.column["w_down"], sems.at[n]))
            n += 1
        for name, (batch, _, _) in SPOT.items():
            if batch is b:
                self.reads += [pltpu.make_async_copy(src[name], dst[name], sems.at[n + i]) for i, (src, dst) in enumerate(((self.m, self.m_in), (self.v, self.v_in)))]
                n += 2
        if b.flat:
            self.reads += [pltpu.make_async_copy(src["w_down"], dst["w_down"], sems.at[n + i]) for i, (src, dst) in enumerate(((self.m, self.m_in), (self.v, self.v_in)))]
            n += 2
        for read in self.reads:
            read.start()
        return n

    def pack(self):
        p, b = self.p, self.b
        for read in self.reads:
            read.wait()
        if b.deep < b.wide:
            for ref in (self.wp, self.mp, self.vp):
                ref[...] = jnp.zeros_like(ref)
        for name, tiles in DEEP:
            batch, half, first = SPOT[name]
            if batch is not b:
                continue
            wide = self.column32
            for t in range(tiles):
                wide[t * 48 : (t + 1) * 48, :] = self.column[name][:, t * 128 : (t + 1) * 128].astype(F32)
            for r in range(3):
                row = p.z * 6 + p.c * 3 + r
                self.wp[half, r * b.wide + first : r * b.wide + first + tiles, :] = wide[pl.ds(row, tiles, stride=48), :] if tiles > 1 else wide[pl.ds(row, 1), :]
                for t in range(tiles):
                    at = slice(r * b.wide + first + t, r * b.wide + first + t + 1)
                    cols = slice(t * 128, (t + 1) * 128)
                    self.mp[half, at, :] = self.m_in[name][r, :, cols]
                    self.vp[half, at, :] = self.v_in[name][r, :, cols]
        if b.flat:
            wide = self.column32
            for t in range(2 * b.flat):
                wide[t * ROW8 : (t + 1) * ROW8, :] = self.column["w_down"][:, t * LANES : (t + 1) * LANES].astype(F32)
            at = 3 * b.wide
            for t in range(2 * b.flat):
                half, rows, cols = t // b.flat, slice(at + t % b.flat * 8, at + t % b.flat * 8 + 8), slice(t * 128, (t + 1) * 128)
                self.wp[half, rows, :] = wide[pl.ds(pl.multiple_of(t * ROW8 + p.z * 16 + p.c * 8, 8), 8), :]
                self.mp[half, rows, :] = self.m_in["w_down"][:, cols]
                self.vp[half, rows, :] = self.v_in["w_down"][:, cols]

    def step(self, gradient, new):
        g = gradient[...].astype(BF16).astype(F32)
        m = 0.9 * self.mp[...] + 0.1 * g
        v = 0.95 * self.vp[...] + 0.05 * g * g
        w = self.wp[...]
        self.moments[0] = m
        self.moments[1] = v
        new[...] = (w - 0.02 * (m * lax.rsqrt(v + 1e-8) + 0.1 * w)).astype(BF16).astype(F32)


def adam_buffers(b):
    o = {k: pltpu.VMEM((2, b.own, 128), F32) for k in ("wp", "mp", "vp")}
    o["new"] = pltpu.VMEM((2, b.own, 128), F32)
    for name, tiles in DEEP:
        if SPOT[name][0] is b:
            o["column." + name] = pltpu.VMEM((48, tiles * 128), BF16)
            o["m_in." + name] = o["v_in." + name] = pltpu.VMEM((3, 1, tiles * 128), F32)
    if b.flat:
        o["column.w_down"] = pltpu.VMEM((128, 768), BF16)
        o["m_in.w_down"] = o["v_in.w_down"] = pltpu.VMEM((8, 768), F32)
    return o


def nest(flat):
    o = {}
    for key, ref in flat.items():
        if "." in key:
            a, b = key.split(".")
            o.setdefault(a, {})[b] = ref
        else:
            o[key] = ref
    return o


COPIES = 88 * 2


class Back:
    def __init__(self, bufs, g):
        self.__dict__.update(bufs)
        self.g = g

    def put(self, half, tile, term):
        at = tile * ROW3 if isinstance(tile, int) else pl.multiple_of(tile * ROW3, ROW3)
        self.g[half, :, pl.ds(at, ROW3), :] = term.astype(BF16).reshape(COLUMNS, ROW3, LANES)

    def out(self):
        self.kt[...] = self.k[...].T
        self.dk[...] = jnp.zeros_like(self.dk)
        self.dv[...] = jnp.zeros_like(self.dv)
        self.at[...] = self.o[...].T

        def head(h):
            cols = pl.ds(pl.multiple_of(h * HEAD, HEAD), HEAD)
            self.do[h] = dot(self.dh[...], self.wo[cols, :], 1, 1).astype(BF16)
            self.put(1, h, dot(self.at[...], self.dh[:, cols]))

        each(HEADS, head)
        self.at[...] = self.a[...].T

    def scores(self, i, part, heads=3):
        rows, past = slice(i * BLOCK, (i + 1) * BLOCK), i * BLOCK
        seen = lax.broadcasted_iota(jnp.int32, (BLOCK, BLOCK), 0) <= lax.broadcasted_iota(jnp.int32, (BLOCK, BLOCK), 1)
        spans = ([slice(0, past)] if i else []) + [rows]
        ps, dss = [[] for _ in spans], [[] for _ in spans]
        hs = [part * heads + n for n in range(heads)]
        qs, dos = [self.q[h, rows, :] for h in hs], [self.do[h, rows, :] for h in hs]
        scores = [[dot(self.k[at, :], one, 1, 1) for at in spans] for one in qs]
        dps = [[dot(self.v[at, :], one, 1, 1) for at in spans] for one in dos]
        for n, h in enumerate(hs):
            p = [jnp.exp2(s * POWER - self.lse[h, :, rows]) for s in scores[n]]
            p[-1] = jnp.where(seen, p[-1], 0.0)
            delta = sum((one * dp).sum(0, keepdims=True) for one, dp in zip(p, dps[n]))
            ds = [(one * (dp - delta)).astype(BF16) for one, dp in zip(p, dps[n])]
            dq = sum(dot(self.kt[:, at], one) for at, one in zip(spans, ds))
            dq = (dq * SCALE).T.astype(BF16).astype(F32)
            self.o[rows, h * HEAD : (h + 1) * HEAD] = turn(dq, self.cos[rows, :], -self.sin[rows, :]).astype(BF16)
            for m, one in enumerate(p):
                ps[m].append(one.astype(BF16))
                dss[m].append(ds[m])
        do, q = jnp.concatenate(dos, 0), jnp.concatenate(qs, 0)
        for m, at in enumerate(spans):
            self.dv[at, :] += dot(jnp.concatenate(ps[m], 1), do)
            self.dk[at, :] += dot(jnp.concatenate(dss[m], 1), q)

    def end(self):
        self.put(1, HEADS, dot(self.at[...], self.dv[...].astype(BF16)))
        dk = (self.dk[...] * SCALE).astype(BF16).astype(F32)
        self.put(0, HEADS, dot(self.at[...], turn(dk, self.cos[...], -self.sin[...]).astype(BF16)))
        each(HEADS, lambda h: self.put(0, h, dot(self.at[...], self.o[:, pl.ds(pl.multiple_of(h * HEAD, HEAD), HEAD)])))


GIVEN = {"q": ((HEADS, TOKENS, HEAD), BF16), "k": ((TOKENS, HEAD), BF16), "v": ((TOKENS, HEAD), BF16), "o": ((TOKENS, D), BF16), "a": ((TOKENS, D), BF16),
         "dh": ((TOKENS, D), BF16), "lse": ((HEADS, 1, TOKENS), F32), "cos": ((TOKENS, LANES), F32), "sin": ((TOKENS, LANES), F32), "wo": ((D, D), BF16)}
MADE = {"kt": ((HEAD, TOKENS), BF16), "dk": ((TOKENS, HEAD), F32), "dv": ((TOKENS, HEAD), F32), "at": ((D, TOKENS), BF16),
        "do": ((HEADS, TOKENS, HEAD), BF16)}


def exchange(gm, given, weights, m, v):
    batches = (MLP, ATT)
    scratch = {}
    for i, b in enumerate(batches):
        for kind, bufs in (("s", sum_buffers(b)), ("g", gather_buffers(b)), ("a", adam_buffers(b))):
            for key, shape in bufs.items():
                scratch[(i, kind, key)] = shape
    for key, shape in (GIVEN | MADE).items():
        scratch[(0, "b", key)] = pltpu.VMEM(*shape)
    scratch[(0, "own", "m")] = pltpu.VMEM((N, N, MLP.rows, LANES), BF16)
    scratch[(0, "own", "c")] = pltpu.VMEM((MLP.space, LANES), F32)
    scratch[(0, "own", "a")] = pltpu.VMEM((2, COLUMNS, ATT.rows, LANES), BF16)
    keys = list(scratch)

    def kernel(*refs):
        refs = list(refs)
        take = lambda n: [refs.pop(0) for _ in range(n)]
        (g,) = take(1)
        from_hbm = dict(zip(GIVEN, take(len(GIVEN))))
        w, m_in, v_in = (dict(zip(NAMES, take(7))) for _ in range(3))
        full, moments = take(2), take(2)
        bufs = dict(zip(keys, take(len(keys))))
        send, recv, reads, loads = take(4)
        part = lambda i, kind: nest({key[2]: ref for key, ref in bufs.items() if key[:2] == (i, kind)})
        p = Place()
        copies = Copies(send, recv)
        own, ga = bufs[(0, "own", "m")], bufs[(0, "own", "a")]
        four = ga.reshape(2, N, N, ATT.rows, LANES)
        mlp = Sum(MLP, copies, p, g, own, part(0, "s"))
        att = Sum(ATT, copies, p, four, four.at[p.c], part(1, "s"))
        adams = [Adam(b, p, w, m_in, v_in, moments[i], bufs[(0, "own", "c")], part(i, "a")) for i, b in enumerate(batches)]
        gathers = [Gather(b, copies, p, adams[i].new, full[i], part(i, "g") | {"block": bufs[(i, "s", "block")]}) for i, b in enumerate(batches)]
        back = Back(part(0, "b"), ga)
        coming = [pltpu.make_async_copy(from_hbm[key], getattr(back, key), loads.at[n]) for n, key in enumerate(GIVEN)]
        coming.append(pltpu.make_async_copy(g.at[p.c], own, loads.at[len(GIVEN)]))
        for one in coming:
            one.start()
        greet(p)
        mlp.pair()
        n = 0
        for a in adams:
            n = a.fetch(reads, n)
        for one in coming[:-1]:
            one.wait()
        back.out()
        for k in range(TWO):
            back.scores(NONE, k)
        coming[-1].wait()
        mlp.first()
        back.scores(ONE, NONE)
        back.scores(ONE, ONE)
        back.scores(TWO, NONE)
        mlp.middle()
        back.scores(TWO, ONE)
        back.scores(THREE, NONE)
        back.scores(THREE, ONE)
        back.end()
        att.pair()
        mlp.second()
        for a in adams:
            a.pack()
        att.first()
        mlp.middle()
        att.middle()
        mlp.third()
        att.second()
        att.middle()
        mlp.last()
        mlp.gradient()
        adams[0].step(mlp.mine, adams[0].new)
        gathers[0].start()
        att.third()
        gathers[0].along_z()
        att.last()
        att.gradient()
        adams[1].step(att.mine, adams[1].new)
        gathers[1].start()
        gathers[1].along_z()
        for step in ("first", "middle", "second", "last_middle", "end", "finish"):
            for o in gathers:
                getattr(o, step)()
        copies.finish()

    vm, hbm = pl.BlockSpec(memory_space=pltpu.VMEM), pl.BlockSpec(memory_space=pl.ANY)
    order = lambda t: [t[name] for name in NAMES]
    return pl.pallas_call(
        kernel,
        out_shape=[jax.ShapeDtypeStruct((2, N, N, b.rows, LANES), BF16) for b in batches] + [jax.ShapeDtypeStruct((2, 2, b.own, LANES), F32) for b in batches],
        in_specs=[hbm] * (1 + len(GIVEN) + 21),
        out_specs=[vm] * 4,
        scratch_shapes=[scratch[key] for key in keys] + [pltpu.SemaphoreType.DMA((COPIES,)), pltpu.SemaphoreType.DMA((COPIES,)), pltpu.SemaphoreType.DMA((21,)),
                                                         pltpu.SemaphoreType.DMA((len(GIVEN) + 1,))],
        compiler_params=pltpu.CompilerParams(collective_id=0, has_side_effects=True, vmem_limit_bytes=63 * 2**20),
    )(gm, *(given[key] for key in GIVEN), *order(weights), *order(m), *order(v))


def lay_out(full, moments):
    def kernel(fm, fa, mm, ma, *refs):
        outs = {name: refs[n] for n, name in enumerate(NAMES)}
        to = [{name: refs[7 * (i + 1) + n] for n, name in enumerate(NAMES)} for i in range(2)]
        sem = refs[-1]
        copies = []

        def go(src, dst):
            copies.append(pltpu.make_async_copy(src, dst, sem.at[len(copies)]))
            copies[-1].start()

        for name, tiles in DEEP:
            batch, half, first = SPOT[name]
            src, packed = (fm, mm) if batch is MLP else (fa, ma)
            for t in range(tiles):
                go(src.at[half, :, pl.ds((first + t) * ROW3, ROW3), :], outs[name].at[:, :, pl.ds(t * LANES, LANES)])
            for i in range(2):
                for r in range(3):
                    for t in range(tiles):
                        at = r * batch.wide + first + t
                        to[i][name][r, :, t * LANES : (t + 1) * LANES] = packed[i, half, at : at + 1, :]
        for t in range(6):
            half, n = divmod(t, 3)
            go(fm.at[half, :, pl.ds(16 * ROW3 + n * ROW8, ROW8), :], outs["w_down"].at[:, :, pl.ds(t * LANES, LANES)])
            at = 3 * MLP.wide + n * 8
            for i in range(2):
                to[i]["w_down"][:, t * LANES : (t + 1) * LANES] = mm[i, half, at : at + 8, :]
        for copy in copies:
            copy.wait()

    vm, hbm = pl.BlockSpec(memory_space=pltpu.VMEM), pl.BlockSpec(memory_space=pl.ANY)
    wide = {name: tiles * LANES for name, tiles in DEEP}
    weights = [jax.ShapeDtypeStruct((COLUMNS, ROW3, wide[n]) if n in wide else (COLUMNS, ROW8, D), BF16) for n in NAMES]
    moment = [jax.ShapeDtypeStruct((3, 1, wide[n]) if n in wide else (8, D), F32) for n in NAMES]
    out = pl.pallas_call(
        kernel, out_shape=weights + moment + moment, in_specs=[vm] * 4, out_specs=[hbm] * 7 + [vm] * 14,
        scratch_shapes=[pltpu.SemaphoreType.DMA((52,))], compiler_params=pltpu.CompilerParams(vmem_limit_bytes=30 * 2**20),
    )(*(t.reshape(2, COLUMNS, -1, LANES) for t in full), *moments)
    new = [t.reshape(1, -1, t.shape[-1]) for t in out[:7]]
    return new + [t[None] if n == "w_down" else t.transpose(1, 0, 2) for i in (7, 14) for n, t in zip(NAMES, out[i : i + 7])]


def solution(mesh):
    def step(x, dy, *arrays):
        weights, m, v = (dict(zip(NAMES, arrays[i : i + 7], strict=True)) for i in (0, 7, 14))
        weights = {name: w[0] for name, w in weights.items()}
        gm, *given = run_forward(x[0], dy[0], weights)
        given = dict(zip(("q", "k", "v", "o", "a", "dh", "lse", "cos", "sin"), given)) | {"wo": weights["wo"]}
        thin = lambda t: {name: one[0] if name == "w_down" else one.transpose(1, 0, 2) for name, one in t.items()}
        full_m, full_a, mom_m, mom_a = exchange(gm.reshape(2, N, N, MLP.rows, LANES), given, weights, thin(m), thin(v))
        return tuple(lay_out((full_m, full_a), (mom_m, mom_a)))

    states, all_of, cut = P(("rep", "dp"), None, None), P(None, None, None), P(None, "dp", None)
    return jax.shard_map(
        step,
        mesh=mesh,
        in_specs=(states, states) + (all_of,) * 7 + (cut,) * 14,
        out_specs=(P("rep", None, None),) * 7 + (P("rep", "dp", None),) * 14,
        check_vma=False,
    )
```

```python
import jax
import jax.numpy as jnp
from jax import lax
from jax.experimental import pallas as pl
from jax.experimental.pallas import tpu as pltpu
from jax.sharding import PartitionSpec as P

NAMES = ("wq", "wk", "wv", "wo", "w_gate", "w_up", "w_down")
F32, BF16 = jnp.float32, jnp.bfloat16
TOKENS, D, FF, HEAD, HEADS = 1024, 768, 2048, 128, 6
BLOCK = 256
BLOCKS = TOKENS // BLOCK
THETA = 10000
LOG2E = 1.4426950408889634
SCALE = HEAD**-0.5
POWER = SCALE * LOG2E
HIDDEN = -1e30
LANES, ROW3, ROW8 = 128, 48, 128
COLUMNS = 16


def dot(a, b, ca=1, cb=0):
    return lax.dot_general(a, b, (((ca,), (cb,)), ((), ())), preferred_element_type=F32)


def scale_of(wide):
    return lax.rsqrt(jnp.mean(wide * wide, -1, keepdims=True) + 1e-6)


def each(n, body):
    lax.fori_loop(0, n, lambda j, _: body(j), None)


def rope_tables(freq, near_s, far_s):
    place = lax.broadcasted_iota(jnp.int32, (32, LANES), 0).astype(F32)
    for ref, step in ((near_s, 1.0), (far_s, 32.0)):
        angle = place * step * freq
        ref[0] = jnp.cos(angle)
        ref[1] = jnp.sin(angle)


def rope_at(group, near_s, far_s):
    cn, sn, cf, sf = near_s[0], near_s[1], far_s[0, pl.ds(group, 1), :], far_s[1, pl.ds(group, 1), :]
    return cn * cf - sn * sf, sn * cf + cn * sf


def turn(t, cos, sin):
    return t * cos + pltpu.roll(t, HEAD // 2, 1) * sin


def forward(x_h, dy_h, wq_h, wk_h, wv_h, wo_h, wg_h, wu_h, wd_h, freq, deep_h, far_deep_h, flat_h, far_flat_h, q_h, k_h, v_h, o_h, a_h, dh_h, lse_h, cos_h, sin_h,
            x, dy, wq, wk, wv, wo, wg, wu, wd, deep, flat, q, k, v, o, a, dh, lse, cos_s, sin_s, near_s, far_s, vt, b, bt, act, d, in_sem, out_sem, send_sem, recv_sem):
    loads = [pltpu.make_async_copy(s, d, in_sem.at[n]) for n, (s, d) in enumerate(
        zip((x_h, wq_h, wk_h, wv_h, wo_h, wg_h, wu_h, wd_h, dy_h), (x, wq, wk, wv, wo, wg, wu, wd, dy)))]
    for load in loads:
        load.start()
    p = Place()
    greet([p.other])
    copies = Copies(send_sem, recv_sem)
    sends = []

    def send(src, dst):
        sends.append(pltpu.make_async_copy(src, dst, out_sem.at[len(sends)]))
        sends[-1].start()

    rope_tables(freq[...], near_s, far_s)
    minus = jnp.where(lax.broadcasted_iota(jnp.int32, (32, LANES), 1) < HEAD // 2, -1.0, 1.0)

    def places(i):
        cos, sin = rope_at(i, near_s, far_s)
        at = pl.ds(pl.multiple_of(i * 32, 32), 32)
        cos_s[at, :] = cos
        sin_s[at, :] = sin * minus
    each(TOKENS // 32, places)

    for load in loads[:4]:
        load.wait()

    def project(i):
        at = pl.ds(pl.multiple_of(i * BLOCK, BLOCK), BLOCK)
        wide = x[at, :].astype(F32)
        low = (wide * scale_of(wide)).astype(BF16)
        a[at, :] = low
        cos, sin = cos_s[at, :], sin_s[at, :]
        for h in range(HEADS):
            q[h, at, :] = turn(dot(low, wq[:, h * HEAD : (h + 1) * HEAD]).astype(BF16).astype(F32), cos, sin).astype(BF16)
        k[at, :] = turn(dot(low, wk[...]).astype(BF16).astype(F32), cos, sin).astype(BF16)
        v[at, :] = dot(low, wv[...]).astype(BF16)
    each(BLOCKS, project)
    vt[:HEAD, :] = v[...].T
    vt[HEAD:, :] = jnp.ones((8, TOKENS), BF16)
    send(a, a_h)
    send(q, q_h)
    send(k, k_h)
    send(v, v_h)
    send(cos_s, cos_h)
    send(sin_s, sin_h)

    seen = lax.broadcasted_iota(jnp.int32, (BLOCK, BLOCK), 0) <= lax.broadcasted_iota(jnp.int32, (BLOCK, BLOCK), 1)
    for i in range(BLOCKS):
        rows, past = slice(i * BLOCK, (i + 1) * BLOCK), i * BLOCK

        def heads(j):
            hs = [j * 3 + n for n in range(3)]
            diag = [jnp.where(seen, dot(k[rows, :], q[h, rows, :], 1, 1), HIDDEN) for h in hs]
            before = [dot(k[:past, :], q[h, rows, :], 1, 1) for h in hs] if i else []
            for n, h in enumerate(hs):
                top = diag[n].max(0, keepdims=True)
                if i:
                    top = jnp.maximum(top, before[n].max(0, keepdims=True))
                p = jnp.exp2((diag[n] - top) * POWER).astype(BF16)
                mix = dot(vt[:, rows], p)
                if i:
                    mix = mix + dot(vt[:, :past], jnp.exp2((before[n] - top) * POWER).astype(BF16))
                total = mix[HEAD : HEAD + 1, :]
                lse[h, :, rows] = top * POWER + jnp.log2(total)
                o[rows, pl.ds(pl.multiple_of(h * HEAD, HEAD), HEAD)] = (mix[:HEAD, :] * (1 / total)).T.astype(BF16)
        each(2, heads)
    send(o, o_h)
    send(lse, lse_h)

    for load in loads[4:]:
        load.wait()

    def rest(i):
        at = pl.ds(pl.multiple_of(i * BLOCK, BLOCK), BLOCK)
        h = (x[at, :].astype(F32) + dot(o[at, :], wo[...]).astype(BF16).astype(F32)).astype(BF16)
        wide = h.astype(F32)
        r = scale_of(wide)
        low = (wide * r).astype(BF16)
        b[at, :] = low
        d_out = dy[at, :]
        back = jnp.zeros((BLOCK, D), F32)
        for t in range(4):
            cols = slice(t * 512, (t + 1) * 512)
            gate, up = dot(low, wg[:, cols]), dot(low, wu[:, cols])
            d_act = dot(d_out, wd[cols, :], 1, 1).astype(BF16).astype(F32)
            sig = 1 / (1 + jnp.exp2(gate * -LOG2E))
            silu = gate * sig
            act[at, cols] = (silu * up).astype(BF16)
            d_gate = (d_act * up * (sig + silu * (1 - sig))).astype(BF16)
            d_up = (d_act * silu).astype(BF16)
            d[0, at, cols] = d_gate
            d[1, at, cols] = d_up
            back = back + dot(d_gate, wg[:, cols], 1, 1) + dot(d_up, wu[:, cols], 1, 1)
        back = back.astype(BF16).astype(F32)
        slope = (back * wide).sum(-1, keepdims=True) * (r * r * r * (1 / D))
        dh[at, :] = (d_out.astype(F32) + (back * r - wide * slope).astype(BF16).astype(F32)).astype(BF16)
    each(BLOCKS, rest)
    send(dh, dh_h)

    def down(i):
        cols = pl.ds(pl.multiple_of(i * 512, 512), 512)
        term = dot(act[:, cols], dy[...], 0, 0).astype(BF16)
        for t in range(6):
            tile = term[:, t * LANES : (t + 1) * LANES].reshape(4, Z, SIXTEEN, LANES)
            for z in range(Z):
                flat[t // 3, z, pl.ds(i * 4, 4), t % 3 * SIXTEEN : (t % 3 + 1) * SIXTEEN, :] = tile[:, z]

    each(4, down)
    copies.go(flat.at[p.o], far_flat_h, p.other)
    send(flat.at[p.c], flat_h)
    bt[...] = b[...].T

    def columns(half, i):
        term = dot(bt[...], d[half, :, pl.ds(pl.multiple_of(i * 512, 512), 512)]).astype(BF16)
        for t in range(4):
            deep[half, :, pl.ds(pl.multiple_of(i * 192 + t * ROW3, ROW3), ROW3), :] = term[:, t * LANES : (t + 1) * LANES].reshape(COLUMNS, ROW3, LANES)

    for part in range(TWO):
        rows = pl.ds(part * 384, 384)
        each(TWO, lambda i: columns(p.o, part * TWO + i))
        copies.go(deep.at[p.o, :, rows, :], far_deep_h.at[:, rows, :], p.other)
    for part in range(TWO):
        rows = pl.ds(part * 384, 384)
        each(TWO, lambda i: columns(p.c, part * TWO + i))
        send(deep.at[p.c, :, rows, :], deep_h.at[:, rows, :])
    for one in sends:
        one.wait()
    copies.finish(True)


def run_forward(x, dy, w):
    half = HEAD // 2
    freq = THETA ** (-jnp.arange(half, dtype=F32) / half)
    freq = jnp.concatenate([freq, freq])[None]
    low = lambda *shape: (shape, BF16)
    blocks = low(COLUMNS, 768, LANES), low(Z, COLUMNS, ROW3, LANES)
    io = [low(HEADS, TOKENS, HEAD), low(TOKENS, HEAD), low(TOKENS, HEAD), low(TOKENS, D), low(TOKENS, D), low(TOKENS, D),
          ((HEADS, 1, TOKENS), F32), ((TOKENS, LANES), F32), ((TOKENS, LANES), F32)]
    outs = [one for one in blocks for _ in range(TWO)] + io
    two = [((TWO, *shape), kind) for shape, kind in blocks]
    tables = [((2, 32, LANES), F32)] * 2
    rest = [low(HEAD + 8, TOKENS), low(TOKENS, D), low(D, TOKENS), low(TOKENS, FF), low(TWO, TOKENS, FF)]
    given = [x, dy, *(w[n] for n in NAMES)]
    hbm = pl.BlockSpec(memory_space=pl.ANY)
    return pl.pallas_call(
        forward,
        out_shape=[jax.ShapeDtypeStruct(*one) for one in outs],
        in_specs=[hbm] * 9 + [pl.BlockSpec(memory_space=pltpu.VMEM)],
        out_specs=[hbm] * len(outs),
        scratch_shapes=[pltpu.VMEM(t.shape, BF16) for t in given] + [pltpu.VMEM(*one) for one in two + io + tables + rest]
        + [pltpu.SemaphoreType.DMA((n,)) for n in (9, 12, THREE, THREE)],
        compiler_params=pltpu.CompilerParams(collective_id=1, has_side_effects=True, vmem_limit_bytes=63 * 2**20),
    )(*given, freq)

N, Z = 4, 8


SIX, EIGHT, SIXTEEN = 6, 8, 16


class Batch:
    def __init__(self, deep, wide, flat, cuts):
        self.deep, self.wide, self.flat, self.cuts = deep, wide, flat, cuts
        self.rows = deep * ROW3 + flat * ROW8
        self.space = wide * ROW3 + flat * ROW8
        self.part = wide * SIX + flat * SIXTEEN
        self.own = self.part // TWO
        self.halves = pl.ds(NONE, sum(cuts[:TWO])), pl.ds(sum(cuts[:TWO]), sum(cuts[TWO:]))

    def at(self, q):
        return pl.ds(sum(self.cuts[:q]), self.cuts[q])

    def core_rows(self, core):
        deep = self.part - self.flat * SIXTEEN
        rows = [(slice(NONE, deep // TWO), slice(core * deep // TWO, (core + ONE) * deep // TWO))] if deep else []
        for t in range(self.flat):
            own, share = deep // TWO + t * EIGHT, deep + t * SIXTEEN + core * EIGHT
            rows.append((slice(own, own + EIGHT), slice(share, share + EIGHT)))
        return rows


NONE, ONE, TWO = range(3)
MLP = Batch(16, 16, 0, (192, 192, 192, 192))
ATT = Batch(7, 8, 0, (96, 96, 96, 48))
DOWN = Batch(0, 0, 3, ())
RIGHT_SLOT, STRAIGHT, JOINED = range(3)
Q0, Q1, Q2, Q3 = range(4)
THREE = 3


class Writes:
    def __init__(self, sems):
        self.sems, self.open = sems, []

    def go(self, src, dst):
        self.open.append(pltpu.make_async_copy(src, dst, self.sems.at[len(self.open)]))
        self.open[-ONE].start()

    def finish(self):
        for copy in self.open:
            copy.wait()


class Axis:
    def __init__(self, i, device):
        self.i, self.right, self.opposite, self.left = i, *(lax.rem(i + k, N) for k in range(ONE, N))
        self.to_right, self.to_left = device(self.right), device(self.left)


class Place:
    def __init__(self):
        me = lax.axis_index("dp")
        self.c = lax.rem(me, TWO)
        self.o = ONE - self.c
        self.z = lax.rem(lax.div(me, TWO), Z)
        self.y = lax.rem(lax.div(me, TWO * Z), N)
        self.x = lax.div(me, TWO * Z * N)
        self.other = self.at(c=self.o)
        self.along_x, self.along_y = Axis(self.x, lambda x: self.at(x=x)), Axis(self.y, lambda y: self.at(y=y))
        self.zs = [lax.rem(self.z + k, Z) for k in range(ONE, Z)]
        self.plane = [(lax.rem(self.x + k // N, N), lax.rem(self.y + k % N, N)) for k in range(ONE, N * N)]

    def everyone(self):
        return [self.other] + [self.at(z=z) for z in self.zs] + [self.at(x=x, y=y) for x, y in self.plane]

    def at(self, x=None, y=None, z=None, c=None):
        x, y, z, c = (mine if other is None else other for mine, other in ((self.x, x), (self.y, y), (self.z, z), (self.c, c)))
        return ((x * N + y) * Z + z) * TWO + c


class Copies:
    def __init__(self, send, recv):
        self.send, self.recv, self.n = send, recv, 0
        self.open = []

    def go(self, src, dst, device):
        copy = pltpu.make_async_remote_copy(src_ref=src, dst_ref=dst, send_sem=self.send.at[self.n], recv_sem=self.recv.at[self.n],
                                            device_id={"dp": device}, device_id_type=pl.DeviceIdType.MESH)
        self.n += 1
        copy.start()
        self.open.append(copy)
        return copy

    def finish(self, arrived=False):
        for copy in self.open:
            copy.wait_send()
            if arrived:
                copy.wait_recv()


def greet(others):
    barrier = pltpu.get_barrier_semaphore()
    for other in others:
        pl.semaphore_signal(barrier, device_id={"dp": other}, device_id_type=pl.DeviceIdType.MESH)
    pl.semaphore_wait(barrier, len(others))


class Ring:
    def __init__(self, copies, axis, inner, quarters, load, keep, out, got, ready=lambda k: None):
        self.__dict__.update(locals())

    def put(self, n, slot, block, add=None):
        def one(j, _):
            term = self.load(block, j, self.quarters[n])
            self.out[n][slot, j] = (term if add is None else self.got[n][add, j].astype(F32) + term).astype(BF16)

        loop(self.inner, one)
        device = self.axis.to_right if (n == NONE) == (slot != STRAIGHT) else self.axis.to_left
        return self.copies.go(self.out[n].at[slot], self.got[n].at[slot], device)

    def start(self):
        at = self.axis
        self.ready(NONE)
        self.far = [self.put(n, RIGHT_SLOT, at.opposite) for n in range(TWO)]
        self.ready(ONE)
        straight = self.put(ONE, STRAIGHT, at.right)
        self.ready(TWO)
        self.straight = [self.put(NONE, STRAIGHT, at.left), straight]

    def middle(self):
        self.joined = []
        for n, block in enumerate((self.axis.right, self.axis.left)):
            self.far[n].wait_recv()
            self.joined.append(self.put(n, JOINED, block, RIGHT_SLOT))

    def end(self):
        self.ready(THREE)
        for n, q in enumerate(self.quarters):
            self.straight[n].wait_recv()
            self.joined[n].wait_recv()

            def one(j, _):
                self.keep(q, j, self.load(self.axis.i, j, q) + self.got[n][STRAIGHT, j].astype(F32) + self.got[n][JOINED, j].astype(F32))

            loop(self.inner, one)


def loop(n, body):
    if n == ONE:
        body(NONE, None)
    else:
        lax.fori_loop(NONE, n, lambda j, _: body(j, None), None)


class Sum:
    def __init__(self, b, copies, p, g, own, bufs):
        self.b, self.copies, self.p, self.g, self.own, self.pairs = b, copies, p, g, own, []
        self.__dict__.update(bufs)

    def pair(self):
        p, b = self.p, self.b
        first, second = b.halves
        x, y = p.along_x, p.along_y
        for i, j in ((x.opposite, y.opposite), (x.right, y.right), (x.left, y.left), (x.i, y.i)):
            self.pairs.append((self.copies.go(self.g.at[p.o, i, :, first, :], self.other.at[i, :, first, :], p.other),
                               self.copies.go(self.g.at[p.o, :, j, second, :], self.other.at[:, j, second, :], p.other)))

    def rings(self, inner, quarters, load, keep, prefix, ready):
        p, b = self.p, self.b
        made = []
        for which, axis, qs in zip(range(TWO), (p.along_x, p.along_y), quarters):
            out, got = ([getattr(self, f"{prefix}{kind}{q}") for q in qs] for kind in ("out", "in"))
            made.append(Ring(self.copies, axis, inner, qs, lambda i, j, q, which=which: load(which, i, j, b.at(q)), keep, out, got,
                             lambda k, which=which: ready(k, which)))
        return made

    def first(self):
        b = self.b

        def load(which, i, j, rows):
            x, y = (j, i) if which else (i, j)
            return self.own[x, y, rows, :].astype(F32) + self.other[x, y, rows, :].astype(F32)

        def keep(q, j, value):
            self.half[j, b.at(q), :] = value

        self.now = self.rings(N, ((Q0, Q1), (Q2, Q3)), load, keep, "", lambda k, which: self.pairs and self.pairs[k][which].wait_recv())
        for ring in self.now:
            ring.start()

    def middle(self):
        for ring in self.now:
            ring.middle()

    def second(self):
        b = self.b

        def keep(q, j, value):
            self.block[b.at(q), :] = value

        for ring in self.now:
            ring.end()
        self.now = self.rings(ONE, ((Q2, Q3), (Q0, Q1)), lambda which, i, j, rows: self.half[i, rows, :], keep, "s", lambda k, which: None)
        for ring in self.now:
            ring.start()

    def third(self):
        p, b = self.p, self.b
        if b.deep < b.wide:
            self.block[b.deep * ROW3 : b.wide * ROW3, :] = jnp.zeros(((b.wide - b.deep) * ROW3, LANES), F32)
        for ring in self.now:
            ring.end()
        for z in range(Z):
            for q in range(SIX):
                self.shares[z, q * b.wide : (q + ONE) * b.wide, :] = self.block[pl.ds(z * SIX + q, b.wide, stride=ROW3), :]
            self.low[z] = self.shares[z].astype(BF16)
        self.zs = [self.copies.go(self.low.at[z], self.got.at[k], p.at(z=z)) for k, z in enumerate(p.zs)]

    def last(self):
        p, b = self.p, self.b
        total = self.shares[p.z]
        for k, copy in enumerate(self.zs):
            copy.wait_recv()
            total = total + self.got[k].astype(F32)
        self.exchange_cores(total)

    def exchange_cores(self, total):
        p, b = self.p, self.b
        for core in range(TWO):
            for own, share in b.core_rows(core):
                self.swap[core, own, :] = total[share, :]
        self.fin = self.copies.go(self.swap.at[p.o], self.swapped, p.other)

    def gradient(self):
        p = self.p
        self.fin.wait_recv()
        self.mine[p.c] = self.swap[p.c]
        self.mine[p.o] = self.swapped[...]


def sum_buffers(b):
    low = lambda *shape: pltpu.VMEM((*shape, LANES), BF16)
    wide = lambda *shape: pltpu.VMEM((*shape, LANES), F32)
    o = {}
    for q, rows in enumerate(b.cuts):
        for kind in ("out", "in"):
            o[f"{kind}{q}"], o[f"s{kind}{q}"] = low(THREE, N, rows), low(THREE, ONE, rows)
    o |= {"other": low(N, N, b.rows), "half": wide(N, b.rows), "block": wide(b.space), "shares": wide(Z, b.part), "low": low(Z, b.part)}
    return o | {"got": low(Z, b.part), "swap": wide(TWO, b.own), "swapped": wide(b.own), "mine": wide(TWO, b.own)}


class Gather:
    def __init__(self, b, copies, p, new, full, result, writes, bufs):
        self.b, self.copies, self.p, self.new, self.full, self.result, self.writes = b, copies, p, new, full, result, writes
        self.__dict__.update(bufs)

    def start(self):
        self.fin = self.copies.go(self.new.at[self.p.o], self.pal, self.p.other)

    def assemble(self):
        p, b = self.p, self.b
        self.fin.wait_recv()
        self.both[p.c] = self.new[p.c]
        self.both[p.o] = self.pal[...]
        for core in range(TWO):
            for own, share in b.core_rows(core):
                self.share[share, :] = self.both[core, own, :]

    def along_z(self):
        p = self.p
        self.assemble()
        self.wide_z[p.z] = self.share[...].astype(BF16)
        self.zs = [self.copies.go(self.wide_z.at[p.z], self.wide_z.at[p.z], p.at(z=z)) for z in p.zs]

    def first(self):
        p, b, full = self.p, self.b, self.full
        for copy in self.zs:
            copy.wait_recv()
        for z in range(Z):
            share = self.wide_z[z].astype(F32)
            for q in range(SIX):
                self.block[pl.ds(z * SIX + q, b.wide, stride=ROW3), :] = share[q * b.wide : (q + ONE) * b.wide, :]
        full[p.c, p.x, p.y] = self.block[: b.rows, :].astype(BF16)
        self.now = [Spread(self.copies, p.along_y, lambda i, q: full.at[p.c, p.x, i, b.at(q), :], (Q0, Q1)),
                    Spread(self.copies, p.along_x, lambda i, q: full.at[p.c, i, p.y, b.at(q), :], (Q2, Q3))]
        for one in self.now:
            one.start()

    def middle(self):
        for one in self.now:
            one.middle()

    def second(self):
        p, b, full = self.p, self.b, self.full
        for one in self.now:
            one.end()
        across = lambda i, q, core=p.c, of=full: of.at[core, i, :, b.at(q), :]
        along = lambda i, q, core=p.c, of=full: of.at[core, :, i, b.at(q), :]
        self.now = [Spread(self.copies, p.along_x, across, (Q0, Q1)), Spread(self.copies, p.along_y, along, (Q2, Q3))]
        self.over = []
        for one in self.now:
            one.start()
        for one in self.now:
            for q in one.quarters:
                self.pass_on(one.ref, one.axis.i, q)

    def pass_on(self, ref, i, q):
        piece = ref(i, q)
        self.over.append((self.copies.go(piece, piece, self.p.other), lambda: self.put(ref, i, q, self.p.o)))
        self.put(ref, i, q, self.p.c)

    def put(self, ref, i, q, core):
        self.writes.go(ref(i, q, core), ref(i, q, core, self.result))

    def last_middle(self):
        for one in self.now:
            one.middle()
        for one in self.now:
            for i, q in zip((one.axis.left, one.axis.right), one.quarters):
                self.pass_on(one.ref, i, q)

    def end(self):
        for one in self.now:
            one.end()
            a, b = one.quarters
            for i, q in ((one.axis.left, b), (one.axis.right, a), (one.axis.opposite, a), (one.axis.opposite, b)):
                self.pass_on(one.ref, i, q)

    def finish(self):
        for copy, put in self.over:
            copy.wait_recv()
            put()


class Spread:
    def __init__(self, copies, axis, ref, quarters):
        self.__dict__.update(locals())

    def send(self, i, q, device):
        return self.copies.go(self.ref(i, q), self.ref(i, q), device)

    def start(self):
        at, (a, b) = self.axis, self.quarters
        self.turns = [self.send(at.i, a, at.to_right), self.send(at.i, b, at.to_left)]
        self.ends = [self.send(at.i, b, at.to_right), self.send(at.i, a, at.to_left)]

    def middle(self):
        at = self.axis
        for turn, i, q, device in zip(self.turns, (at.left, at.right), self.quarters, (at.to_right, at.to_left)):
            turn.wait_recv()
            self.ends.append(self.send(i, q, device))

    def end(self):
        for copy in self.ends:
            copy.wait_recv()


def gather_buffers(b):
    wide = lambda *shape: pltpu.VMEM((*shape, LANES), F32)
    o = {"pal": wide(b.own), "both": wide(TWO, b.own), "share": wide(b.part)}
    return o | ({"wide_z": pltpu.VMEM((Z, b.part, LANES), BF16)} if b.deep else {})


HALF = N * N // TWO


class Flow:
    def __init__(self, copies, p, sign, reach, half):
        self.copies, self.p, self.sign, self.reach, self.half = copies, p, sign, reach, half
        self.device = p.at(z=lax.rem(p.z + Z + sign, Z))
        self.n, self.last = NONE, None

    def z(self, steps):
        return lax.rem(self.p.z + Z + self.sign * steps, Z)


def flows(copies, p):
    return [Flow(copies, p, sign, reach, half) for sign, reaches in ((ONE, (4, 3)), (-ONE, (3, 4))) for half, reach in enumerate(reaches)]


class DownSum(Sum):
    def term(self, z, j):
        return self.own[z, j].astype(F32) + self.other[z, j].astype(F32)

    def along_z(self):
        if not hasattr(self, "flows"):
            self.flows = flows(self.copies, self.p)
        for f, (flow, out, got) in enumerate(zip(self.flows, self.outs.values(), self.gots.values())):
            n = flow.n
            if n == flow.reach:
                continue
            if flow.last:
                flow.last.wait_recv()
            z = flow.z(flow.reach - n)

            def one(j, _):
                term = self.term(z, flow.half * HALF + j)
                out[n, j] = (got[n - ONE, j].astype(F32) + term if n else term).astype(BF16)

            loop(HALF, one)
            flow.last = self.copies.go(out.at[n], got.at[n], flow.device)
            flow.n = n + ONE

    def in_plane(self):
        p = self.p
        for flow in self.flows:
            flow.last.wait_recv()
        for half in range(TWO):
            mine = [(flow.reach - ONE, got) for flow, got in zip(self.flows, self.gots.values()) if flow.half == half]

            def one(j, _):
                at = half * HALF + j
                total = self.term(p.z, at)
                for n, got in mine:
                    total = total + got[n, j].astype(F32)
                self.block[at] = total
                self.low[at] = total.astype(BF16)

            loop(HALF, one)
        self.plane = [self.copies.go(self.low.at[x * N + y], self.got.at[k], p.at(x=x, y=y)) for k, (x, y) in enumerate(p.plane)]

    def last(self):
        p = self.p
        total = self.block[p.x * N + p.y]
        for k, copy in enumerate(self.plane):
            copy.wait_recv()
            total = total + self.got[k].astype(F32)
        self.exchange_cores(total)


class DownGather(Gather):
    def in_plane(self):
        p, b, full = self.p, self.b, self.full
        self.assemble()
        me = p.x * N + p.y
        full[p.c, p.z, me] = self.share[...].astype(BF16)
        ref = full.at[p.c, p.z, me]
        self.plane = [self.copies.go(ref, ref, p.at(x=x, y=y)) for x, y in p.plane]

    def ref(self, z, half, core=None, of=None):
        return (self.full if of is None else of).at[self.p.c if core is None else core, z, pl.ds(half * HALF, HALF)]

    def along_z(self):
        p = self.p
        if not hasattr(self, "flows"):
            for copy in self.plane:
                copy.wait_recv()
            self.flows, self.over = flows(self.copies, p), []
            for half in range(TWO):
                self.pass_on(self.ref, p.z, half)
        for flow in self.flows:
            if flow.last:
                flow.last.wait_recv()
                flow.last = None
                self.pass_on(self.ref, flow.z(-flow.n), flow.half)
            if flow.n < flow.reach:
                ref = self.ref(flow.z(-flow.n), flow.half)
                flow.last = self.copies.go(ref, ref, flow.device)
                flow.n += ONE


def down_buffers():
    low = lambda *shape: pltpu.VMEM((*shape, LANES), BF16)
    wide = lambda *shape: pltpu.VMEM((*shape, LANES), F32)
    o = {"own": low(Z, N * N, ROW3), "other": low(Z, N * N, ROW3), "low": low(N * N, ROW3), "got": low(N * N, ROW3), "block": wide(N * N, ROW3)}
    for i, n in enumerate((4, 3, 3, 4)):
        o[f"outs.{i}"], o[f"gots.{i}"] = low(n, HALF, ROW3), low(n, HALF, ROW3)
    return o | {"swap": wide(TWO, DOWN.own), "swapped": wide(DOWN.own), "mine": wide(TWO, DOWN.own)}


DEEP = (("w_gate", 16), ("w_up", 16), ("wq", 6), ("wk", 1), ("wo", 6), ("wv", 1))
SPOT = {"w_gate": (MLP, 0, 0), "w_up": (MLP, 1, 0), "wq": (ATT, 0, 0), "wk": (ATT, 0, 6), "wo": (ATT, 1, 0), "wv": (ATT, 1, 6)}


class Adam:
    def __init__(self, b, p, w, m, v, moments, column32, bufs):
        self.b, self.p, self.w, self.m, self.v, self.moments, self.column32 = b, p, w, m, v, moments, column32
        self.__dict__.update(bufs)

    def fetch(self, sems, n):
        p, b = self.p, self.b
        column = p.x * N + p.y
        self.reads = []
        for name, (batch, _, _) in SPOT.items():
            if batch is b:
                self.reads.append(pltpu.make_async_copy(self.w[name].at[pl.ds(pl.multiple_of(column * 48, 48), 48), :], self.column[name], sems.at[n]))
                n += 1
        if b.flat:
            self.reads.append(pltpu.make_async_copy(self.w["w_down"].at[pl.ds(pl.multiple_of(column * 128, 128), 128), :], self.column["w_down"], sems.at[n]))
            n += 1
        for name, (batch, _, _) in SPOT.items():
            if batch is b:
                self.reads += [pltpu.make_async_copy(src[name], dst[name], sems.at[n + i]) for i, (src, dst) in enumerate(((self.m, self.m_in), (self.v, self.v_in)))]
                n += 2
        if b.flat:
            self.reads += [pltpu.make_async_copy(src["w_down"], dst["w_down"], sems.at[n + i]) for i, (src, dst) in enumerate(((self.m, self.m_in), (self.v, self.v_in)))]
            n += 2
        for read in self.reads:
            read.start()
        return n

    def pack(self):
        p, b = self.p, self.b
        for read in self.reads:
            read.wait()
        if b.deep < b.wide:
            for ref in (self.wp, self.mp, self.vp):
                ref[...] = jnp.zeros_like(ref)
        for name, tiles in DEEP:
            batch, half, first = SPOT[name]
            if batch is not b:
                continue
            wide = self.column32
            for t in range(tiles):
                wide[t * 48 : (t + 1) * 48, :] = self.column[name][:, t * 128 : (t + 1) * 128].astype(F32)
            for r in range(3):
                row = p.z * 6 + p.c * 3 + r
                self.wp[half, r * b.wide + first : r * b.wide + first + tiles, :] = wide[pl.ds(row, tiles, stride=48), :] if tiles > 1 else wide[pl.ds(row, 1), :]
                for t in range(tiles):
                    at = slice(r * b.wide + first + t, r * b.wide + first + t + 1)
                    cols = slice(t * 128, (t + 1) * 128)
                    self.mp[half, at, :] = self.m_in[name][r, :, cols]
                    self.vp[half, at, :] = self.v_in[name][r, :, cols]
        if b.flat:
            wide = self.column32
            for t in range(2 * b.flat):
                wide[t * ROW8 : (t + 1) * ROW8, :] = self.column["w_down"][:, t * LANES : (t + 1) * LANES].astype(F32)
            at = 3 * b.wide
            for t in range(2 * b.flat):
                half, rows, cols = t // b.flat, slice(at + t % b.flat * 8, at + t % b.flat * 8 + 8), slice(t * 128, (t + 1) * 128)
                self.wp[half, rows, :] = wide[pl.ds(pl.multiple_of(t * ROW8 + p.z * 16 + p.c * 8, 8), 8), :]
                self.mp[half, rows, :] = self.m_in["w_down"][:, cols]
                self.vp[half, rows, :] = self.v_in["w_down"][:, cols]

    def step(self, gradient, new):
        g = gradient[...].astype(BF16).astype(F32)
        m = 0.9 * self.mp[...] + 0.1 * g
        v = 0.95 * self.vp[...] + 0.05 * g * g
        w = self.wp[...]
        self.moments[0] = m
        self.moments[1] = v
        new[...] = (w - 0.02 * (m * lax.rsqrt(v + 1e-8) + 0.1 * w)).astype(BF16).astype(F32)


def adam_buffers(b):
    o = {k: pltpu.VMEM((2, b.own, 128), F32) for k in ("wp", "mp", "vp")}
    o["new"] = pltpu.VMEM((2, b.own, 128), F32)
    for name, tiles in DEEP:
        if SPOT[name][0] is b:
            o["column." + name] = pltpu.VMEM((48, tiles * 128), BF16)
            o["m_in." + name] = o["v_in." + name] = pltpu.VMEM((3, 1, tiles * 128), F32)
    if b.flat:
        o["column.w_down"] = pltpu.VMEM((128, 768), BF16)
        o["m_in.w_down"] = o["v_in.w_down"] = pltpu.VMEM((8, 768), F32)
    return o


def nest(flat):
    o = {}
    for key, ref in flat.items():
        if "." in key:
            a, b = key.split(".")
            o.setdefault(a, {})[b] = ref
        else:
            o[key] = ref
    return o


COPIES = 244


class Back:
    def __init__(self, bufs, g):
        self.__dict__.update(bufs)
        self.g = g

    def put(self, half, tile, term):
        at = tile * ROW3 if isinstance(tile, int) else pl.multiple_of(tile * ROW3, ROW3)
        self.g[half, :, pl.ds(at, ROW3), :] = term.astype(BF16).reshape(COLUMNS, ROW3, LANES)

    def out(self):
        self.kt[...] = self.k[...].T
        self.dk[...] = jnp.zeros_like(self.dk)
        self.dv[...] = jnp.zeros_like(self.dv)
        self.at[...] = self.o[...].T

        def head(h):
            cols = pl.ds(pl.multiple_of(h * HEAD, HEAD), HEAD)
            self.do[h] = dot(self.dh[...], self.wo[cols, :], 1, 1).astype(BF16)
            self.put(1, h, dot(self.at[...], self.dh[:, cols]))

        each(HEADS, head)
        self.at[...] = self.a[...].T

    def scores(self, i, part, heads=3):
        rows, past = slice(i * BLOCK, (i + 1) * BLOCK), i * BLOCK
        seen = lax.broadcasted_iota(jnp.int32, (BLOCK, BLOCK), 0) <= lax.broadcasted_iota(jnp.int32, (BLOCK, BLOCK), 1)
        spans = ([slice(0, past)] if i else []) + [rows]
        ps, dss = [[] for _ in spans], [[] for _ in spans]
        hs = [part * heads + n for n in range(heads)]
        qs, dos = [self.q[h, rows, :] for h in hs], [self.do[h, rows, :] for h in hs]
        scores = [[dot(self.k[at, :], one, 1, 1) for at in spans] for one in qs]
        dps = [[dot(self.v[at, :], one, 1, 1) for at in spans] for one in dos]
        for n, h in enumerate(hs):
            p = [jnp.exp2(s * POWER - self.lse[h, :, rows]) for s in scores[n]]
            p[-1] = jnp.where(seen, p[-1], 0.0)
            delta = sum((one * dp).sum(0, keepdims=True) for one, dp in zip(p, dps[n]))
            ds = [(one * (dp - delta)).astype(BF16) for one, dp in zip(p, dps[n])]
            dq = sum(dot(self.kt[:, at], one) for at, one in zip(spans, ds))
            dq = (dq * SCALE).T.astype(BF16).astype(F32)
            self.o[rows, h * HEAD : (h + 1) * HEAD] = turn(dq, self.cos[rows, :], -self.sin[rows, :]).astype(BF16)
            for m, one in enumerate(p):
                ps[m].append(one.astype(BF16))
                dss[m].append(ds[m])
        do, q = jnp.concatenate(dos, 0), jnp.concatenate(qs, 0)
        for m, at in enumerate(spans):
            self.dv[at, :] += dot(jnp.concatenate(ps[m], 1), do)
            self.dk[at, :] += dot(jnp.concatenate(dss[m], 1), q)

    def end(self):
        self.put(1, HEADS, dot(self.at[...], self.dv[...].astype(BF16)))
        dk = (self.dk[...] * SCALE).astype(BF16).astype(F32)
        self.put(0, HEADS, dot(self.at[...], turn(dk, self.cos[...], -self.sin[...]).astype(BF16)))
        each(HEADS, lambda h: self.put(0, h, dot(self.at[...], self.o[:, pl.ds(pl.multiple_of(h * HEAD, HEAD), HEAD)])))


GIVEN = {"q": ((HEADS, TOKENS, HEAD), BF16), "k": ((TOKENS, HEAD), BF16), "v": ((TOKENS, HEAD), BF16), "o": ((TOKENS, D), BF16), "a": ((TOKENS, D), BF16),
         "dh": ((TOKENS, D), BF16), "lse": ((HEADS, 1, TOKENS), F32), "cos": ((TOKENS, LANES), F32), "sin": ((TOKENS, LANES), F32), "wo": ((D, D), BF16)}
MADE = {"kt": ((HEAD, TOKENS), BF16), "dk": ((TOKENS, HEAD), F32), "dv": ((TOKENS, HEAD), F32), "at": ((D, TOKENS), BF16),
        "do": ((HEADS, TOKENS, HEAD), BF16)}


BATCHES = {"deep": MLP, "down": DOWN, "att": ATT}
SHAPES = {"deep": (N, N, MLP.rows), "down": (Z, N * N, ROW3), "att": (N, N, ATT.rows)}
WRITES = 96


def exchange(terms, given, weights, m, v):
    scratch = {}
    for i, b in BATCHES.items():
        sums = sum_buffers(b) if b.deep else down_buffers()
        for kind, bufs in (("s", sums), ("g", gather_buffers(b)), ("a", adam_buffers(b)), ("full", {i: pltpu.VMEM((TWO, *SHAPES[i], LANES), BF16)})):
            for key, shape in bufs.items():
                scratch[(i, kind, key)] = shape
    for key, shape in (GIVEN | MADE).items():
        scratch[("att", "b", key)] = pltpu.VMEM(*shape)
    scratch[("deep", "s", "own")] = pltpu.VMEM((N, N, MLP.rows, LANES), BF16)
    scratch[("att", "terms", "")] = pltpu.VMEM((TWO, COLUMNS, ATT.rows, LANES), BF16)
    scratch[("all", "column", "")] = pltpu.VMEM((MLP.space, LANES), F32)
    keys = list(scratch)

    def kernel(*refs):
        refs = list(refs)
        take = lambda n: [refs.pop(NONE) for _ in range(n)]
        term = take(len(terms))
        from_hbm = dict(zip(GIVEN, take(len(GIVEN))))
        w, m_in, v_in = (dict(zip(NAMES, take(len(NAMES)))) for _ in range(THREE))
        result, moments = (dict(zip(BATCHES, take(len(BATCHES)))) for _ in range(TWO))
        bufs = dict(zip(keys, take(len(keys))))
        send, recv, reads, loads, out_sems = refs
        part = lambda i, kind: nest({key[TWO]: ref for key, ref in bufs.items() if key[:TWO] == (i, kind)})
        p = Place()
        copies, writes = Copies(send, recv), Writes(out_sems)
        ga = bufs[("att", "terms", "")]
        four = ga.reshape(TWO, N, N, ATT.rows, LANES)
        deep = Sum(MLP, copies, p, None, None, part("deep", "s"))
        down = DownSum(DOWN, copies, p, None, None, part("down", "s"))
        att = Sum(ATT, copies, p, four, four.at[p.c], part("att", "s"))
        sums = {"deep": deep, "down": down, "att": att}
        adams = {i: Adam(b, p, w, m_in, v_in, moments[i], bufs[("all", "column", "")], part(i, "a")) for i, b in BATCHES.items()}
        out = {}
        for i, b in BATCHES.items():
            block = {"block": bufs[(i, "s", "block")]} if b.deep else {}
            kind = Gather if b.deep else DownGather
            out[i] = kind(b, copies, p, adams[i].new, bufs[(i, "full", i)], result[i], writes, part(i, "g") | block)
        back = Back(part("att", "b"), ga)
        pairs = list(zip(term, (deep.own, deep.other, down.own, down.other))) + [(from_hbm[key], getattr(back, key)) for key in GIVEN]
        coming = [pltpu.make_async_copy(src, dst, loads.at[n]) for n, (src, dst) in enumerate(pairs)]
        for one in coming:
            one.start()
        n = NONE
        for a in adams.values():
            n = a.fetch(reads, n)
        greet(p.everyone())
        for one in coming[:TWO]:
            one.wait()
        deep.first()
        for one in coming[TWO:4]:
            one.wait()
        down.along_z()
        for one in coming[4:]:
            one.wait()
        back.out()
        for k in range(TWO):
            back.scores(NONE, k)
        down.along_z()
        deep.middle()
        back.scores(ONE, NONE)
        back.scores(ONE, ONE)
        down.along_z()
        back.scores(TWO, NONE)
        back.scores(TWO, ONE)
        deep.second()
        down.along_z()
        back.scores(THREE, NONE)
        deep.middle()
        back.scores(THREE, ONE)
        deep.third()
        down.in_plane()
        back.end()
        att.pair()
        for a in adams.values():
            a.pack()

        def update(i):
            sums[i].gradient()
            adams[i].step(sums[i].mine, adams[i].new)
            out[i].start()

        att.first()
        deep.last()
        down.last()
        update("deep")
        update("down")
        out["deep"].along_z()
        out["down"].in_plane()
        att.middle()
        out["deep"].first()
        out["down"].along_z()
        att.second()
        out["deep"].middle()
        out["down"].along_z()
        att.middle()
        out["deep"].second()
        out["down"].along_z()
        att.third()
        out["deep"].last_middle()
        out["down"].along_z()
        att.last()
        update("att")
        out["att"].along_z()
        out["down"].along_z()
        out["deep"].end()
        for step in ("first", "middle", "second", "last_middle", "end"):
            getattr(out["att"], step)()
        for one in out.values():
            one.finish()
        copies.finish()
        writes.finish()
        assert copies.n == COPIES and len(writes.open) == WRITES, (copies.n, len(writes.open))

    vm, hbm = pl.BlockSpec(memory_space=pltpu.VMEM), pl.BlockSpec(memory_space=pl.ANY)
    order = lambda t: [t[name] for name in NAMES]
    sems = (COPIES, COPIES, 21, len(GIVEN) + 4, WRITES)
    return pl.pallas_call(
        kernel,
        out_shape=[jax.ShapeDtypeStruct((TWO, *SHAPES[i], LANES), BF16) for i in BATCHES]
        + [jax.ShapeDtypeStruct((TWO, TWO, b.own, LANES), F32) for b in BATCHES.values()],
        in_specs=[hbm] * (len(terms) + len(GIVEN) + THREE * len(NAMES)),
        out_specs=[hbm] * THREE + [vm] * THREE,
        scratch_shapes=[scratch[key] for key in keys] + [pltpu.SemaphoreType.DMA((n,)) for n in sems],
        compiler_params=pltpu.CompilerParams(collective_id=0, has_side_effects=True, vmem_limit_bytes=63 * 2**20),
    )(*terms, *(given[key] for key in GIVEN), *order(weights), *order(m), *order(v))


def lay_out(full, moments):
    names = list(BATCHES)

    def kernel(*refs):
        refs = list(refs)
        take = lambda n: [refs.pop(NONE) for _ in range(n)]
        given, packed = dict(zip(names, take(THREE))), dict(zip(names, take(THREE)))
        outs = dict(zip(NAMES, take(len(NAMES))))
        to = [dict(zip(NAMES, take(len(NAMES)))) for _ in range(TWO)]
        held = dict(zip(names, take(THREE)))
        in_sem, sem = refs
        writes = Writes(sem)
        reads = {}
        for n, (i, half) in enumerate((i, half) for half in range(TWO) for i in names):
            reads[i, half] = pltpu.make_async_copy(given[i].at[half], held[i].at[half], in_sem.at[n])
            reads[i, half].start()
        for (i, half), read in reads.items():
            read.wait()
            src = held[i]
            if i == "down":
                for t in range(THREE):
                    for z in range(Z):
                        writes.go(src.at[half, z, :, pl.ds(t * SIXTEEN, SIXTEEN), :],
                                  outs["w_down"].at[:, pl.ds(z * SIXTEEN, SIXTEEN), pl.ds((half * THREE + t) * LANES, LANES)])
            for name, tiles in DEEP:
                batch, h, first = SPOT[name]
                if BATCHES[i] is batch and h == half:
                    for t in range(tiles):
                        writes.go(src.at[half, :, pl.ds((first + t) * ROW3, ROW3), :], outs[name].at[:, :, pl.ds(t * LANES, LANES)])
        for k in range(TWO):
            for name, tiles in DEEP:
                batch, half, first = SPOT[name]
                src = packed["deep" if batch is MLP else "att"]
                for r in range(THREE):
                    for t in range(tiles):
                        at = r * batch.wide + first + t
                        to[k][name][r, :, t * LANES : (t + ONE) * LANES] = src[k, half, at : at + ONE, :]
            for t in range(SIX):
                half, n = divmod(t, THREE)
                to[k]["w_down"][:, t * LANES : (t + ONE) * LANES] = packed["down"][k, half, n * EIGHT : (n + ONE) * EIGHT, :]
        writes.finish()
        assert len(writes.open) == 94

    vm, hbm = pl.BlockSpec(memory_space=pltpu.VMEM), pl.BlockSpec(memory_space=pl.ANY)
    wide = {name: tiles * LANES for name, tiles in DEEP}
    weights = [jax.ShapeDtypeStruct((COLUMNS, ROW3, wide[n]) if n in wide else (COLUMNS, ROW8, D), BF16) for n in NAMES]
    moment = [jax.ShapeDtypeStruct((THREE, ONE, wide[n]) if n in wide else (EIGHT, D), F32) for n in NAMES]
    full = [t.reshape(TWO, COLUMNS, -1, LANES) if i != "down" else t for i, t in zip(names, full)]
    out = pl.pallas_call(
        kernel, out_shape=weights + moment + moment, in_specs=[hbm] * THREE + [vm] * THREE, out_specs=[hbm] * len(NAMES) + [vm] * (TWO * len(NAMES)),
        scratch_shapes=[pltpu.VMEM(t.shape, BF16) for t in full] + [pltpu.SemaphoreType.DMA((n,)) for n in (SIX, 94)],
        compiler_params=pltpu.CompilerParams(vmem_limit_bytes=63 * 2**20),
    )(*full, *moments)
    new = [t.reshape(ONE, -1, t.shape[-ONE]) for t in out[:7]]
    return new + [t[None] if n == "w_down" else t.transpose(1, 0, 2) for i in (7, 14) for n, t in zip(NAMES, out[i : i + 7])]


def solution(mesh):
    def step(x, dy, *arrays):
        weights, m, v = (dict(zip(NAMES, arrays[i : i + 7], strict=True)) for i in (0, 7, 14))
        weights = {name: w[0] for name, w in weights.items()}
        *terms, q, k, v_, o, a, dh, lse, cos, sin = run_forward(x[0], dy[0], weights)
        given = {"q": q, "k": k, "v": v_, "o": o, "a": a, "dh": dh, "lse": lse, "cos": cos, "sin": sin, "wo": weights["wo"]}
        thin = lambda t: {name: one[0] if name == "w_down" else one.transpose(1, 0, 2) for name, one in t.items()}
        terms = [t.reshape(N, N, MLP.rows, LANES) for t in terms[:2]] + terms[2:]
        out = exchange(terms, given, weights, thin(m), thin(v))
        return tuple(lay_out(out[:3], out[3:]))

    states, all_of, cut = P(("rep", "dp"), None, None), P(None, None, None), P(None, "dp", None)
    return jax.shard_map(
        step,
        mesh=mesh,
        in_specs=(states, states) + (all_of,) * 7 + (cut,) * 14,
        out_specs=(P("rep", None, None),) * 7 + (P("rep", "dp", None),) * 14,
        check_vma=False,
    )
```

```python
import jax
import jax.numpy as jnp
import numpy as np
from jax import lax
from jax.experimental import pallas as pl
from jax.experimental.pallas import tpu as pltpu
from jax.sharding import PartitionSpec as P

NAMES = ("wq", "wk", "wv", "wo", "w_gate", "w_up", "w_down")
F32, BF16 = jnp.float32, jnp.bfloat16
TOKENS, D, FF, HEAD, HEADS = 1024, 768, 2048, 128, 6
BLOCK = 256
BLOCKS = TOKENS // BLOCK
THETA = 10000
LOG2E = 1.4426950408889634
SCALE = HEAD**-0.5
POWER = SCALE * LOG2E
HIDDEN = -1e30
LANES, ROW3, ROW8 = 128, 48, 128
COLUMNS = 16


def dot(a, b, ca=1, cb=0):
    return lax.dot_general(a, b, (((ca,), (cb,)), ((), ())), preferred_element_type=F32)


def scale_of(wide):
    return lax.rsqrt(jnp.mean(wide * wide, -1, keepdims=True) + 1e-6)


def each(n, body):
    lax.fori_loop(0, n, lambda j, _: body(j), None)


def rope_tables(freq, near_s, far_s):
    place = lax.broadcasted_iota(jnp.int32, (32, LANES), 0).astype(F32)
    for ref, step in ((near_s, 1.0), (far_s, 32.0)):
        angle = place * step * freq
        ref[0] = jnp.cos(angle)
        ref[1] = jnp.sin(angle)


def rope_at(group, near_s, far_s):
    cn, sn, cf, sf = near_s[0], near_s[1], far_s[0, pl.ds(group, 1), :], far_s[1, pl.ds(group, 1), :]
    return cn * cf - sn * sf, sn * cf + cn * sf


def turn(t, cos, sin):
    return t * cos + pltpu.roll(t, HEAD // 2, 1) * sin


def forward(x_h, dy_h, wq_h, wk_h, wv_h, wo_h, wg_h, wu_h, wd_h, freq, deep_h, far_deep_h, flat_h, far_flat_h, q_h, k_h, v_h, o_h, a_h, dh_h, lse_h, cos_h, sin_h,
            x, dy, wq, wk, wv, wo, wg, wu, wd, deep, flat, q, k, v, o, a, dh, lse, cos_s, sin_s, near_s, far_s, vt, b, bt, act, d, in_sem, out_sem, sems):
    loads = [pltpu.make_async_copy(s, d, in_sem.at[n]) for n, (s, d) in enumerate(
        zip((x_h, wq_h, wk_h, wv_h, wo_h, wg_h, wu_h, wd_h, dy_h), (x, wq, wk, wv, wo, wg, wu, wd, dy)))]
    for load in loads:
        load.start()
    p = Place()
    greet([p.other])
    copies = Copies(sems)
    sends = []

    def send(src, dst):
        sends.append(pltpu.make_async_copy(src, dst, out_sem.at[len(sends)]))
        sends[-1].start()

    rope_tables(freq[...], near_s, far_s)
    minus = jnp.where(lax.broadcasted_iota(jnp.int32, (32, LANES), 1) < HEAD // 2, -1.0, 1.0)

    def places(i):
        cos, sin = rope_at(i, near_s, far_s)
        at = pl.ds(pl.multiple_of(i * 32, 32), 32)
        cos_s[at, :] = cos
        sin_s[at, :] = sin * minus
    each(TOKENS // 32, places)

    for load in loads[:4]:
        load.wait()

    def project(i):
        at = pl.ds(pl.multiple_of(i * BLOCK, BLOCK), BLOCK)
        wide = x[at, :].astype(F32)
        low = (wide * scale_of(wide)).astype(BF16)
        a[at, :] = low
        cos, sin = cos_s[at, :], sin_s[at, :]
        for h in range(HEADS):
            q[h, at, :] = turn(dot(low, wq[:, h * HEAD : (h + 1) * HEAD]).astype(BF16).astype(F32), cos, sin).astype(BF16)
        k[at, :] = turn(dot(low, wk[...]).astype(BF16).astype(F32), cos, sin).astype(BF16)
        v[at, :] = dot(low, wv[...]).astype(BF16)
    each(BLOCKS, project)
    vt[:HEAD, :] = v[...].T
    vt[HEAD:, :] = jnp.ones((8, TOKENS), BF16)
    send(a, a_h)
    send(q, q_h)
    send(k, k_h)
    send(v, v_h)
    send(cos_s, cos_h)
    send(sin_s, sin_h)

    seen = lax.broadcasted_iota(jnp.int32, (BLOCK, BLOCK), 0) <= lax.broadcasted_iota(jnp.int32, (BLOCK, BLOCK), 1)
    for i in range(BLOCKS):
        rows, past = slice(i * BLOCK, (i + 1) * BLOCK), i * BLOCK

        def heads(j):
            hs = [j * 3 + n for n in range(3)]
            diag = [jnp.where(seen, dot(k[rows, :], q[h, rows, :], 1, 1), HIDDEN) for h in hs]
            before = [dot(k[:past, :], q[h, rows, :], 1, 1) for h in hs] if i else []
            for n, h in enumerate(hs):
                top = diag[n].max(0, keepdims=True)
                if i:
                    top = jnp.maximum(top, before[n].max(0, keepdims=True))
                p = jnp.exp2((diag[n] - top) * POWER).astype(BF16)
                mix = dot(vt[:, rows], p)
                if i:
                    mix = mix + dot(vt[:, :past], jnp.exp2((before[n] - top) * POWER).astype(BF16))
                total = mix[HEAD : HEAD + 1, :]
                lse[h, :, rows] = top * POWER + jnp.log2(total)
                o[rows, pl.ds(pl.multiple_of(h * HEAD, HEAD), HEAD)] = (mix[:HEAD, :] * (1 / total)).T.astype(BF16)
        each(2, heads)
    send(o, o_h)
    send(lse, lse_h)

    for load in loads[4:]:
        load.wait()

    def rest(i):
        at = pl.ds(pl.multiple_of(i * BLOCK, BLOCK), BLOCK)
        h = (x[at, :].astype(F32) + dot(o[at, :], wo[...]).astype(BF16).astype(F32)).astype(BF16)
        wide = h.astype(F32)
        r = scale_of(wide)
        low = (wide * r).astype(BF16)
        b[at, :] = low
        d_out = dy[at, :]
        back = jnp.zeros((BLOCK, D), F32)
        for t in range(4):
            cols = slice(t * 512, (t + 1) * 512)
            gate, up = dot(low, wg[:, cols]), dot(low, wu[:, cols])
            d_act = dot(d_out, wd[cols, :], 1, 1).astype(BF16).astype(F32)
            sig = 1 / (1 + jnp.exp2(gate * -LOG2E))
            silu = gate * sig
            act[at, cols] = (silu * up).astype(BF16)
            d_gate = (d_act * up * (sig + silu * (1 - sig))).astype(BF16)
            d_up = (d_act * silu).astype(BF16)
            d[0, at, cols] = d_gate
            d[1, at, cols] = d_up
            back = back + dot(d_gate, wg[:, cols], 1, 1) + dot(d_up, wu[:, cols], 1, 1)
        back = back.astype(BF16).astype(F32)
        slope = (back * wide).sum(-1, keepdims=True) * (r * r * r * (1 / D))
        dh[at, :] = (d_out.astype(F32) + (back * r - wide * slope).astype(BF16).astype(F32)).astype(BF16)
    each(BLOCKS, rest)
    send(dh, dh_h)

    def down(i):
        cols = pl.ds(pl.multiple_of(i * 512, 512), 512)
        term = dot(act[:, cols], dy[...], 0, 0).astype(BF16)
        for t in range(6):
            tile = term[:, t * LANES : (t + 1) * LANES].reshape(4, Z, SIXTEEN, LANES)
            for z in range(Z):
                flat[t // 3, z, pl.ds(i * 4, 4), t % 3 * SIXTEEN : (t % 3 + 1) * SIXTEEN, :] = tile[:, z]

    each(4, down)
    copies.go(flat.at[p.o], far_flat_h, p.other)
    send(flat.at[p.c], flat_h)
    bt[...] = b[...].T

    def columns(half, i):
        term = dot(bt[...], d[half, :, pl.ds(pl.multiple_of(i * 512, 512), 512)]).astype(BF16)
        for t in range(4):
            deep[half, :, pl.ds(pl.multiple_of(i * 192 + t * ROW3, ROW3), ROW3), :] = term[:, t * LANES : (t + 1) * LANES].reshape(COLUMNS, ROW3, LANES)

    for part in range(TWO):
        rows = pl.ds(part * 384, 384)
        each(TWO, lambda i: columns(p.o, part * TWO + i))
        copies.go(deep.at[p.o, :, rows, :], far_deep_h.at[:, rows, :], p.other)
    for part in range(TWO):
        rows = pl.ds(part * 384, 384)
        each(TWO, lambda i: columns(p.c, part * TWO + i))
        send(deep.at[p.c, :, rows, :], deep_h.at[:, rows, :])
    for one in sends:
        one.wait()
    copies.finish(True)


def run_forward(x, dy, w):
    half = HEAD // 2
    freq = np.float32(THETA) ** (-np.arange(half, dtype=np.float32) / np.float32(half))
    freq = jnp.asarray(np.concatenate([freq, freq])[None])
    low = lambda *shape: (shape, BF16)
    blocks = low(COLUMNS, 768, LANES), low(Z, COLUMNS, ROW3, LANES)
    io = [low(HEADS, TOKENS, HEAD), low(TOKENS, HEAD), low(TOKENS, HEAD), low(TOKENS, D), low(TOKENS, D), low(TOKENS, D),
          ((HEADS, 1, TOKENS), F32), ((TOKENS, LANES), F32), ((TOKENS, LANES), F32)]
    outs = [one for one in blocks for _ in range(TWO)] + io
    two = [((TWO, *shape), kind) for shape, kind in blocks]
    tables = [((2, 32, LANES), F32)] * 2
    rest = [low(HEAD + 8, TOKENS), low(TOKENS, D), low(D, TOKENS), low(TOKENS, FF), low(TWO, TOKENS, FF)]
    given = [x, dy, *(w[n] for n in NAMES)]
    hbm = pl.BlockSpec(memory_space=pl.ANY)
    return pl.pallas_call(
        forward,
        out_shape=[jax.ShapeDtypeStruct(*one) for one in outs],
        in_specs=[hbm] * 9 + [pl.BlockSpec(memory_space=pltpu.VMEM)],
        out_specs=[hbm] * len(outs),
        scratch_shapes=[pltpu.VMEM(t.shape, BF16) for t in given] + [pltpu.VMEM(*one) for one in two + io + tables + rest]
        + [pltpu.SemaphoreType.DMA((n,)) for n in (9, 12, SIX)],
        compiler_params=pltpu.CompilerParams(collective_id=1, has_side_effects=True, vmem_limit_bytes=63 * 2**20),
    )(*given, freq)

N, Z = 4, 8


SIX, EIGHT, SIXTEEN = 6, 8, 16


class Batch:
    def __init__(self, deep, wide, flat, cuts):
        self.deep, self.wide, self.flat, self.cuts = deep, wide, flat, cuts
        self.rows = deep * ROW3 + flat * ROW8
        self.space = wide * ROW3 + flat * ROW8
        self.part = wide * SIX + flat * SIXTEEN
        self.own = self.part // TWO
        self.halves = pl.ds(NONE, sum(cuts[:TWO])), pl.ds(sum(cuts[:TWO]), sum(cuts[TWO:]))

    def at(self, q):
        return pl.ds(sum(self.cuts[:q]), self.cuts[q])

    def core_rows(self, core):
        deep = self.part - self.flat * SIXTEEN
        rows = [(slice(NONE, deep // TWO), slice(core * deep // TWO, (core + ONE) * deep // TWO))] if deep else []
        for t in range(self.flat):
            own, share = deep // TWO + t * EIGHT, deep + t * SIXTEEN + core * EIGHT
            rows.append((slice(own, own + EIGHT), slice(share, share + EIGHT)))
        return rows


NONE, ONE, TWO = range(3)
MLP = Batch(16, 16, 0, (192, 192, 192, 192))
ATT = Batch(7, 8, 0, (96, 96, 96, 48))
DOWN = Batch(0, 0, 3, ())
RIGHT_SLOT, STRAIGHT, JOINED = range(3)
Q0, Q1, Q2, Q3 = range(4)
THREE = 3


class Axis:
    def __init__(self, i, device):
        self.i, self.right, self.opposite, self.left = i, *(lax.rem(i + k, N) for k in range(ONE, N))
        self.to_right, self.to_left = device(self.right), device(self.left)


class Place:
    def __init__(self):
        me = lax.axis_index("dp")
        self.c = lax.rem(me, TWO)
        self.o = ONE - self.c
        self.z = lax.rem(lax.div(me, TWO), Z)
        self.y = lax.rem(lax.div(me, TWO * Z), N)
        self.x = lax.div(me, TWO * Z * N)
        self.other = self.at(c=self.o)
        self.along_x, self.along_y = Axis(self.x, lambda x: self.at(x=x)), Axis(self.y, lambda y: self.at(y=y))
        self.zs = [lax.rem(self.z + k, Z) for k in range(ONE, Z)]
        self.plane = [(lax.rem(self.x + k // N, N), lax.rem(self.y + k % N, N)) for k in range(ONE, N * N)]

    def everyone(self):
        return [self.other] + [self.at(z=z) for z in self.zs] + [self.at(x=x, y=y) for x, y in self.plane]

    def at(self, x=None, y=None, z=None, c=None):
        x, y, z, c = (mine if other is None else other for mine, other in ((self.x, x), (self.y, y), (self.z, z), (self.c, c)))
        return ((x * N + y) * Z + z) * TWO + c


class Copies:
    def __init__(self, sems):
        self.sems, self.n, self.open = sems, NONE, []

    def new(self):
        self.n += ONE
        return self.n - ONE

    def of(self, src, dst, device, send, recv):
        return pltpu.make_async_remote_copy(src_ref=src, dst_ref=dst, send_sem=self.sems.at[send], recv_sem=self.sems.at[recv],
                                            device_id={"dp": device}, device_id_type=pl.DeviceIdType.MESH)

    def go(self, src, dst, device, send=None, recv=None):
        copy = self.of(src, dst, device, self.new() if send is None else send, self.new() if recv is None else recv)
        copy.start()
        if send is None:
            self.open.append(copy)
        return copy

    def all_sent(self, sem, ref, device):
        self.open.append(self.of(ref, ref, device, sem, sem))

    def arrived(self, sem, ref, device):
        self.of(ref, ref, device, sem, sem).wait_recv()

    def finish(self, arrived=False):
        for copy in self.open:
            copy.wait_send()
            if arrived:
                copy.wait_recv()


def greet(others):
    barrier = pltpu.get_barrier_semaphore()
    for other in others:
        pl.semaphore_signal(barrier, device_id={"dp": other}, device_id_type=pl.DeviceIdType.MESH)
    pl.semaphore_wait(barrier, len(others))


class Ring:
    def __init__(self, copies, axis, inner, quarters, load, keep, out, got, ready=lambda k: None):
        self.__dict__.update(locals())
        self.sent, self.came = [copies.new() for _ in quarters], [copies.new() for _ in quarters]
        for sem, ref in zip(self.sent, out):
            copies.all_sent(sem, ref, axis.to_right)

    def put(self, n, slot, block, add=None):
        def one(j, _):
            term = self.load(block, j, self.quarters[n])
            self.out[n][slot, j] = (term if add is None else self.got[n][add, j].astype(F32) + term).astype(BF16)

        loop(self.inner, one)
        device = self.axis.to_right if (n == NONE) == (slot != STRAIGHT) else self.axis.to_left
        recv = None if slot == RIGHT_SLOT else self.came[n]
        return self.copies.go(self.out[n].at[slot], self.got[n].at[slot], device, self.sent[n], recv)

    def start(self):
        at = self.axis
        self.ready(NONE)
        self.far = [self.put(n, RIGHT_SLOT, at.opposite) for n in range(TWO)]
        self.ready(ONE)
        self.put(ONE, STRAIGHT, at.right)
        self.ready(TWO)
        self.put(NONE, STRAIGHT, at.left)

    def middle(self):
        for n, block in enumerate((self.axis.right, self.axis.left)):
            self.far[n].wait_recv()
            self.put(n, JOINED, block, RIGHT_SLOT)

    def end(self):
        self.ready(THREE)
        for n, q in enumerate(self.quarters):
            self.copies.arrived(self.came[n], self.got[n].at[pl.ds(STRAIGHT, TWO)], self.axis.to_right)

            def one(j, _):
                self.keep(q, j, self.load(self.axis.i, j, q) + self.got[n][STRAIGHT, j].astype(F32) + self.got[n][JOINED, j].astype(F32))

            loop(self.inner, one)


def loop(n, body):
    if n == ONE:
        body(NONE, None)
    else:
        lax.fori_loop(NONE, n, lambda j, _: body(j, None), None)


class Sum:
    def __init__(self, b, copies, p, g, own, bufs):
        self.b, self.copies, self.p, self.g, self.own, self.pairs = b, copies, p, g, own, []
        self.__dict__.update(bufs)

    def pair(self):
        p, b = self.p, self.b
        first, second = b.halves
        x, y = p.along_x, p.along_y
        sent = self.copies.new()
        self.copies.all_sent(sent, self.g.at[p.o], p.other)
        for i, j in ((x.opposite, y.opposite), (x.right, y.right), (x.left, y.left), (x.i, y.i)):
            self.pairs.append((self.copies.go(self.g.at[p.o, i, :, first, :], self.other.at[i, :, first, :], p.other, sent),
                               self.copies.go(self.g.at[p.o, :, j, second, :], self.other.at[:, j, second, :], p.other, sent)))

    def rings(self, inner, quarters, load, keep, prefix, ready):
        p, b = self.p, self.b
        made = []
        for which, axis, qs in zip(range(TWO), (p.along_x, p.along_y), quarters):
            out, got = ([getattr(self, f"{prefix}{kind}{q}") for q in qs] for kind in ("out", "in"))
            made.append(Ring(self.copies, axis, inner, qs, lambda i, j, q, which=which: load(which, i, j, b.at(q)), keep, out, got,
                             lambda k, which=which: ready(k, which)))
        return made

    def first(self):
        b = self.b

        def load(which, i, j, rows):
            x, y = (j, i) if which else (i, j)
            return self.own[x, y, rows, :].astype(F32) + self.other[x, y, rows, :].astype(F32)

        def keep(q, j, value):
            self.half[j, b.at(q), :] = value

        self.now = self.rings(N, ((Q0, Q1), (Q2, Q3)), load, keep, "", lambda k, which: self.pairs and self.pairs[k][which].wait_recv())
        for ring in self.now:
            ring.start()

    def middle(self):
        for ring in self.now:
            ring.middle()

    def second(self):
        b = self.b

        def keep(q, j, value):
            self.block[b.at(q), :] = value

        for ring in self.now:
            ring.end()
        self.now = self.rings(ONE, ((Q2, Q3), (Q0, Q1)), lambda which, i, j, rows: self.half[i, rows, :], keep, "s", lambda k, which: None)
        for ring in self.now:
            ring.start()

    def third(self):
        p, b = self.p, self.b
        if b.deep < b.wide:
            self.block[b.deep * ROW3 : b.wide * ROW3, :] = jnp.zeros(((b.wide - b.deep) * ROW3, LANES), F32)
        for ring in self.now:
            ring.end()
        for z in range(Z):
            for q in range(SIX):
                self.shares[z, q * b.wide : (q + ONE) * b.wide, :] = self.block[pl.ds(z * SIX + q, b.wide, stride=ROW3), :]
            self.low[z] = self.shares[z].astype(BF16)
        sent, self.came = self.copies.new(), self.copies.new()
        self.copies.all_sent(sent, self.got.at[pl.ds(NONE, Z - ONE)], p.other)
        for k, z in enumerate(p.zs):
            self.copies.go(self.low.at[z], self.got.at[k], p.at(z=z), sent, self.came)

    def last(self):
        p, b = self.p, self.b
        total = self.shares[p.z]
        self.copies.arrived(self.came, self.got.at[pl.ds(NONE, Z - ONE)], p.other)
        for k in range(Z - ONE):
            total = total + self.got[k].astype(F32)
        self.exchange_cores(total)

    def exchange_cores(self, total):
        p, b = self.p, self.b
        for core in range(TWO):
            for own, share in b.core_rows(core):
                self.swap[core, own, :] = total[share, :]
        self.fin = self.copies.go(self.swap.at[p.o], self.swapped, p.other)

    def gradient(self):
        p = self.p
        self.fin.wait_recv()
        self.mine[p.c] = self.swap[p.c]
        self.mine[p.o] = self.swapped[...]


def sum_buffers(b):
    low = lambda *shape: pltpu.VMEM((*shape, LANES), BF16)
    wide = lambda *shape: pltpu.VMEM((*shape, LANES), F32)
    o = {}
    for q, rows in enumerate(b.cuts):
        for kind in ("out", "in"):
            o[f"{kind}{q}"], o[f"s{kind}{q}"] = low(THREE, N, rows), low(THREE, ONE, rows)
    o |= {"other": low(N, N, b.rows), "half": wide(N, b.rows), "block": wide(b.space), "shares": wide(Z, b.part), "low": low(Z, b.part)}
    return o | {"got": low(Z, b.part), "swap": wide(TWO, b.own), "swapped": wide(b.own), "mine": wide(TWO, b.own)}


class Gather:
    def __init__(self, b, copies, p, new, full, result, write, bufs):
        self.b, self.copies, self.p, self.new, self.full, self.result, self.write = b, copies, p, new, full, result, write
        self.__dict__.update(bufs)

    def start(self):
        self.fin = self.copies.go(self.new.at[self.p.o], self.pal, self.p.other)

    def assemble(self):
        p, b = self.p, self.b
        self.fin.wait_recv()
        self.both[p.c] = self.new[p.c]
        self.both[p.o] = self.pal[...]
        for core in range(TWO):
            for own, share in b.core_rows(core):
                self.share[share, :] = self.both[core, own, :]

    def along_z(self):
        p = self.p
        self.assemble()
        self.wide_z[p.z] = self.share[...].astype(BF16)
        sent, self.came = self.copies.new(), self.copies.new()
        self.copies.all_sent(sent, self.wide_z.at[pl.ds(NONE, Z - ONE)], p.other)
        for z in p.zs:
            self.copies.go(self.wide_z.at[p.z], self.wide_z.at[p.z], p.at(z=z), sent, self.came)

    def first(self):
        p, b, full = self.p, self.b, self.full
        self.copies.arrived(self.came, self.wide_z.at[pl.ds(NONE, Z - ONE)], p.other)
        for z in range(Z):
            share = self.wide_z[z].astype(F32)
            for q in range(SIX):
                self.block[pl.ds(z * SIX + q, b.wide, stride=ROW3), :] = share[q * b.wide : (q + ONE) * b.wide, :]
        full[p.c, p.x, p.y] = self.block[: b.rows, :].astype(BF16)
        few = lambda n, rows: full.at[p.c, NONE, pl.ds(NONE, n), rows, :]
        self.now = [Spread(self.copies, p.along_y, lambda i, q: full.at[p.c, p.x, i, b.at(q), :], (Q0, Q1), lambda n: few(n, b.halves[NONE])),
                    Spread(self.copies, p.along_x, lambda i, q: full.at[p.c, i, p.y, b.at(q), :], (Q2, Q3), lambda n: few(n, b.halves[ONE]))]
        for one in self.now:
            one.start()

    def middle(self):
        for one in self.now:
            one.middle()

    def second(self):
        p, b, full = self.p, self.b, self.full
        for one in self.now:
            one.end()
        across = lambda i, q, core=p.c, of=full: of.at[core, i, :, b.at(q), :]
        along = lambda i, q, core=p.c, of=full: of.at[core, :, i, b.at(q), :]
        many = lambda n, rows: full.at[p.c, pl.ds(NONE, n), :, rows, :]
        self.now = [Spread(self.copies, p.along_x, across, (Q0, Q1), lambda n: many(n, b.halves[NONE])),
                    Spread(self.copies, p.along_y, along, (Q2, Q3), lambda n: many(n, b.halves[ONE]))]
        self.pass_all()
        self.group(ONE)
        for one in self.now:
            one.start()
        for one in self.now:
            for q in one.quarters:
                self.pass_on(one.ref, one.axis.i, q)

    def pass_all(self):
        self.groups, self.passed = [], self.copies.new()
        self.copies.all_sent(self.passed, self.full.at[self.p.c], self.p.other)

    def group(self, n):
        self.groups.append((self.copies.new(), self.full.at[self.p.c, pl.ds(NONE, n)], []))

    def pass_on(self, ref, i, q):
        piece = ref(i, q)
        sem, _, puts = self.groups[-ONE]
        self.copies.go(piece, piece, self.p.other, self.passed, sem)
        puts.append((ref, i, q))
        self.put(ref, i, q, self.p.c)

    def put(self, ref, i, q, core):
        pltpu.make_async_copy(ref(i, q, core), ref(i, q, core, self.result), self.write).start()

    def last_middle(self):
        for one in self.now:
            one.middle()
        self.group(ONE)
        for one in self.now:
            for i, q in zip((one.axis.left, one.axis.right), one.quarters):
                self.pass_on(one.ref, i, q)

    def end(self):
        self.group(TWO)
        for one in self.now:
            one.end()
            a, b = one.quarters
            for i, q in ((one.axis.left, b), (one.axis.right, a), (one.axis.opposite, a), (one.axis.opposite, b)):
                self.pass_on(one.ref, i, q)

    def finish(self):
        for sem, ref, puts in self.groups:
            self.copies.arrived(sem, ref, self.p.other)
            for piece in puts:
                self.put(*piece, self.p.o)
        pltpu.make_async_copy(self.full, self.result, self.write).wait()


class Spread:
    def __init__(self, copies, axis, ref, quarters, many):
        self.__dict__.update(locals())
        self.sent, self.came = copies.new(), copies.new()
        copies.all_sent(self.sent, many(THREE), axis.to_right)

    def send(self, i, q, device, recv=None):
        return self.copies.go(self.ref(i, q), self.ref(i, q), device, self.sent, recv)

    def start(self):
        at, (a, b) = self.axis, self.quarters
        self.turns = [self.send(at.i, a, at.to_right), self.send(at.i, b, at.to_left)]
        self.send(at.i, b, at.to_right, self.came)
        self.send(at.i, a, at.to_left, self.came)

    def middle(self):
        at = self.axis
        for turn, i, q, device in zip(self.turns, (at.left, at.right), self.quarters, (at.to_right, at.to_left)):
            turn.wait_recv()
            self.send(i, q, device, self.came)

    def end(self):
        self.copies.arrived(self.came, self.many(TWO), self.axis.to_right)


def gather_buffers(b):
    wide = lambda *shape: pltpu.VMEM((*shape, LANES), F32)
    o = {"pal": wide(b.own), "both": wide(TWO, b.own), "share": wide(b.part)}
    return o | ({"wide_z": pltpu.VMEM((Z, b.part, LANES), BF16)} if b.deep else {})


HALF = N * N // TWO


class Flow:
    def __init__(self, copies, p, sign, reach, half):
        self.copies, self.p, self.sign, self.reach, self.half = copies, p, sign, reach, half
        self.device = p.at(z=lax.rem(p.z + Z + sign, Z))
        self.n, self.last = NONE, None

    def z(self, steps):
        return lax.rem(self.p.z + Z + self.sign * steps, Z)


def flows(copies, p):
    return [Flow(copies, p, sign, reach, half) for sign, reaches in ((ONE, (4, 3)), (-ONE, (3, 4))) for half, reach in enumerate(reaches)]


class DownSum(Sum):
    def term(self, z, j):
        return self.own[z, j].astype(F32) + self.other[z, j].astype(F32)

    def along_z(self):
        if not hasattr(self, "flows"):
            self.flows = flows(self.copies, self.p)
            for flow, out in zip(self.flows, self.outs.values()):
                flow.sent = self.copies.new()
                self.copies.all_sent(flow.sent, out, flow.device)
        for f, (flow, out, got) in enumerate(zip(self.flows, self.outs.values(), self.gots.values())):
            n = flow.n
            if n == flow.reach:
                continue
            if flow.last:
                flow.last.wait_recv()
            z = flow.z(flow.reach - n)

            def one(j, _):
                term = self.term(z, flow.half * HALF + j)
                out[n, j] = (got[n - ONE, j].astype(F32) + term if n else term).astype(BF16)

            loop(HALF, one)
            flow.last = self.copies.go(out.at[n], got.at[n], flow.device, flow.sent)
            flow.n = n + ONE

    def in_plane(self):
        p = self.p
        for flow in self.flows:
            flow.last.wait_recv()
        for half in range(TWO):
            mine = [(flow.reach - ONE, got) for flow, got in zip(self.flows, self.gots.values()) if flow.half == half]

            def one(j, _):
                at = half * HALF + j
                total = self.term(p.z, at)
                for n, got in mine:
                    total = total + got[n, j].astype(F32)
                self.block[at] = total
                self.low[at] = total.astype(BF16)

            loop(HALF, one)
        sent, self.came = self.copies.new(), self.copies.new()
        self.copies.all_sent(sent, self.got.at[pl.ds(NONE, N * N - ONE)], p.other)
        for k, (x, y) in enumerate(p.plane):
            self.copies.go(self.low.at[x * N + y], self.got.at[k], p.at(x=x, y=y), sent, self.came)

    def last(self):
        p = self.p
        total = self.block[p.x * N + p.y]
        self.copies.arrived(self.came, self.got.at[pl.ds(NONE, N * N - ONE)], p.other)
        for k in range(N * N - ONE):
            total = total + self.got[k].astype(F32)
        self.exchange_cores(total)


class DownGather(Gather):
    def in_plane(self):
        p, b, full = self.p, self.b, self.full
        self.assemble()
        me = p.x * N + p.y
        full[p.c, p.z, me] = self.share[...].astype(BF16)
        ref = full.at[p.c, p.z, me]
        sent, self.came = self.copies.new(), self.copies.new()
        self.plane = full.at[p.c, NONE, pl.ds(NONE, N * N - ONE)]
        self.copies.all_sent(sent, self.plane, p.other)
        for x, y in p.plane:
            self.copies.go(ref, ref, p.at(x=x, y=y), sent, self.came)

    def ref(self, z, half, core=None, of=None):
        return (self.full if of is None else of).at[self.p.c if core is None else core, z, pl.ds(half * HALF, HALF)]

    def along_z(self):
        p = self.p
        if not hasattr(self, "flows"):
            self.copies.arrived(self.came, self.plane, p.other)
            self.flows, self.sent = flows(self.copies, p), self.copies.new()
            self.copies.all_sent(self.sent, self.full.at[p.c, pl.ds(NONE, Z - ONE)], p.other)
            self.pass_all()
            self.group(ONE)
            for half in range(TWO):
                self.pass_on(self.ref, p.z, half)
        if self.flows[NONE].n in (ONE, THREE):
            self.group({ONE: N, THREE: THREE}[self.flows[NONE].n])
        for flow in self.flows:
            if flow.last:
                flow.last.wait_recv()
                flow.last = None
                self.pass_on(self.ref, flow.z(-flow.n), flow.half)
            if flow.n < flow.reach:
                ref = self.ref(flow.z(-flow.n), flow.half)
                flow.last = self.copies.go(ref, ref, flow.device, self.sent)
                flow.n += ONE


def down_buffers():
    low = lambda *shape: pltpu.VMEM((*shape, LANES), BF16)
    wide = lambda *shape: pltpu.VMEM((*shape, LANES), F32)
    o = {"own": low(Z, N * N, ROW3), "other": low(Z, N * N, ROW3), "low": low(N * N, ROW3), "got": low(N * N, ROW3), "block": wide(N * N, ROW3)}
    for i, n in enumerate((4, 3, 3, 4)):
        o[f"outs.{i}"], o[f"gots.{i}"] = low(n, HALF, ROW3), low(n, HALF, ROW3)
    return o | {"swap": wide(TWO, DOWN.own), "swapped": wide(DOWN.own), "mine": wide(TWO, DOWN.own)}


DEEP = (("w_gate", 16), ("w_up", 16), ("wq", 6), ("wk", 1), ("wo", 6), ("wv", 1))
SPOT = {"w_gate": (MLP, 0, 0), "w_up": (MLP, 1, 0), "wq": (ATT, 0, 0), "wk": (ATT, 0, 6), "wo": (ATT, 1, 0), "wv": (ATT, 1, 6)}


class Adam:
    def __init__(self, b, p, w, m, v, moments, column32, bufs):
        self.b, self.p, self.w, self.m, self.v, self.moments, self.column32 = b, p, w, m, v, moments, column32
        self.__dict__.update(bufs)

    def fetch(self, sems, n):
        p, b = self.p, self.b
        column = p.x * N + p.y
        self.reads = []
        for name, (batch, _, _) in SPOT.items():
            if batch is b:
                self.reads.append(pltpu.make_async_copy(self.w[name].at[pl.ds(pl.multiple_of(column * 48, 48), 48), :], self.column[name], sems.at[n]))
                n += 1
        if b.flat:
            self.reads.append(pltpu.make_async_copy(self.w["w_down"].at[pl.ds(pl.multiple_of(column * 128, 128), 128), :], self.column["w_down"], sems.at[n]))
            n += 1
        for name, (batch, _, _) in SPOT.items():
            if batch is b:
                self.reads += [pltpu.make_async_copy(src[name], dst[name], sems.at[n + i]) for i, (src, dst) in enumerate(((self.m, self.m_in), (self.v, self.v_in)))]
                n += 2
        if b.flat:
            self.reads += [pltpu.make_async_copy(src["w_down"], dst["w_down"], sems.at[n + i]) for i, (src, dst) in enumerate(((self.m, self.m_in), (self.v, self.v_in)))]
            n += 2
        for read in self.reads:
            read.start()
        return n

    def pack(self):
        p, b = self.p, self.b
        for read in self.reads:
            read.wait()
        if b.deep < b.wide:
            for ref in (self.wp, self.mp, self.vp):
                ref[...] = jnp.zeros_like(ref)
        for name, tiles in DEEP:
            batch, half, first = SPOT[name]
            if batch is not b:
                continue
            wide = self.column32
            for t in range(tiles):
                wide[t * 48 : (t + 1) * 48, :] = self.column[name][:, t * 128 : (t + 1) * 128].astype(F32)
            for r in range(3):
                row = p.z * 6 + p.c * 3 + r
                self.wp[half, r * b.wide + first : r * b.wide + first + tiles, :] = wide[pl.ds(row, tiles, stride=48), :] if tiles > 1 else wide[pl.ds(row, 1), :]
                for t in range(tiles):
                    at = slice(r * b.wide + first + t, r * b.wide + first + t + 1)
                    cols = slice(t * 128, (t + 1) * 128)
                    self.mp[half, at, :] = self.m_in[name][r, :, cols]
                    self.vp[half, at, :] = self.v_in[name][r, :, cols]
        if b.flat:
            wide = self.column32
            for t in range(2 * b.flat):
                wide[t * ROW8 : (t + 1) * ROW8, :] = self.column["w_down"][:, t * LANES : (t + 1) * LANES].astype(F32)
            at = 3 * b.wide
            for t in range(2 * b.flat):
                half, rows, cols = t // b.flat, slice(at + t % b.flat * 8, at + t % b.flat * 8 + 8), slice(t * 128, (t + 1) * 128)
                self.wp[half, rows, :] = wide[pl.ds(pl.multiple_of(t * ROW8 + p.z * 16 + p.c * 8, 8), 8), :]
                self.mp[half, rows, :] = self.m_in["w_down"][:, cols]
                self.vp[half, rows, :] = self.v_in["w_down"][:, cols]

    def step(self, gradient, new):
        g = gradient[...].astype(BF16).astype(F32)
        m = 0.9 * self.mp[...] + 0.1 * g
        v = 0.95 * self.vp[...] + 0.05 * g * g
        w = self.wp[...]
        self.moments[0] = m
        self.moments[1] = v
        new[...] = (w - 0.02 * (m * lax.rsqrt(v + 1e-8) + 0.1 * w)).astype(BF16).astype(F32)


def adam_buffers(b):
    o = {k: pltpu.VMEM((2, b.own, 128), F32) for k in ("wp", "mp", "vp")}
    o["new"] = pltpu.VMEM((2, b.own, 128), F32)
    for name, tiles in DEEP:
        if SPOT[name][0] is b:
            o["column." + name] = pltpu.VMEM((48, tiles * 128), BF16)
            o["m_in." + name] = o["v_in." + name] = pltpu.VMEM((3, 1, tiles * 128), F32)
    if b.flat:
        o["column.w_down"] = pltpu.VMEM((128, 768), BF16)
        o["m_in.w_down"] = o["v_in.w_down"] = pltpu.VMEM((8, 768), F32)
    return o


def nest(flat):
    o = {}
    for key, ref in flat.items():
        if "." in key:
            a, b = key.split(".")
            o.setdefault(a, {})[b] = ref
        else:
            o[key] = ref
    return o


COPIES = 158


class Back:
    def __init__(self, bufs, g):
        self.__dict__.update(bufs)
        self.g = g

    def put(self, half, tile, term):
        at = tile * ROW3 if isinstance(tile, int) else pl.multiple_of(tile * ROW3, ROW3)
        self.g[half, :, pl.ds(at, ROW3), :] = term.astype(BF16).reshape(COLUMNS, ROW3, LANES)

    def start(self):
        self.kt[...] = self.k[...].T
        self.dk[...] = jnp.zeros_like(self.dk)
        self.dv[...] = jnp.zeros_like(self.dv)
        self.at[...] = self.o[...].T

    def out(self, part):
        cols = slice(part * D // TWO, (part + ONE) * D // TWO)
        do, term = dot(self.dh[...], self.wo[cols, :], 1, 1).astype(BF16), dot(self.at[...], self.dh[:, cols])
        for n in range(THREE):
            at = slice(n * HEAD, (n + ONE) * HEAD)
            self.do[part * THREE + n] = do[:, at]
            self.put(1, part * THREE + n, term[:, at])

    def turn_to_a(self):
        self.at[...] = self.a[...].T

    def scores(self, i, part, heads=3):
        rows, past = slice(i * BLOCK, (i + 1) * BLOCK), i * BLOCK
        seen = lax.broadcasted_iota(jnp.int32, (BLOCK, BLOCK), 0) <= lax.broadcasted_iota(jnp.int32, (BLOCK, BLOCK), 1)
        spans = ([slice(0, past)] if i else []) + [rows]
        ps, dss = [[] for _ in spans], [[] for _ in spans]
        hs = [part * heads + n for n in range(heads)]
        qs, dos = [self.q[h, rows, :] for h in hs], [self.do[h, rows, :] for h in hs]
        scores = [[dot(self.k[at, :], one, 1, 1) for at in spans] for one in qs]
        dps = [[dot(self.v[at, :], one, 1, 1) for at in spans] for one in dos]
        for n, h in enumerate(hs):
            p = [jnp.exp2(s * POWER - self.lse[h, :, rows]) for s in scores[n]]
            p[-1] = jnp.where(seen, p[-1], 0.0)
            delta = sum((one * dp).sum(0, keepdims=True) for one, dp in zip(p, dps[n]))
            ds = [(one * (dp - delta)).astype(BF16) for one, dp in zip(p, dps[n])]
            dq = sum(dot(self.kt[:, at], one) for at, one in zip(spans, ds))
            dq = (dq * SCALE).T.astype(BF16).astype(F32)
            self.o[rows, h * HEAD : (h + 1) * HEAD] = turn(dq, self.cos[rows, :], -self.sin[rows, :]).astype(BF16)
            for m, one in enumerate(p):
                ps[m].append(one.astype(BF16))
                dss[m].append(ds[m])
        do, q = jnp.concatenate(dos, 0), jnp.concatenate(qs, 0)
        for m, at in enumerate(spans):
            self.dv[at, :] += dot(jnp.concatenate(ps[m], 1), do)
            self.dk[at, :] += dot(jnp.concatenate(dss[m], 1), q)

    def end(self):
        dk = (self.dk[...] * SCALE).astype(BF16).astype(F32)
        both = dot(self.at[...], jnp.concatenate([turn(dk, self.cos[...], -self.sin[...]).astype(BF16), self.dv[...].astype(BF16)], 1))
        for half in range(TWO):
            self.put(half, HEADS, both[:, half * HEAD : (half + ONE) * HEAD])
        for part in range(TWO):
            term = dot(self.at[...], self.o[:, part * D // TWO : (part + ONE) * D // TWO])
            for n in range(THREE):
                self.put(NONE, part * THREE + n, term[:, n * HEAD : (n + ONE) * HEAD])


GIVEN = {"q": ((HEADS, TOKENS, HEAD), BF16), "k": ((TOKENS, HEAD), BF16), "v": ((TOKENS, HEAD), BF16), "o": ((TOKENS, D), BF16), "a": ((TOKENS, D), BF16),
         "dh": ((TOKENS, D), BF16), "lse": ((HEADS, 1, TOKENS), F32), "cos": ((TOKENS, LANES), F32), "sin": ((TOKENS, LANES), F32), "wo": ((D, D), BF16)}
MADE = {"kt": ((HEAD, TOKENS), BF16), "dk": ((TOKENS, HEAD), F32), "dv": ((TOKENS, HEAD), F32), "at": ((D, TOKENS), BF16),
        "do": ((HEADS, TOKENS, HEAD), BF16)}


BATCHES = {"deep": MLP, "down": DOWN, "att": ATT}
SHAPES = {"deep": (N, N, MLP.rows), "down": (Z, N * N, ROW3), "att": (N, N, ATT.rows)}


def exchange(terms, given, weights, m, v):
    scratch = {}
    for i, b in BATCHES.items():
        sums = sum_buffers(b) if b.deep else down_buffers()
        for kind, bufs in (("s", sums), ("g", gather_buffers(b)), ("a", adam_buffers(b)), ("full", {i: pltpu.VMEM((TWO, *SHAPES[i], LANES), BF16)})):
            for key, shape in bufs.items():
                scratch[(i, kind, key)] = shape
    for key, shape in (GIVEN | MADE).items():
        scratch[("att", "b", key)] = pltpu.VMEM(*shape)
    scratch[("deep", "s", "own")] = pltpu.VMEM((N, N, MLP.rows, LANES), BF16)
    scratch[("att", "terms", "")] = pltpu.VMEM((TWO, COLUMNS, ATT.rows, LANES), BF16)
    scratch[("all", "column", "")] = pltpu.VMEM((MLP.space, LANES), F32)
    keys = list(scratch)

    def kernel(*refs):
        refs = list(refs)
        take = lambda n: [refs.pop(NONE) for _ in range(n)]
        term = take(len(terms))
        from_hbm = dict(zip(GIVEN, take(len(GIVEN))))
        w, m_in, v_in = (dict(zip(NAMES, take(len(NAMES)))) for _ in range(THREE))
        result, moments = (dict(zip(BATCHES, take(len(BATCHES)))) for _ in range(TWO))
        bufs = dict(zip(keys, take(len(keys))))
        sems, reads, loads, out_sems = refs
        part = lambda i, kind: nest({key[TWO]: ref for key, ref in bufs.items() if key[:TWO] == (i, kind)})
        p = Place()
        copies = Copies(sems)
        ga = bufs[("att", "terms", "")]
        four = ga.reshape(TWO, N, N, ATT.rows, LANES)
        deep = Sum(MLP, copies, p, None, None, part("deep", "s"))
        down = DownSum(DOWN, copies, p, None, None, part("down", "s"))
        att = Sum(ATT, copies, p, four, four.at[p.c], part("att", "s"))
        sums = {"deep": deep, "down": down, "att": att}
        adams = {i: Adam(b, p, w, m_in, v_in, moments[i], bufs[("all", "column", "")], part(i, "a")) for i, b in BATCHES.items()}
        out = {}
        for n, (i, b) in enumerate(BATCHES.items()):
            block = {"block": bufs[(i, "s", "block")]} if b.deep else {}
            kind = Gather if b.deep else DownGather
            out[i] = kind(b, copies, p, adams[i].new, bufs[(i, "full", i)], result[i], out_sems.at[n], part(i, "g") | block)
        back = Back(part("att", "b"), ga)
        pairs = list(zip(term, (deep.own, deep.other, down.own, down.other))) + [(from_hbm[key], getattr(back, key)) for key in GIVEN]
        coming = [pltpu.make_async_copy(src, dst, loads.at[n]) for n, (src, dst) in enumerate(pairs)]
        for one in coming:
            one.start()
        n = NONE
        for a in adams.values():
            n = a.fetch(reads, n)
        greet(p.everyone())
        for one in coming[:TWO]:
            one.wait()
        deep.first()
        for one in coming[TWO:4]:
            one.wait()
        down.along_z()
        for one in coming[4:]:
            one.wait()
        back.start()
        back.out(NONE)
        back.out(ONE)
        down.along_z()
        back.turn_to_a()
        back.scores(NONE, NONE)
        back.scores(NONE, ONE)
        deep.middle()
        back.scores(ONE, NONE)
        back.scores(ONE, ONE)
        back.scores(TWO, NONE)
        down.along_z()
        back.scores(TWO, ONE)
        deep.second()
        back.scores(THREE, NONE)
        deep.middle()
        down.along_z()
        back.scores(THREE, ONE)
        back.end()
        att.pair()
        deep.third()
        down.in_plane()
        for a in adams.values():
            a.pack()

        def update(i):
            sums[i].gradient()
            adams[i].step(sums[i].mine, adams[i].new)
            out[i].start()

        att.first()
        down.last()
        deep.last()
        update("down")
        update("deep")
        out["down"].in_plane()
        att.middle()
        out["deep"].along_z()
        att.second()
        out["down"].along_z()
        att.middle()
        out["deep"].first()
        out["down"].along_z()
        att.third()
        out["deep"].middle()
        out["down"].along_z()
        out["deep"].second()
        att.last()
        out["down"].along_z()
        update("att")
        out["att"].along_z()
        out["deep"].last_middle()
        out["down"].along_z()
        out["att"].first()
        out["att"].middle()
        out["deep"].end()
        for step in ("second", "last_middle", "end"):
            getattr(out["att"], step)()
        for one in out.values():
            one.finish()
        copies.finish()
        assert copies.n == COPIES, copies.n

    vm, hbm = pl.BlockSpec(memory_space=pltpu.VMEM), pl.BlockSpec(memory_space=pl.ANY)
    order = lambda t: [t[name] for name in NAMES]
    sems = (COPIES, 21, len(GIVEN) + 4, THREE)
    return pl.pallas_call(
        kernel,
        out_shape=[jax.ShapeDtypeStruct((TWO, *SHAPES[i], LANES), BF16) for i in BATCHES]
        + [jax.ShapeDtypeStruct((TWO, TWO, b.own, LANES), F32) for b in BATCHES.values()],
        in_specs=[hbm] * (len(terms) + len(GIVEN) + THREE * len(NAMES)),
        out_specs=[hbm] * THREE + [vm] * THREE,
        scratch_shapes=[scratch[key] for key in keys] + [pltpu.SemaphoreType.DMA((n,)) for n in sems],
        compiler_params=pltpu.CompilerParams(collective_id=0, has_side_effects=True, vmem_limit_bytes=63 * 2**20),
    )(*terms, *(given[key] for key in GIVEN), *order(weights), *order(m), *order(v))


def lay_out(full, moments):
    names = list(BATCHES)

    def kernel(*refs):
        refs = list(refs)
        take = lambda n: [refs.pop(NONE) for _ in range(n)]
        given, packed = dict(zip(names, take(THREE))), dict(zip(names, take(THREE)))
        outs = dict(zip(NAMES, take(len(NAMES))))
        to = [dict(zip(NAMES, take(len(NAMES)))) for _ in range(TWO)]
        held = dict(zip(names, take(THREE)))
        in_sem, sem = refs

        def go(src, dst):
            pltpu.make_async_copy(src, dst, sem.at[names.index(i)]).start()

        reads = {}
        for n, (i, half) in enumerate((i, half) for half in range(TWO) for i in names):
            reads[i, half] = pltpu.make_async_copy(given[i].at[half], held[i].at[half], in_sem.at[n])
            reads[i, half].start()
        for (i, half), read in reads.items():
            read.wait()
            src = held[i]
            if i == "down":
                for t in range(THREE):
                    for z in range(Z):
                        go(src.at[half, z, :, pl.ds(t * SIXTEEN, SIXTEEN), :],
                           outs["w_down"].at[:, pl.ds(z * SIXTEEN, SIXTEEN), pl.ds((half * THREE + t) * LANES, LANES)])
            for name, tiles in DEEP:
                batch, h, first = SPOT[name]
                if BATCHES[i] is batch and h == half:
                    for t in range(tiles):
                        go(src.at[half, :, pl.ds((first + t) * ROW3, ROW3), :], outs[name].at[:, :, pl.ds(t * LANES, LANES)])
        for k in range(TWO):
            for name, tiles in DEEP:
                batch, half, first = SPOT[name]
                src = packed["deep" if batch is MLP else "att"]
                for r in range(THREE):
                    for t in range(tiles):
                        at = r * batch.wide + first + t
                        to[k][name][r, :, t * LANES : (t + ONE) * LANES] = src[k, half, at : at + ONE, :]
            for t in range(SIX):
                half, n = divmod(t, THREE)
                to[k]["w_down"][:, t * LANES : (t + ONE) * LANES] = packed["down"][k, half, n * EIGHT : (n + ONE) * EIGHT, :]
        for n, i in enumerate(names):
            pltpu.make_async_copy(held[i], held[i], sem.at[n]).wait()

    vm, hbm = pl.BlockSpec(memory_space=pltpu.VMEM), pl.BlockSpec(memory_space=pl.ANY)
    wide = {name: tiles * LANES for name, tiles in DEEP}
    weights = [jax.ShapeDtypeStruct((COLUMNS, ROW3, wide[n]) if n in wide else (COLUMNS, ROW8, D), BF16) for n in NAMES]
    moment = [jax.ShapeDtypeStruct((THREE, ONE, wide[n]) if n in wide else (EIGHT, D), F32) for n in NAMES]
    full = [t.reshape(TWO, COLUMNS, -1, LANES) if i != "down" else t for i, t in zip(names, full)]
    out = pl.pallas_call(
        kernel, out_shape=weights + moment + moment, in_specs=[hbm] * THREE + [vm] * THREE, out_specs=[hbm] * len(NAMES) + [vm] * (TWO * len(NAMES)),
        scratch_shapes=[pltpu.VMEM(t.shape, BF16) for t in full] + [pltpu.SemaphoreType.DMA((n,)) for n in (SIX, THREE)],
        compiler_params=pltpu.CompilerParams(vmem_limit_bytes=63 * 2**20),
    )(*full, *moments)
    new = [t.reshape(ONE, -1, t.shape[-ONE]) for t in out[:7]]
    return new + [t[None] if n == "w_down" else t.transpose(1, 0, 2) for i in (7, 14) for n, t in zip(NAMES, out[i : i + 7])]


def solution(mesh):
    def step(x, dy, *arrays):
        weights, m, v = (dict(zip(NAMES, arrays[i : i + 7], strict=True)) for i in (0, 7, 14))
        weights = {name: w[0] for name, w in weights.items()}
        *terms, q, k, v_, o, a, dh, lse, cos, sin = run_forward(x[0], dy[0], weights)
        given = {"q": q, "k": k, "v": v_, "o": o, "a": a, "dh": dh, "lse": lse, "cos": cos, "sin": sin, "wo": weights["wo"]}
        thin = lambda t: {name: one[0] if name == "w_down" else one.transpose(1, 0, 2) for name, one in t.items()}
        terms = [t.reshape(N, N, MLP.rows, LANES) for t in terms[:2]] + terms[2:]
        out = exchange(terms, given, weights, thin(m), thin(v))
        return tuple(lay_out(out[:3], out[3:]))

    states, all_of, cut = P(("rep", "dp"), None, None), P(None, None, None), P(None, "dp", None)
    return jax.shard_map(
        step,
        mesh=mesh,
        in_specs=(states, states) + (all_of,) * 7 + (cut,) * 14,
        out_specs=(P("rep", None, None),) * 7 + (P("rep", "dp", None),) * 14,
        check_vma=False,
    )
```

```python
import jax
import jax.numpy as jnp
import numpy as np
from jax import lax
from jax.experimental import pallas as pl
from jax.experimental.pallas import tpu as pltpu
from jax.sharding import PartitionSpec as P

NAMES = ("wq", "wk", "wv", "wo", "w_gate", "w_up", "w_down")
F32, BF16 = jnp.float32, jnp.bfloat16
TOKENS, D, FF, HEAD, HEADS = 1024, 768, 2048, 128, 6
BLOCK = 256
BLOCKS = TOKENS // BLOCK
THETA = 10000
LOG2E = 1.4426950408889634
SCALE = HEAD**-0.5
POWER = SCALE * LOG2E
HIDDEN = -1e30
LANES, ROW3, ROW8 = 128, 48, 128
COLUMNS = 16


def dot(a, b, ca=1, cb=0):
    return lax.dot_general(a, b, (((ca,), (cb,)), ((), ())), preferred_element_type=F32)


def scale_of(wide):
    return lax.rsqrt(jnp.mean(wide * wide, -1, keepdims=True) + 1e-6)


def each(n, body):
    lax.fori_loop(0, n, lambda j, _: body(j), None)


def rope_tables(freq, near_s, far_s):
    place = lax.broadcasted_iota(jnp.int32, (32, LANES), 0).astype(F32)
    for ref, step in ((near_s, 1.0), (far_s, 32.0)):
        angle = place * step * freq
        ref[0] = jnp.cos(angle)
        ref[1] = jnp.sin(angle)


def rope_at(group, near_s, far_s):
    cn, sn, cf, sf = near_s[0], near_s[1], far_s[0, pl.ds(group, 1), :], far_s[1, pl.ds(group, 1), :]
    return cn * cf - sn * sf, sn * cf + cn * sf


def turn(t, cos, sin):
    return t * cos + pltpu.roll(t, HEAD // 2, 1) * sin


def forward(x_h, dy_h, wq_h, wk_h, wv_h, wo_h, wg_h, wu_h, wd_h, freq, deep_h, far_deep_h, flat_h, far_flat_h, q_h, k_h, v_h, a_h, dh_h, lse_h, cos_h, sin_h,
            x, dy, wq, wk, wv, wo, wg, wu, wd, deep, flat, q, k, v, a, dh, lse, cos_s, sin_s, near_s, far_s, o, vt, b, bt, act, d, in_sem, out_sem, sems):
    loads = [pltpu.make_async_copy(s, d, in_sem.at[n]) for n, (s, d) in enumerate(
        zip((x_h, wq_h, wk_h, wv_h, wo_h, wg_h, wu_h, wd_h, dy_h), (x, wq, wk, wv, wo, wg, wu, wd, dy)))]
    for load in loads:
        load.start()
    p = Place()
    greet([p.other])
    copies = Copies(sems)
    sends = []

    def send(src, dst):
        sends.append(pltpu.make_async_copy(src, dst, out_sem.at[len(sends)]))
        sends[-1].start()

    rope_tables(freq[...], near_s, far_s)
    minus = jnp.where(lax.broadcasted_iota(jnp.int32, (32, LANES), 1) < HEAD // 2, -1.0, 1.0)

    def places(i):
        cos, sin = rope_at(i, near_s, far_s)
        at = pl.ds(pl.multiple_of(i * 32, 32), 32)
        cos_s[at, :] = cos
        sin_s[at, :] = sin * minus
    each(TOKENS // 32, places)

    for load in loads[:4]:
        load.wait()

    def project(i):
        at = pl.ds(pl.multiple_of(i * BLOCK, BLOCK), BLOCK)
        wide = x[at, :].astype(F32)
        low = (wide * scale_of(wide)).astype(BF16)
        a[at, :] = low
        cos, sin = cos_s[at, :], sin_s[at, :]
        for h in range(HEADS):
            q[h, at, :] = turn(dot(low, wq[:, h * HEAD : (h + 1) * HEAD]).astype(BF16).astype(F32), cos, sin).astype(BF16)
        k[at, :] = turn(dot(low, wk[...]).astype(BF16).astype(F32), cos, sin).astype(BF16)
        v[at, :] = dot(low, wv[...]).astype(BF16)
    each(BLOCKS, project)
    vt[:HEAD, :] = v[...].T
    vt[HEAD:, :] = jnp.ones((8, TOKENS), BF16)
    send(a, a_h)
    send(q, q_h)
    send(k, k_h)
    send(v, v_h)
    send(cos_s, cos_h)
    send(sin_s, sin_h)

    seen = lax.broadcasted_iota(jnp.int32, (BLOCK, BLOCK), 0) <= lax.broadcasted_iota(jnp.int32, (BLOCK, BLOCK), 1)
    for i in range(BLOCKS):
        rows, past = slice(i * BLOCK, (i + 1) * BLOCK), i * BLOCK

        def heads(j):
            hs = [j * 3 + n for n in range(3)]
            diag = [jnp.where(seen, dot(k[rows, :], q[h, rows, :], 1, 1), HIDDEN) for h in hs]
            before = [dot(k[:past, :], q[h, rows, :], 1, 1) for h in hs] if i else []
            for n, h in enumerate(hs):
                top = diag[n].max(0, keepdims=True)
                if i:
                    top = jnp.maximum(top, before[n].max(0, keepdims=True))
                p = jnp.exp2((diag[n] - top) * POWER).astype(BF16)
                mix = dot(vt[:, rows], p)
                if i:
                    mix = mix + dot(vt[:, :past], jnp.exp2((before[n] - top) * POWER).astype(BF16))
                total = mix[HEAD : HEAD + 1, :]
                lse[h, :, rows] = top * POWER + jnp.log2(total)
                o[rows, pl.ds(pl.multiple_of(h * HEAD, HEAD), HEAD)] = (mix[:HEAD, :] * (1 / total)).T.astype(BF16)
        each(2, heads)
    send(lse, lse_h)

    for load in loads[4:]:
        load.wait()

    def rest(i):
        at = pl.ds(pl.multiple_of(i * BLOCK, BLOCK), BLOCK)
        h = (x[at, :].astype(F32) + dot(o[at, :], wo[...]).astype(BF16).astype(F32)).astype(BF16)
        wide = h.astype(F32)
        r = scale_of(wide)
        low = (wide * r).astype(BF16)
        b[at, :] = low
        d_out = dy[at, :]
        back = jnp.zeros((BLOCK, D), F32)
        for t in range(4):
            cols = slice(t * 512, (t + 1) * 512)
            gate, up = dot(low, wg[:, cols]), dot(low, wu[:, cols])
            d_act = dot(d_out, wd[cols, :], 1, 1).astype(BF16).astype(F32)
            sig = 1 / (1 + jnp.exp2(gate * -LOG2E))
            silu = gate * sig
            act[at, cols] = (silu * up).astype(BF16)
            d_gate = (d_act * up * (sig + silu * (1 - sig))).astype(BF16)
            d_up = (d_act * silu).astype(BF16)
            d[0, at, cols] = d_gate
            d[1, at, cols] = d_up
            back = back + dot(d_gate, wg[:, cols], 1, 1) + dot(d_up, wu[:, cols], 1, 1)
        back = back.astype(BF16).astype(F32)
        slope = (back * wide).sum(-1, keepdims=True) * (r * r * r * (1 / D))
        dh[at, :] = (d_out.astype(F32) + (back * r - wide * slope).astype(BF16).astype(F32)).astype(BF16)
    each(BLOCKS, rest)
    send(dh, dh_h)

    def down(i):
        cols = pl.ds(pl.multiple_of(i * 512, 512), 512)
        term = dot(act[:, cols], dy[...], 0, 0).astype(BF16)
        for t in range(6):
            tile = term[:, t * LANES : (t + 1) * LANES].reshape(4, Z, SIXTEEN, LANES)
            for z in range(Z):
                flat[t // 3, z, pl.ds(i * 4, 4), t % 3 * SIXTEEN : (t % 3 + 1) * SIXTEEN, :] = tile[:, z]

    each(4, down)
    copies.go(flat.at[p.o], far_flat_h, p.other)
    send(flat.at[p.c], flat_h)
    bt[...] = o[...].T
    for half in range(TWO):
        term = dot(bt[...], dh[:, half * 384 : (half + 1) * 384]).astype(BF16)
        for t in range(THREE):
            deep[half, :, 768 + t * ROW3 : 768 + (t + 1) * ROW3, :] = term[:, t * LANES : (t + 1) * LANES].reshape(COLUMNS, ROW3, LANES)
    rows = pl.ds(768, THREE * ROW3)
    copies.go(deep.at[p.o, :, rows, :], far_deep_h.at[:, rows, :], p.other)
    send(deep.at[p.c, :, rows, :], deep_h.at[:, rows, :])
    bt[...] = b[...].T

    def columns(half, i):
        term = dot(bt[...], d[half, :, pl.ds(pl.multiple_of(i * 512, 512), 512)]).astype(BF16)
        for t in range(4):
            deep[half, :, pl.ds(pl.multiple_of(i * 192 + t * ROW3, ROW3), ROW3), :] = term[:, t * LANES : (t + 1) * LANES].reshape(COLUMNS, ROW3, LANES)

    for part in range(TWO):
        rows = pl.ds(part * 384, 384)
        each(TWO, lambda i: columns(p.o, part * TWO + i))
        copies.go(deep.at[p.o, :, rows, :], far_deep_h.at[:, rows, :], p.other)
    for part in range(TWO):
        rows = pl.ds(part * 384, 384)
        each(TWO, lambda i: columns(p.c, part * TWO + i))
        send(deep.at[p.c, :, rows, :], deep_h.at[:, rows, :])
    for one in sends:
        one.wait()
    copies.finish(True)


def run_forward(x, dy, w):
    half = HEAD // 2
    freq = np.float32(THETA) ** (-np.arange(half, dtype=np.float32) / np.float32(half))
    freq = jnp.asarray(np.concatenate([freq, freq])[None])
    low = lambda *shape: (shape, BF16)
    blocks = low(COLUMNS, MLP.rows, LANES), low(Z, COLUMNS, ROW3, LANES)
    io = [low(HEADS, TOKENS, HEAD), low(TOKENS, HEAD), low(TOKENS, HEAD), low(TOKENS, D), low(TOKENS, D),
          ((HEADS, 1, TOKENS), F32), ((TOKENS, LANES), F32), ((TOKENS, LANES), F32)]
    outs = [one for one in blocks for _ in range(TWO)] + io
    two = [((TWO, *shape), kind) for shape, kind in blocks]
    tables = [((2, 32, LANES), F32)] * 2
    rest = [low(TOKENS, D), low(HEAD + 8, TOKENS), low(TOKENS, D), low(D, TOKENS), low(TOKENS, FF), low(TWO, TOKENS, FF)]
    given = [x, dy, *(w[n] for n in NAMES)]
    hbm = pl.BlockSpec(memory_space=pl.ANY)
    return pl.pallas_call(
        forward,
        out_shape=[jax.ShapeDtypeStruct(*one) for one in outs],
        in_specs=[hbm] * 9 + [pl.BlockSpec(memory_space=pltpu.VMEM)],
        out_specs=[hbm] * len(outs),
        scratch_shapes=[pltpu.VMEM(t.shape, BF16) for t in given] + [pltpu.VMEM(*one) for one in two + io + tables + rest]
        + [pltpu.SemaphoreType.DMA((n,)) for n in (9, 12, EIGHT)],
        compiler_params=pltpu.CompilerParams(collective_id=1, has_side_effects=True, vmem_limit_bytes=63 * 2**20),
    )(*given, freq)

N, Z = 4, 8


SIX, EIGHT, SIXTEEN = 6, 8, 16


class Batch:
    def __init__(self, deep, wide, flat, cuts):
        self.deep, self.wide, self.flat, self.cuts = deep, wide, flat, cuts
        self.rows = deep * ROW3 + flat * ROW8
        self.space = wide * ROW3 + flat * ROW8
        self.part = wide * SIX + flat * SIXTEEN
        self.own = self.part // TWO
        self.halves = pl.ds(NONE, sum(cuts[:TWO])), pl.ds(sum(cuts[:TWO]), sum(cuts[TWO:]))

    def at(self, q):
        return pl.ds(sum(self.cuts[:q]), self.cuts[q])

    def core_rows(self, core):
        deep = self.part - self.flat * SIXTEEN
        rows = [(slice(NONE, deep // TWO), slice(core * deep // TWO, (core + ONE) * deep // TWO))] if deep else []
        for t in range(self.flat):
            own, share = deep // TWO + t * EIGHT, deep + t * SIXTEEN + core * EIGHT
            rows.append((slice(own, own + EIGHT), slice(share, share + EIGHT)))
        return rows


NONE, ONE, TWO = range(3)
MLP = Batch(19, 20, 0, (240, 240, 240, 192))
ATT = Batch(4, 8, 0, (48, 48, 48, 48))
DOWN = Batch(0, 0, 3, ())
RIGHT_SLOT, STRAIGHT, JOINED = range(3)
Q0, Q1, Q2, Q3 = range(4)
THREE = 3


class Axis:
    def __init__(self, i, device):
        self.i, self.right, self.opposite, self.left = i, *(lax.rem(i + k, N) for k in range(ONE, N))
        self.to_right, self.to_left = device(self.right), device(self.left)


class Place:
    def __init__(self):
        me = lax.axis_index("dp")
        self.c = lax.rem(me, TWO)
        self.o = ONE - self.c
        self.z = lax.rem(lax.div(me, TWO), Z)
        self.y = lax.rem(lax.div(me, TWO * Z), N)
        self.x = lax.div(me, TWO * Z * N)
        self.other = self.at(c=self.o)
        self.along_x, self.along_y = Axis(self.x, lambda x: self.at(x=x)), Axis(self.y, lambda y: self.at(y=y))
        self.zs = [lax.rem(self.z + k, Z) for k in range(ONE, Z)]
        self.plane = [(lax.rem(self.x + k // N, N), lax.rem(self.y + k % N, N)) for k in range(ONE, N * N)]

    def everyone(self):
        return [self.other] + [self.at(z=z) for z in self.zs] + [self.at(x=x, y=y) for x, y in self.plane]

    def at(self, x=None, y=None, z=None, c=None):
        x, y, z, c = (mine if other is None else other for mine, other in ((self.x, x), (self.y, y), (self.z, z), (self.c, c)))
        return ((x * N + y) * Z + z) * TWO + c


class Copies:
    def __init__(self, sems):
        self.sems, self.n, self.open = sems, NONE, []

    def new(self):
        self.n += ONE
        return self.n - ONE

    def of(self, src, dst, device, send, recv):
        return pltpu.make_async_remote_copy(src_ref=src, dst_ref=dst, send_sem=self.sems.at[send], recv_sem=self.sems.at[recv],
                                            device_id={"dp": device}, device_id_type=pl.DeviceIdType.MESH)

    def go(self, src, dst, device, send=None, recv=None):
        copy = self.of(src, dst, device, self.new() if send is None else send, self.new() if recv is None else recv)
        copy.start()
        if send is None:
            self.open.append(copy)
        return copy

    def all_sent(self, sem, ref, device):
        self.open.append(self.of(ref, ref, device, sem, sem))

    def arrived(self, sem, ref, device):
        self.of(ref, ref, device, sem, sem).wait_recv()

    def finish(self, arrived=False):
        for copy in self.open:
            copy.wait_send()
            if arrived:
                copy.wait_recv()


def greet(others):
    barrier = pltpu.get_barrier_semaphore()
    for other in others:
        pl.semaphore_signal(barrier, device_id={"dp": other}, device_id_type=pl.DeviceIdType.MESH)
    pl.semaphore_wait(barrier, len(others))


class Ring:
    def __init__(self, copies, axis, inner, quarters, load, keep, out, got, ready=lambda k: None):
        self.__dict__.update(locals())
        self.sent, self.came = [copies.new() for _ in quarters], [copies.new() for _ in quarters]
        for sem, ref in zip(self.sent, out):
            copies.all_sent(sem, ref, axis.to_right)

    def put(self, n, slot, block, add=None):
        def one(j, _):
            term = self.load(block, j, self.quarters[n])
            self.out[n][slot, j] = (term if add is None else self.got[n][add, j].astype(F32) + term).astype(BF16)

        loop(self.inner, one)
        device = self.axis.to_right if (n == NONE) == (slot != STRAIGHT) else self.axis.to_left
        recv = None if slot == RIGHT_SLOT else self.came[n]
        return self.copies.go(self.out[n].at[slot], self.got[n].at[slot], device, self.sent[n], recv)

    def start(self):
        at = self.axis
        self.ready(NONE)
        self.far = [self.put(n, RIGHT_SLOT, at.opposite) for n in range(TWO)]
        self.ready(ONE)
        self.put(ONE, STRAIGHT, at.right)
        self.ready(TWO)
        self.put(NONE, STRAIGHT, at.left)

    def middle(self):
        for n, block in enumerate((self.axis.right, self.axis.left)):
            self.far[n].wait_recv()
            self.put(n, JOINED, block, RIGHT_SLOT)

    def end(self):
        self.ready(THREE)
        for n, q in enumerate(self.quarters):
            self.copies.arrived(self.came[n], self.got[n].at[pl.ds(STRAIGHT, TWO)], self.axis.to_right)

            def one(j, _):
                self.keep(q, j, self.load(self.axis.i, j, q) + self.got[n][STRAIGHT, j].astype(F32) + self.got[n][JOINED, j].astype(F32))

            loop(self.inner, one)


def loop(n, body):
    if n == ONE:
        body(NONE, None)
    else:
        lax.fori_loop(NONE, n, lambda j, _: body(j, None), None)


class Sum:
    def __init__(self, b, copies, p, g, own, bufs):
        self.b, self.copies, self.p, self.g, self.own, self.pairs = b, copies, p, g, own, []
        self.__dict__.update(bufs)

    def pair(self):
        p, b = self.p, self.b
        first, second = b.halves
        x, y = p.along_x, p.along_y
        sent = self.copies.new()
        self.copies.all_sent(sent, self.g.at[p.o], p.other)
        for i, j in ((x.opposite, y.opposite), (x.right, y.right), (x.left, y.left), (x.i, y.i)):
            self.pairs.append((self.copies.go(self.g.at[p.o, i, :, first, :], self.other.at[i, :, first, :], p.other, sent),
                               self.copies.go(self.g.at[p.o, :, j, second, :], self.other.at[:, j, second, :], p.other, sent)))

    def rings(self, inner, quarters, load, keep, prefix, ready):
        p, b = self.p, self.b
        made = []
        for which, axis, qs in zip(range(TWO), (p.along_x, p.along_y), quarters):
            out, got = ([getattr(self, f"{prefix}{kind}{q}") for q in qs] for kind in ("out", "in"))
            made.append(Ring(self.copies, axis, inner, qs, lambda i, j, q, which=which: load(which, i, j, b.at(q)), keep, out, got,
                             lambda k, which=which: ready(k, which)))
        return made

    def first(self):
        b = self.b

        def load(which, i, j, rows):
            x, y = (j, i) if which else (i, j)
            return self.own[x, y, rows, :].astype(F32) + self.other[x, y, rows, :].astype(F32)

        def keep(q, j, value):
            self.half[j, b.at(q), :] = value

        self.now = self.rings(N, ((Q0, Q1), (Q2, Q3)), load, keep, "", lambda k, which: self.pairs and self.pairs[k][which].wait_recv())
        for ring in self.now:
            ring.start()

    def middle(self):
        for ring in self.now:
            ring.middle()

    def second(self):
        b = self.b

        def keep(q, j, value):
            self.block[b.at(q), :] = value

        for ring in self.now:
            ring.end()
        self.now = self.rings(ONE, ((Q2, Q3), (Q0, Q1)), lambda which, i, j, rows: self.half[i, rows, :], keep, "s", lambda k, which: None)
        for ring in self.now:
            ring.start()

    def third(self):
        p, b = self.p, self.b
        if b.deep < b.wide:
            self.block[b.deep * ROW3 : b.wide * ROW3, :] = jnp.zeros(((b.wide - b.deep) * ROW3, LANES), F32)
        for ring in self.now:
            ring.end()
        for z in range(Z):
            for q in range(SIX):
                self.shares[z, q * b.wide : (q + ONE) * b.wide, :] = self.block[pl.ds(z * SIX + q, b.wide, stride=ROW3), :]
            self.low[z] = self.shares[z].astype(BF16)
        sent, self.came = self.copies.new(), self.copies.new()
        self.copies.all_sent(sent, self.got.at[pl.ds(NONE, Z - ONE)], p.other)
        for k, z in enumerate(p.zs):
            self.copies.go(self.low.at[z], self.got.at[k], p.at(z=z), sent, self.came)

    def last(self):
        p, b = self.p, self.b
        total = self.shares[p.z]
        self.copies.arrived(self.came, self.got.at[pl.ds(NONE, Z - ONE)], p.other)
        for k in range(Z - ONE):
            total = total + self.got[k].astype(F32)
        self.exchange_cores(total)

    def exchange_cores(self, total):
        p, b = self.p, self.b
        for core in range(TWO):
            for own, share in b.core_rows(core):
                self.swap[core, own, :] = total[share, :]
        self.fin = self.copies.go(self.swap.at[p.o], self.swapped, p.other)

    def gradient(self):
        p = self.p
        self.fin.wait_recv()
        self.mine[p.c] = self.swap[p.c]
        self.mine[p.o] = self.swapped[...]


def sum_buffers(b):
    low = lambda *shape: pltpu.VMEM((*shape, LANES), BF16)
    wide = lambda *shape: pltpu.VMEM((*shape, LANES), F32)
    o = {}
    for q, rows in enumerate(b.cuts):
        for kind in ("out", "in"):
            o[f"{kind}{q}"], o[f"s{kind}{q}"] = low(THREE, N, rows), low(THREE, ONE, rows)
    o |= {"other": low(N, N, b.rows), "half": wide(N, b.rows), "block": wide(b.space), "shares": wide(Z, b.part), "low": low(Z, b.part)}
    return o | {"got": low(Z, b.part), "swap": wide(TWO, b.own), "swapped": wide(b.own), "mine": wide(TWO, b.own)}


class Gather:
    def __init__(self, b, copies, p, new, full, result, write, bufs):
        self.b, self.copies, self.p, self.new, self.full, self.result, self.write = b, copies, p, new, full, result, write
        self.__dict__.update(bufs)

    def start(self):
        self.fin = self.copies.go(self.new.at[self.p.o], self.pal, self.p.other)

    def assemble(self):
        p, b = self.p, self.b
        self.fin.wait_recv()
        self.both[p.c] = self.new[p.c]
        self.both[p.o] = self.pal[...]
        for core in range(TWO):
            for own, share in b.core_rows(core):
                self.share[share, :] = self.both[core, own, :]

    def along_z(self):
        p = self.p
        self.assemble()
        self.wide_z[p.z] = self.share[...].astype(BF16)
        sent, self.came = self.copies.new(), self.copies.new()
        self.copies.all_sent(sent, self.wide_z.at[pl.ds(NONE, Z - ONE)], p.other)
        for z in p.zs:
            self.copies.go(self.wide_z.at[p.z], self.wide_z.at[p.z], p.at(z=z), sent, self.came)

    def first(self):
        p, b, full = self.p, self.b, self.full
        self.copies.arrived(self.came, self.wide_z.at[pl.ds(NONE, Z - ONE)], p.other)
        for z in range(Z):
            share = self.wide_z[z].astype(F32)
            for q in range(SIX):
                self.block[pl.ds(z * SIX + q, b.wide, stride=ROW3), :] = share[q * b.wide : (q + ONE) * b.wide, :]
        full[p.x, p.y] = self.block[: b.rows, :].astype(BF16)
        few = lambda n, rows: full.at[NONE, pl.ds(NONE, n), rows, :]
        self.now = [Spread(self.copies, p.along_y, lambda i, q: full.at[p.x, i, b.at(q), :], (Q0, Q1), lambda n: few(n, b.halves[NONE])),
                    Spread(self.copies, p.along_x, lambda i, q: full.at[i, p.y, b.at(q), :], (Q2, Q3), lambda n: few(n, b.halves[ONE]))]
        for one in self.now:
            one.start()

    def middle(self):
        for one in self.now:
            one.middle()

    def second(self):
        p, b, full = self.p, self.b, self.full
        for one in self.now:
            one.end()
        across = lambda i, q, of=full: of.at[i, :, b.at(q), :]
        along = lambda i, q, of=full: of.at[:, i, b.at(q), :]
        many = lambda n, rows: full.at[pl.ds(NONE, n), :, rows, :]
        self.now = [Spread(self.copies, p.along_x, across, (Q0, Q1), lambda n: many(n, b.halves[NONE])),
                    Spread(self.copies, p.along_y, along, (Q2, Q3), lambda n: many(n, b.halves[ONE]))]
        self.pass_all()
        for one in self.now:
            one.start()
        for one in self.now:
            for q in one.quarters:
                self.pass_on(one.ref, one.axis.i, q)

    def pass_all(self):
        self.passed, self.came_over = self.copies.new(), self.copies.new()
        self.copies.all_sent(self.passed, self.full, self.p.other)

    def pass_on(self, ref, i, q):
        to = ref(i, q, self.result.at[self.p.c])
        self.copies.go(ref(i, q), to, self.p.other, self.passed, self.came_over)
        pltpu.make_async_copy(ref(i, q), to, self.write).start()

    def last_middle(self):
        for one in self.now:
            one.middle()
        for one in self.now:
            for i, q in zip((one.axis.left, one.axis.right), one.quarters):
                self.pass_on(one.ref, i, q)

    def end(self):
        for one in self.now:
            one.end()
            a, b = one.quarters
            for i, q in ((one.axis.left, b), (one.axis.right, a), (one.axis.opposite, a), (one.axis.opposite, b)):
                self.pass_on(one.ref, i, q)

    def finish(self):
        self.copies.arrived(self.came_over, self.full, self.p.other)
        pltpu.make_async_copy(self.full, self.result.at[self.p.c], self.write).wait()


class Spread:
    def __init__(self, copies, axis, ref, quarters, many):
        self.__dict__.update(locals())
        self.sent, self.came = copies.new(), copies.new()
        copies.all_sent(self.sent, many(THREE), axis.to_right)

    def send(self, i, q, device, recv=None):
        return self.copies.go(self.ref(i, q), self.ref(i, q), device, self.sent, recv)

    def start(self):
        at, (a, b) = self.axis, self.quarters
        self.turns = [self.send(at.i, a, at.to_right), self.send(at.i, b, at.to_left)]
        self.send(at.i, b, at.to_right, self.came)
        self.send(at.i, a, at.to_left, self.came)

    def middle(self):
        at = self.axis
        for turn, i, q, device in zip(self.turns, (at.left, at.right), self.quarters, (at.to_right, at.to_left)):
            turn.wait_recv()
            self.send(i, q, device, self.came)

    def end(self):
        self.copies.arrived(self.came, self.many(TWO), self.axis.to_right)


def gather_buffers(b):
    wide = lambda *shape: pltpu.VMEM((*shape, LANES), F32)
    o = {"pal": wide(b.own), "both": wide(TWO, b.own), "share": wide(b.part)}
    return o | ({"wide_z": pltpu.VMEM((Z, b.part, LANES), BF16)} if b.deep else {})


HALF = N * N // TWO


class Flow:
    def __init__(self, copies, p, sign, reach, half):
        self.copies, self.p, self.sign, self.reach, self.half = copies, p, sign, reach, half
        self.device = p.at(z=lax.rem(p.z + Z + sign, Z))
        self.n, self.last = NONE, None

    def z(self, steps):
        return lax.rem(self.p.z + Z + self.sign * steps, Z)


def flows(copies, p):
    return [Flow(copies, p, sign, reach, half) for sign, reaches in ((ONE, (4, 3)), (-ONE, (3, 4))) for half, reach in enumerate(reaches)]


class DownSum(Sum):
    def term(self, z, j):
        return self.own[z, j].astype(F32) + self.other[z, j].astype(F32)

    def along_z(self):
        if not hasattr(self, "flows"):
            self.flows = flows(self.copies, self.p)
            for flow, out in zip(self.flows, self.outs.values()):
                flow.sent = self.copies.new()
                self.copies.all_sent(flow.sent, out, flow.device)
        for f, (flow, out, got) in enumerate(zip(self.flows, self.outs.values(), self.gots.values())):
            n = flow.n
            if n == flow.reach:
                continue
            if flow.last:
                flow.last.wait_recv()
            z = flow.z(flow.reach - n)

            def one(j, _):
                term = self.term(z, flow.half * HALF + j)
                out[n, j] = (got[n - ONE, j].astype(F32) + term if n else term).astype(BF16)

            loop(HALF, one)
            flow.last = self.copies.go(out.at[n], got.at[n], flow.device, flow.sent)
            flow.n = n + ONE

    def in_plane(self):
        p = self.p
        for flow in self.flows:
            flow.last.wait_recv()
        for half in range(TWO):
            mine = [(flow.reach - ONE, got) for flow, got in zip(self.flows, self.gots.values()) if flow.half == half]

            def one(j, _):
                at = half * HALF + j
                total = self.term(p.z, at)
                for n, got in mine:
                    total = total + got[n, j].astype(F32)
                self.block[at] = total
                self.low[at] = total.astype(BF16)

            loop(HALF, one)
        sent, self.came = self.copies.new(), self.copies.new()
        self.copies.all_sent(sent, self.got.at[pl.ds(NONE, N * N - ONE)], p.other)
        for k, (x, y) in enumerate(p.plane):
            self.copies.go(self.low.at[x * N + y], self.got.at[k], p.at(x=x, y=y), sent, self.came)

    def last(self):
        p = self.p
        total = self.block[p.x * N + p.y]
        self.copies.arrived(self.came, self.got.at[pl.ds(NONE, N * N - ONE)], p.other)
        for k in range(N * N - ONE):
            total = total + self.got[k].astype(F32)
        self.exchange_cores(total)


class DownGather(Gather):
    def in_plane(self):
        p, b, full = self.p, self.b, self.full
        self.assemble()
        me = p.x * N + p.y
        full[p.z, me] = self.share[...].astype(BF16)
        ref = full.at[p.z, me]
        sent, self.came = self.copies.new(), self.copies.new()
        self.plane = full.at[NONE, pl.ds(NONE, N * N - ONE)]
        self.copies.all_sent(sent, self.plane, p.other)
        for x, y in p.plane:
            self.copies.go(ref, ref, p.at(x=x, y=y), sent, self.came)

    def ref(self, z, half, of=None):
        return (self.full if of is None else of).at[z, pl.ds(half * HALF, HALF)]

    def along_z(self):
        p = self.p
        if not hasattr(self, "flows"):
            self.copies.arrived(self.came, self.plane, p.other)
            self.flows, self.sent = flows(self.copies, p), self.copies.new()
            self.copies.all_sent(self.sent, self.full.at[pl.ds(NONE, Z - ONE)], p.other)
            self.pass_all()
            for half in range(TWO):
                self.pass_on(self.ref, p.z, half)
        for flow in self.flows:
            if flow.last:
                flow.last.wait_recv()
                flow.last = None
                self.pass_on(self.ref, flow.z(-flow.n), flow.half)
            if flow.n < flow.reach:
                ref = self.ref(flow.z(-flow.n), flow.half)
                flow.last = self.copies.go(ref, ref, flow.device, self.sent)
                flow.n += ONE


def down_buffers():
    low = lambda *shape: pltpu.VMEM((*shape, LANES), BF16)
    wide = lambda *shape: pltpu.VMEM((*shape, LANES), F32)
    o = {"own": low(Z, N * N, ROW3), "other": low(Z, N * N, ROW3), "low": low(N * N, ROW3), "got": low(N * N, ROW3), "block": wide(N * N, ROW3)}
    for i, n in enumerate((4, 3, 3, 4)):
        o[f"outs.{i}"], o[f"gots.{i}"] = low(n, HALF, ROW3), low(n, HALF, ROW3)
    return o | {"swap": wide(TWO, DOWN.own), "swapped": wide(DOWN.own), "mine": wide(TWO, DOWN.own)}


WIDTHS = {"w_gate": 16, "w_up": 16, "wo": 6, "wq": 6, "wk": 1, "wv": 1}
PIECES = (("w_gate", 0, 16, MLP, 0, 0), ("w_up", 0, 16, MLP, 1, 0), ("wo", 0, 3, MLP, 0, 16), ("wo", 3, 3, MLP, 1, 16),
          ("wq", 0, 4, ATT, 0, 0), ("wq", 4, 2, ATT, 1, 0), ("wk", 0, 1, ATT, 1, 2), ("wv", 0, 1, ATT, 1, 3))


def held_by(b):
    return dict.fromkeys(piece[0] for piece in PIECES if piece[3] is b)


class Adam:
    def __init__(self, b, p, w, m, v, moments, column32, bufs):
        self.b, self.p, self.w, self.m, self.v, self.moments, self.column32 = b, p, w, m, v, moments, column32
        self.__dict__.update(bufs)

    def fetch(self, sems, n):
        p, b = self.p, self.b
        column = p.x * N + p.y
        self.reads = []
        for name in held_by(b):
            self.reads.append(pltpu.make_async_copy(self.w[name].at[pl.ds(pl.multiple_of(column * ROW3, ROW3), ROW3), :], self.column[name], sems.at[n]))
            n += 1
        if b.flat:
            self.reads.append(pltpu.make_async_copy(self.w["w_down"].at[pl.ds(pl.multiple_of(column * 128, 128), 128), :], self.column["w_down"], sems.at[n]))
            n += 1
        for name in held_by(b):
            self.reads += [pltpu.make_async_copy(src[name], dst[name], sems.at[n + i]) for i, (src, dst) in enumerate(((self.m, self.m_in), (self.v, self.v_in)))]
            n += 2
        if b.flat:
            self.reads += [pltpu.make_async_copy(src["w_down"], dst["w_down"], sems.at[n + i]) for i, (src, dst) in enumerate(((self.m, self.m_in), (self.v, self.v_in)))]
            n += 2
        for read in self.reads:
            read.start()
        return n

    def pack(self):
        p, b = self.p, self.b
        for read in self.reads:
            read.wait()
        if b.deep < b.wide:
            for ref in (self.wp, self.mp, self.vp):
                ref[...] = jnp.zeros_like(ref)
        for name, start, tiles, batch, half, first in PIECES:
            if batch is not b:
                continue
            wide = self.column32
            for t in range(tiles):
                wide[t * ROW3 : (t + 1) * ROW3, :] = self.column[name][:, (start + t) * LANES : (start + t + 1) * LANES].astype(F32)
            for r in range(3):
                row = p.z * SIX + p.c * 3 + r
                to = r * b.wide + first
                self.wp[half, to : to + tiles, :] = wide[pl.ds(row, tiles, stride=ROW3), :] if tiles > 1 else wide[pl.ds(row, 1), :]
                for t in range(tiles):
                    at, cols = slice(to + t, to + t + 1), slice((start + t) * LANES, (start + t + 1) * LANES)
                    self.mp[half, at, :] = self.m_in[name][r, :, cols]
                    self.vp[half, at, :] = self.v_in[name][r, :, cols]
        if b.flat:
            wide = self.column32
            for t in range(2 * b.flat):
                wide[t * ROW8 : (t + 1) * ROW8, :] = self.column["w_down"][:, t * LANES : (t + 1) * LANES].astype(F32)
            at = 3 * b.wide
            for t in range(2 * b.flat):
                half, rows, cols = t // b.flat, slice(at + t % b.flat * 8, at + t % b.flat * 8 + 8), slice(t * 128, (t + 1) * 128)
                self.wp[half, rows, :] = wide[pl.ds(pl.multiple_of(t * ROW8 + p.z * 16 + p.c * 8, 8), 8), :]
                self.mp[half, rows, :] = self.m_in["w_down"][:, cols]
                self.vp[half, rows, :] = self.v_in["w_down"][:, cols]

    def step(self, gradient, new):
        g = gradient[...].astype(BF16).astype(F32)
        m = 0.9 * self.mp[...] + 0.1 * g
        v = 0.95 * self.vp[...] + 0.05 * g * g
        w = self.wp[...]
        self.moments[0] = m
        self.moments[1] = v
        new[...] = (w - 0.02 * (m * lax.rsqrt(v + 1e-8) + 0.1 * w)).astype(BF16).astype(F32)


def adam_buffers(b):
    o = {k: pltpu.VMEM((2, b.own, 128), F32) for k in ("wp", "mp", "vp")}
    o["new"] = pltpu.VMEM((2, b.own, 128), F32)
    for name in held_by(b):
        cols = WIDTHS[name] * LANES
        o["column." + name] = pltpu.VMEM((ROW3, cols), BF16)
        o["m_in." + name] = o["v_in." + name] = pltpu.VMEM((3, 1, cols), F32)
    if b.flat:
        o["column.w_down"] = pltpu.VMEM((128, 768), BF16)
        o["m_in.w_down"] = o["v_in.w_down"] = pltpu.VMEM((8, 768), F32)
    return o


def nest(flat):
    o = {}
    for key, ref in flat.items():
        if "." in key:
            a, b = key.split(".")
            o.setdefault(a, {})[b] = ref
        else:
            o[key] = ref
    return o


COPIES = 152


class Back:
    def __init__(self, bufs, g):
        self.__dict__.update(bufs)
        self.g = g

    def put(self, half, tile, term):
        self.g[half, :, pl.ds(tile * ROW3, ROW3), :] = term.astype(BF16).reshape(COLUMNS, ROW3, LANES)

    def start(self):
        self.kt[...] = self.k[...].T
        self.dk[...] = jnp.zeros_like(self.dk)
        self.dv[...] = jnp.zeros_like(self.dv)
        self.at[...] = self.a[...].T

    def out(self, part):
        do = dot(self.dh[...], self.wo[part * D // TWO : (part + ONE) * D // TWO, :], 1, 1).astype(BF16)
        for n in range(THREE):
            self.do[part * THREE + n] = do[:, n * HEAD : (n + ONE) * HEAD]

    def scores(self, i, part, heads=3):
        rows, past = slice(i * BLOCK, (i + 1) * BLOCK), i * BLOCK
        seen = lax.broadcasted_iota(jnp.int32, (BLOCK, BLOCK), 0) <= lax.broadcasted_iota(jnp.int32, (BLOCK, BLOCK), 1)
        spans = ([slice(0, past)] if i else []) + [rows]
        ps, dss = [[] for _ in spans], [[] for _ in spans]
        hs = [part * heads + n for n in range(heads)]
        qs, dos = [self.q[h, rows, :] for h in hs], [self.do[h, rows, :] for h in hs]
        scores = [[dot(self.k[at, :], one, 1, 1) for at in spans] for one in qs]
        dps = [[dot(self.v[at, :], one, 1, 1) for at in spans] for one in dos]
        for n, h in enumerate(hs):
            p = [jnp.exp2(s * POWER - self.lse[h, :, rows]) for s in scores[n]]
            p[-1] = jnp.where(seen, p[-1], 0.0)
            delta = sum((one * dp).sum(0, keepdims=True) for one, dp in zip(p, dps[n]))
            ds = [(one * (dp - delta)).astype(BF16) for one, dp in zip(p, dps[n])]
            dq = sum(dot(self.kt[:, at], one) for at, one in zip(spans, ds))
            dq = (dq * SCALE).T.astype(BF16).astype(F32)
            self.dq[rows, h * HEAD : (h + 1) * HEAD] = turn(dq, self.cos[rows, :], -self.sin[rows, :]).astype(BF16)
            for m, one in enumerate(p):
                ps[m].append(one.astype(BF16))
                dss[m].append(ds[m])
        do, q = jnp.concatenate(dos, 0), jnp.concatenate(qs, 0)
        for m, at in enumerate(spans):
            self.dv[at, :] += dot(jnp.concatenate(ps[m], 1), do)
            self.dk[at, :] += dot(jnp.concatenate(dss[m], 1), q)

    def end(self):
        dk = (self.dk[...] * SCALE).astype(BF16).astype(F32)
        both = dot(self.at[...], jnp.concatenate([turn(dk, self.cos[...], -self.sin[...]).astype(BF16), self.dv[...].astype(BF16)], 1))
        terms = {"wk": both, "wv": both[:, HEAD:]}
        for part in range(TWO):
            dq = dot(self.at[...], self.dq[:, part * D // TWO : (part + ONE) * D // TWO])
            terms |= {part * THREE + n: dq[:, n * HEAD :] for n in range(THREE)}
        for name, start, tiles, batch, half, first in PIECES:
            if batch is ATT:
                for t in range(tiles):
                    self.put(half, first + t, terms[start + t if name == "wq" else name][:, :HEAD])


GIVEN = {"q": ((HEADS, TOKENS, HEAD), BF16), "k": ((TOKENS, HEAD), BF16), "v": ((TOKENS, HEAD), BF16), "a": ((TOKENS, D), BF16),
         "dh": ((TOKENS, D), BF16), "lse": ((HEADS, 1, TOKENS), F32), "cos": ((TOKENS, LANES), F32), "sin": ((TOKENS, LANES), F32), "wo": ((D, D), BF16)}
MADE = {"kt": ((HEAD, TOKENS), BF16), "dk": ((TOKENS, HEAD), F32), "dv": ((TOKENS, HEAD), F32), "at": ((D, TOKENS), BF16),
        "do": ((HEADS, TOKENS, HEAD), BF16), "dq": ((TOKENS, D), BF16)}


BATCHES = {"deep": MLP, "down": DOWN, "att": ATT}
SHAPES = {"deep": (N, N, MLP.rows), "down": (Z, N * N, ROW3), "att": (N, N, ATT.rows)}


def exchange(terms, given, weights, m, v):
    scratch = {}
    for i, b in BATCHES.items():
        sums = sum_buffers(b) if b.deep else down_buffers()
        for kind, bufs in (("s", sums), ("g", gather_buffers(b)), ("a", adam_buffers(b)), ("full", {i: pltpu.VMEM((*SHAPES[i], LANES), BF16)})):
            for key, shape in bufs.items():
                scratch[(i, kind, key)] = shape
    for key, shape in (GIVEN | MADE).items():
        scratch[("att", "b", key)] = pltpu.VMEM(*shape)
    scratch[("deep", "s", "own")] = pltpu.VMEM((N, N, MLP.rows, LANES), BF16)
    scratch[("att", "terms", "")] = pltpu.VMEM((TWO, COLUMNS, ATT.rows, LANES), BF16)
    scratch[("all", "column", "")] = pltpu.VMEM((MLP.space, LANES), F32)
    keys = list(scratch)

    def kernel(*refs):
        refs = list(refs)
        take = lambda n: [refs.pop(NONE) for _ in range(n)]
        term = take(len(terms))
        from_hbm = dict(zip(GIVEN, take(len(GIVEN))))
        w, m_in, v_in = (dict(zip(NAMES, take(len(NAMES)))) for _ in range(THREE))
        result, moments = (dict(zip(BATCHES, take(len(BATCHES)))) for _ in range(TWO))
        bufs = dict(zip(keys, take(len(keys))))
        sems, reads, loads, out_sems = refs
        part = lambda i, kind: nest({key[TWO]: ref for key, ref in bufs.items() if key[:TWO] == (i, kind)})
        p = Place()
        copies = Copies(sems)
        ga = bufs[("att", "terms", "")]
        four = ga.reshape(TWO, N, N, ATT.rows, LANES)
        deep = Sum(MLP, copies, p, None, None, part("deep", "s"))
        down = DownSum(DOWN, copies, p, None, None, part("down", "s"))
        att = Sum(ATT, copies, p, four, four.at[p.c], part("att", "s"))
        sums = {"deep": deep, "down": down, "att": att}
        adams = {i: Adam(b, p, w, m_in, v_in, moments[i], bufs[("all", "column", "")], part(i, "a")) for i, b in BATCHES.items()}
        out = {}
        for n, (i, b) in enumerate(BATCHES.items()):
            block = {"block": bufs[(i, "s", "block")]} if b.deep else {}
            kind = Gather if b.deep else DownGather
            out[i] = kind(b, copies, p, adams[i].new, bufs[(i, "full", i)], result[i], out_sems.at[n], part(i, "g") | block)
        back = Back(part("att", "b"), ga)
        pairs = list(zip(term, (deep.own, deep.other, down.own, down.other))) + [(from_hbm[key], getattr(back, key)) for key in GIVEN]
        coming = [pltpu.make_async_copy(src, dst, loads.at[n]) for n, (src, dst) in enumerate(pairs)]
        for one in coming:
            one.start()
        n = NONE
        for a in adams.values():
            n = a.fetch(reads, n)
        greet(p.everyone())
        for one in coming[:TWO]:
            one.wait()
        deep.first()
        for one in coming[TWO:4]:
            one.wait()
        down.along_z()
        for one in coming[4:]:
            one.wait()
        back.start()
        back.out(NONE)
        back.out(ONE)
        back.scores(NONE, NONE)
        back.scores(NONE, ONE)
        down.along_z()
        deep.middle()
        back.scores(ONE, NONE)
        back.scores(ONE, ONE)
        back.scores(TWO, NONE)
        down.along_z()
        back.scores(TWO, ONE)
        deep.second()
        back.scores(THREE, NONE)
        down.along_z()
        deep.middle()
        back.scores(THREE, ONE)
        back.end()
        att.pair()
        deep.third()
        down.in_plane()
        for a in adams.values():
            a.pack()
        new_deep, new_down, new_att = out["deep"], out["down"], out["att"]
        att.first()
        att.middle()
        down.last()
        deep.last()
        for i in ("down", "deep"):
            sums[i].gradient()
            adams[i].step(sums[i].mine, adams[i].new)
            out[i].start()
        new_down.in_plane()
        new_deep.along_z()
        att.second()
        att.middle()
        new_down.along_z()
        att.third()
        new_deep.first()
        new_down.along_z()
        new_deep.middle()
        att.last()
        att.gradient()
        adams["att"].step(att.mine, adams["att"].new)
        new_att.start()
        new_att.along_z()
        new_deep.second()
        new_down.along_z()
        new_att.first()
        new_deep.last_middle()
        new_down.along_z()
        new_att.middle()
        new_att.second()
        new_down.along_z()
        new_deep.end()
        new_att.last_middle()
        new_att.end()
        for one in out.values():
            one.finish()
        copies.finish()
        assert copies.n == COPIES, copies.n

    vm, hbm = pl.BlockSpec(memory_space=pltpu.VMEM), pl.BlockSpec(memory_space=pl.ANY)
    order = lambda t: [t[name] for name in NAMES]
    sems = (COPIES, 21, len(GIVEN) + 4, THREE)
    return pl.pallas_call(
        kernel,
        out_shape=[jax.ShapeDtypeStruct((TWO, *SHAPES[i], LANES), BF16) for i in BATCHES]
        + [jax.ShapeDtypeStruct((TWO, TWO, b.own, LANES), F32) for b in BATCHES.values()],
        in_specs=[hbm] * (len(terms) + len(GIVEN) + THREE * len(NAMES)),
        out_specs=[hbm] * THREE + [vm] * THREE,
        scratch_shapes=[scratch[key] for key in keys] + [pltpu.SemaphoreType.DMA((n,)) for n in sems],
        compiler_params=pltpu.CompilerParams(collective_id=0, has_side_effects=True, vmem_limit_bytes=63 * 2**20),
    )(*terms, *(given[key] for key in GIVEN), *order(weights), *order(m), *order(v))


def lay_out(full, moments):
    names = list(BATCHES)

    def kernel(*refs):
        refs = list(refs)
        take = lambda n: [refs.pop(NONE) for _ in range(n)]
        given, packed = dict(zip(names, take(THREE))), dict(zip(names, take(THREE)))
        outs = dict(zip(NAMES, take(len(NAMES))))
        to = [dict(zip(NAMES, take(len(NAMES)))) for _ in range(TWO)]
        held = dict(zip(names, take(THREE)))
        in_sem, sem = refs

        def go(src, dst):
            pltpu.make_async_copy(src, dst, sem.at[names.index(i)]).start()

        reads = {}
        for n, (i, half) in enumerate((i, half) for half in range(TWO) for i in names):
            reads[i, half] = pltpu.make_async_copy(given[i].at[half], held[i].at[half], in_sem.at[n])
            reads[i, half].start()
        for (i, half), read in reads.items():
            read.wait()
            src = held[i]
            if i == "down":
                for t in range(THREE):
                    for z in range(Z):
                        go(src.at[half, z, :, pl.ds(t * SIXTEEN, SIXTEEN), :],
                           outs["w_down"].at[:, pl.ds(z * SIXTEEN, SIXTEEN), pl.ds((half * THREE + t) * LANES, LANES)])
            for name, start, tiles, batch, h, first in PIECES:
                if BATCHES[i] is batch and h == half:
                    for t in range(tiles):
                        go(src.at[half, :, pl.ds((first + t) * ROW3, ROW3), :], outs[name].at[:, :, pl.ds((start + t) * LANES, LANES)])
        for k in range(TWO):
            for name, start, tiles, batch, half, first in PIECES:
                src = packed["deep" if batch is MLP else "att"]
                for r in range(THREE):
                    for t in range(tiles):
                        at, cols = r * batch.wide + first + t, slice((start + t) * LANES, (start + t + ONE) * LANES)
                        to[k][name][r, :, cols] = src[k, half, at : at + ONE, :]
            for t in range(SIX):
                half, n = divmod(t, THREE)
                to[k]["w_down"][:, t * LANES : (t + ONE) * LANES] = packed["down"][k, half, n * EIGHT : (n + ONE) * EIGHT, :]
        for n, i in enumerate(names):
            pltpu.make_async_copy(held[i], held[i], sem.at[n]).wait()

    vm, hbm = pl.BlockSpec(memory_space=pltpu.VMEM), pl.BlockSpec(memory_space=pl.ANY)
    wide = {name: tiles * LANES for name, tiles in WIDTHS.items()}
    weights = [jax.ShapeDtypeStruct((COLUMNS, ROW3, wide[n]) if n in wide else (COLUMNS, ROW8, D), BF16) for n in NAMES]
    moment = [jax.ShapeDtypeStruct((THREE, ONE, wide[n]) if n in wide else (EIGHT, D), F32) for n in NAMES]
    full = [t.reshape(TWO, COLUMNS, -1, LANES) if i != "down" else t for i, t in zip(names, full)]
    out = pl.pallas_call(
        kernel, out_shape=weights + moment + moment, in_specs=[hbm] * THREE + [vm] * THREE, out_specs=[hbm] * len(NAMES) + [vm] * (TWO * len(NAMES)),
        scratch_shapes=[pltpu.VMEM(t.shape, BF16) for t in full] + [pltpu.SemaphoreType.DMA((n,)) for n in (SIX, THREE)],
        compiler_params=pltpu.CompilerParams(vmem_limit_bytes=63 * 2**20),
    )(*full, *moments)
    new = [t.reshape(ONE, -1, t.shape[-ONE]) for t in out[:7]]
    return new + [t[None] if n == "w_down" else t.transpose(1, 0, 2) for i in (7, 14) for n, t in zip(NAMES, out[i : i + 7])]


def solution(mesh):
    def step(x, dy, *arrays):
        weights, m, v = (dict(zip(NAMES, arrays[i : i + 7], strict=True)) for i in (0, 7, 14))
        weights = {name: w[0] for name, w in weights.items()}
        *terms, q, k, v_, a, dh, lse, cos, sin = run_forward(x[0], dy[0], weights)
        given = {"q": q, "k": k, "v": v_, "a": a, "dh": dh, "lse": lse, "cos": cos, "sin": sin, "wo": weights["wo"]}
        thin = lambda t: {name: one[0] if name == "w_down" else one.transpose(1, 0, 2) for name, one in t.items()}
        terms = [t.reshape(N, N, MLP.rows, LANES) for t in terms[:2]] + terms[2:]
        out = exchange(terms, given, weights, thin(m), thin(v))
        return tuple(lay_out(out[:3], out[3:]))

    states, all_of, cut = P(("rep", "dp"), None, None), P(None, None, None), P(None, "dp", None)
    return jax.shard_map(
        step,
        mesh=mesh,
        in_specs=(states, states) + (all_of,) * 7 + (cut,) * 14,
        out_specs=(P("rep", None, None),) * 7 + (P("rep", "dp", None),) * 14,
        check_vma=False,
    )
```

```python
import jax
import jax.numpy as jnp
import numpy as np
from jax import lax
from jax.experimental import pallas as pl
from jax.experimental.pallas import tpu as pltpu
from jax.sharding import PartitionSpec as P

NAMES = ("wq", "wk", "wv", "wo", "w_gate", "w_up", "w_down")
F32, BF16 = jnp.float32, jnp.bfloat16
TOKENS, D, FF, HEAD, HEADS = 1024, 768, 2048, 128, 6
BLOCK = 256
BLOCKS = TOKENS // BLOCK
THETA = 10000
LOG2E = 1.4426950408889634
SCALE = HEAD**-0.5
POWER = SCALE * LOG2E
HIDDEN = -1e30
LANES, ROW3, ROW8 = 128, 48, 128
COLUMNS = 16


def dot(a, b, ca=1, cb=0):
    return lax.dot_general(a, b, (((ca,), (cb,)), ((), ())), preferred_element_type=F32)


def scale_of(wide):
    return lax.rsqrt(jnp.mean(wide * wide, -1, keepdims=True) + 1e-6)


def each(n, body):
    lax.fori_loop(0, n, lambda j, _: body(j), None)


def rope_tables(freq, near_s, far_s):
    place = lax.broadcasted_iota(jnp.int32, (32, LANES), 0).astype(F32)
    for ref, step in ((near_s, 1.0), (far_s, 32.0)):
        angle = place * step * freq
        ref[0] = jnp.cos(angle)
        ref[1] = jnp.sin(angle)


def rope_at(group, near_s, far_s):
    cn, sn, cf, sf = near_s[0], near_s[1], far_s[0, pl.ds(group, 1), :], far_s[1, pl.ds(group, 1), :]
    return cn * cf - sn * sf, sn * cf + cn * sf


def turn(t, cos, sin):
    return t * cos + pltpu.roll(t, HEAD // 2, 1) * sin


def forward(x_h, dy_h, wq_h, wk_h, wv_h, wo_h, wg_h, wu_h, wd_h, freq, deep_h, far_deep_h, flat_h, far_flat_h, q_h, k_h, v_h, o_h, a_h, dh_h, lse_h, cos_h, sin_h,
            x, dy, wq, wk, wv, wo, wg, wu, wd, deep, flat, q, k, v, o, a, dh, lse, cos_s, sin_s, near_s, far_s, vt, b, bt, act, d, in_sem, out_sem, sems):
    loads = [pltpu.make_async_copy(s, d, in_sem.at[n]) for n, (s, d) in enumerate(
        zip((x_h, wq_h, wk_h, wv_h, wo_h, wg_h, wu_h, wd_h, dy_h), (x, wq, wk, wv, wo, wg, wu, wd, dy)))]
    for load in loads:
        load.start()
    p = Place()
    greet([p.other])
    copies = Copies(sems)
    sends = []

    def send(src, dst):
        sends.append(pltpu.make_async_copy(src, dst, out_sem.at[len(sends)]))
        sends[-1].start()

    rope_tables(freq[...], near_s, far_s)
    minus = jnp.where(lax.broadcasted_iota(jnp.int32, (32, LANES), 1) < HEAD // 2, -1.0, 1.0)

    def places(i):
        cos, sin = rope_at(i, near_s, far_s)
        at = pl.ds(pl.multiple_of(i * 32, 32), 32)
        cos_s[at, :] = cos
        sin_s[at, :] = sin * minus
    each(TOKENS // 32, places)

    for load in loads[:4]:
        load.wait()

    def project(i):
        at = pl.ds(pl.multiple_of(i * BLOCK, BLOCK), BLOCK)
        wide = x[at, :].astype(F32)
        low = (wide * scale_of(wide)).astype(BF16)
        a[at, :] = low
        cos, sin = cos_s[at, :], sin_s[at, :]
        for h in range(HEADS):
            q[h, at, :] = turn(dot(low, wq[:, h * HEAD : (h + 1) * HEAD]).astype(BF16).astype(F32), cos, sin).astype(BF16)
        k[at, :] = turn(dot(low, wk[...]).astype(BF16).astype(F32), cos, sin).astype(BF16)
        v[at, :] = dot(low, wv[...]).astype(BF16)
    each(BLOCKS, project)
    vt[:HEAD, :] = v[...].T
    vt[HEAD:, :] = jnp.ones((8, TOKENS), BF16)
    send(a, a_h)
    send(q, q_h)
    send(k, k_h)
    send(v, v_h)
    send(cos_s, cos_h)
    send(sin_s, sin_h)

    seen = lax.broadcasted_iota(jnp.int32, (BLOCK, BLOCK), 0) <= lax.broadcasted_iota(jnp.int32, (BLOCK, BLOCK), 1)
    for i in range(BLOCKS):
        rows, past = slice(i * BLOCK, (i + 1) * BLOCK), i * BLOCK

        def heads(j):
            hs = [j * 3 + n for n in range(3)]
            diag = [jnp.where(seen, dot(k[rows, :], q[h, rows, :], 1, 1), HIDDEN) for h in hs]
            before = [dot(k[:past, :], q[h, rows, :], 1, 1) for h in hs] if i else []
            for n, h in enumerate(hs):
                top = diag[n].max(0, keepdims=True)
                if i:
                    top = jnp.maximum(top, before[n].max(0, keepdims=True))
                p = jnp.exp2((diag[n] - top) * POWER).astype(BF16)
                mix = dot(vt[:, rows], p)
                if i:
                    mix = mix + dot(vt[:, :past], jnp.exp2((before[n] - top) * POWER).astype(BF16))
                total = mix[HEAD : HEAD + 1, :]
                lse[h, :, rows] = top * POWER + jnp.log2(total)
                o[rows, pl.ds(pl.multiple_of(h * HEAD, HEAD), HEAD)] = (mix[:HEAD, :] * (1 / total)).T.astype(BF16)
        each(2, heads)
    send(o, o_h)
    send(lse, lse_h)

    for load in loads[4:]:
        load.wait()

    def rest(i):
        at = pl.ds(pl.multiple_of(i * BLOCK, BLOCK), BLOCK)
        h = (x[at, :].astype(F32) + dot(o[at, :], wo[...]).astype(BF16).astype(F32)).astype(BF16)
        wide = h.astype(F32)
        r = scale_of(wide)
        low = (wide * r).astype(BF16)
        b[at, :] = low
        d_out = dy[at, :]
        back = jnp.zeros((BLOCK, D), F32)
        for t in range(4):
            cols = slice(t * 512, (t + 1) * 512)
            gate, up = dot(low, wg[:, cols]), dot(low, wu[:, cols])
            d_act = dot(d_out, wd[cols, :], 1, 1).astype(BF16).astype(F32)
            sig = 1 / (1 + jnp.exp2(gate * -LOG2E))
            silu = gate * sig
            act[at, cols] = (silu * up).astype(BF16)
            d_gate = (d_act * up * (sig + silu * (1 - sig))).astype(BF16)
            d_up = (d_act * silu).astype(BF16)
            d[0, at, cols] = d_gate
            d[1, at, cols] = d_up
            back = back + dot(d_gate, wg[:, cols], 1, 1) + dot(d_up, wu[:, cols], 1, 1)
        back = back.astype(BF16).astype(F32)
        slope = (back * wide).sum(-1, keepdims=True) * (r * r * r * (1 / D))
        dh[at, :] = (d_out.astype(F32) + (back * r - wide * slope).astype(BF16).astype(F32)).astype(BF16)
    each(BLOCKS, rest)
    send(dh, dh_h)

    def down(i):
        cols = pl.ds(pl.multiple_of(i * 512, 512), 512)
        term = dot(act[:, cols], dy[...], 0, 0).astype(BF16)
        for t in range(6):
            tile = term[:, t * LANES : (t + 1) * LANES].reshape(4, Z, SIXTEEN, LANES)
            for z in range(Z):
                flat[t // 3, z, pl.ds(i * 4, 4), t % 3 * SIXTEEN : (t % 3 + 1) * SIXTEEN, :] = tile[:, z]

    each(4, down)
    copies.go(flat.at[p.o], far_flat_h, p.other)
    send(flat.at[p.c], flat_h)
    bt[...] = b[...].T

    def columns(half, i):
        term = dot(bt[...], d[half, :, pl.ds(pl.multiple_of(i * 512, 512), 512)]).astype(BF16)
        for t in range(4):
            deep[half, :, pl.ds(pl.multiple_of(i * 192 + t * ROW3, ROW3), ROW3), :] = term[:, t * LANES : (t + 1) * LANES].reshape(COLUMNS, ROW3, LANES)

    for part in range(TWO):
        rows = pl.ds(part * 384, 384)
        each(TWO, lambda i: columns(p.o, part * TWO + i))
        copies.go(deep.at[p.o, :, rows, :], far_deep_h.at[:, rows, :], p.other)
    for part in range(TWO):
        rows = pl.ds(part * 384, 384)
        each(TWO, lambda i: columns(p.c, part * TWO + i))
        send(deep.at[p.c, :, rows, :], deep_h.at[:, rows, :])
    for one in sends:
        one.wait()
    copies.finish(True)


def run_forward(x, dy, w):
    half = HEAD // 2
    freq = np.float32(THETA) ** (-np.arange(half, dtype=np.float32) / np.float32(half))
    freq = jnp.asarray(np.concatenate([freq, freq])[None])
    low = lambda *shape: (shape, BF16)
    blocks = low(COLUMNS, 768, LANES), low(Z, COLUMNS, ROW3, LANES)
    io = [low(HEADS, TOKENS, HEAD), low(TOKENS, HEAD), low(TOKENS, HEAD), low(TOKENS, D), low(TOKENS, D), low(TOKENS, D),
          ((HEADS, 1, TOKENS), F32), ((TOKENS, LANES), F32), ((TOKENS, LANES), F32)]
    outs = [one for one in blocks for _ in range(TWO)] + io
    two = [((TWO, *shape), kind) for shape, kind in blocks]
    tables = [((2, 32, LANES), F32)] * 2
    rest = [low(HEAD + 8, TOKENS), low(TOKENS, D), low(D, TOKENS), low(TOKENS, FF), low(TWO, TOKENS, FF)]
    given = [x, dy, *(w[n] for n in NAMES)]
    hbm = pl.BlockSpec(memory_space=pl.ANY)
    return pl.pallas_call(
        forward,
        out_shape=[jax.ShapeDtypeStruct(*one) for one in outs],
        in_specs=[hbm] * 9 + [pl.BlockSpec(memory_space=pltpu.VMEM)],
        out_specs=[hbm] * len(outs),
        scratch_shapes=[pltpu.VMEM(t.shape, BF16) for t in given] + [pltpu.VMEM(*one) for one in two + io + tables + rest]
        + [pltpu.SemaphoreType.DMA((n,)) for n in (9, 12, SIX)],
        compiler_params=pltpu.CompilerParams(collective_id=1, has_side_effects=True, vmem_limit_bytes=63 * 2**20),
    )(*given, freq)

N, Z = 4, 8


SIX, EIGHT, SIXTEEN = 6, 8, 16


class Batch:
    def __init__(self, deep, wide, flat, cuts):
        self.deep, self.wide, self.flat, self.cuts = deep, wide, flat, cuts
        self.rows = deep * ROW3 + flat * ROW8
        self.space = wide * ROW3 + flat * ROW8
        self.part = wide * SIX + flat * SIXTEEN
        self.own = self.part // TWO
        self.halves = pl.ds(NONE, sum(cuts[:TWO])), pl.ds(sum(cuts[:TWO]), sum(cuts[TWO:]))

    def at(self, q):
        return pl.ds(sum(self.cuts[:q]), self.cuts[q])

    def core_rows(self, core):
        deep = self.part - self.flat * SIXTEEN
        rows = [(slice(NONE, deep // TWO), slice(core * deep // TWO, (core + ONE) * deep // TWO))] if deep else []
        for t in range(self.flat):
            own, share = deep // TWO + t * EIGHT, deep + t * SIXTEEN + core * EIGHT
            rows.append((slice(own, own + EIGHT), slice(share, share + EIGHT)))
        return rows


NONE, ONE, TWO = range(3)
MLP = Batch(16, 16, 0, (192, 192, 192, 192))
ATT = Batch(7, 8, 0, (96, 96, 96, 48))
DOWN = Batch(0, 0, 3, ())
RIGHT_SLOT, STRAIGHT, JOINED = range(3)
Q0, Q1, Q2, Q3 = range(4)
THREE = 3


class Axis:
    def __init__(self, i, device):
        self.i, self.right, self.opposite, self.left = i, *(lax.rem(i + k, N) for k in range(ONE, N))
        self.to_right, self.to_left = device(self.right), device(self.left)


class Place:
    def __init__(self):
        me = lax.axis_index("dp")
        self.c = lax.rem(me, TWO)
        self.o = ONE - self.c
        self.z = lax.rem(lax.div(me, TWO), Z)
        self.y = lax.rem(lax.div(me, TWO * Z), N)
        self.x = lax.div(me, TWO * Z * N)
        self.other = self.at(c=self.o)
        self.along_x, self.along_y = Axis(self.x, lambda x: self.at(x=x)), Axis(self.y, lambda y: self.at(y=y))
        self.zs = [lax.rem(self.z + k, Z) for k in range(ONE, Z)]
        self.plane = [(lax.rem(self.x + k // N, N), lax.rem(self.y + k % N, N)) for k in range(ONE, N * N)]

    def everyone(self):
        return [self.other] + [self.at(z=z) for z in self.zs] + [self.at(x=x, y=y) for x, y in self.plane]

    def at(self, x=None, y=None, z=None, c=None):
        x, y, z, c = (mine if other is None else other for mine, other in ((self.x, x), (self.y, y), (self.z, z), (self.c, c)))
        return ((x * N + y) * Z + z) * TWO + c


class Copies:
    def __init__(self, sems):
        self.sems, self.n, self.open = sems, NONE, []

    def new(self):
        self.n += ONE
        return self.n - ONE

    def of(self, src, dst, device, send, recv):
        return pltpu.make_async_remote_copy(src_ref=src, dst_ref=dst, send_sem=self.sems.at[send], recv_sem=self.sems.at[recv],
                                            device_id={"dp": device}, device_id_type=pl.DeviceIdType.MESH)

    def go(self, src, dst, device, send=None, recv=None):
        copy = self.of(src, dst, device, self.new() if send is None else send, self.new() if recv is None else recv)
        copy.start()
        if send is None:
            self.open.append(copy)
        return copy

    def all_sent(self, sem, ref, device):
        self.open.append(self.of(ref, ref, device, sem, sem))

    def arrived(self, sem, ref, device):
        self.of(ref, ref, device, sem, sem).wait_recv()

    def finish(self, arrived=False):
        for copy in self.open:
            copy.wait_send()
            if arrived:
                copy.wait_recv()


def greet(others):
    barrier = pltpu.get_barrier_semaphore()
    for other in others:
        pl.semaphore_signal(barrier, device_id={"dp": other}, device_id_type=pl.DeviceIdType.MESH)
    pl.semaphore_wait(barrier, len(others))


class Ring:
    def __init__(self, copies, axis, inner, quarters, load, keep, out, got, ready=lambda k: None):
        self.__dict__.update(locals())
        self.sent, self.came = [copies.new() for _ in quarters], [copies.new() for _ in quarters]
        for sem, ref in zip(self.sent, out):
            copies.all_sent(sem, ref, axis.to_right)

    def put(self, n, slot, block, add=None):
        def one(j, _):
            term = self.load(block, j, self.quarters[n])
            self.out[n][slot, j] = (term if add is None else self.got[n][add, j].astype(F32) + term).astype(BF16)

        loop(self.inner, one)
        device = self.axis.to_right if (n == NONE) == (slot != STRAIGHT) else self.axis.to_left
        recv = None if slot == RIGHT_SLOT else self.came[n]
        return self.copies.go(self.out[n].at[slot], self.got[n].at[slot], device, self.sent[n], recv)

    def start(self):
        at = self.axis
        self.ready(NONE)
        self.far = [self.put(n, RIGHT_SLOT, at.opposite) for n in range(TWO)]
        self.ready(ONE)
        self.put(ONE, STRAIGHT, at.right)
        self.ready(TWO)
        self.put(NONE, STRAIGHT, at.left)

    def middle(self):
        for n, block in enumerate((self.axis.right, self.axis.left)):
            self.far[n].wait_recv()
            self.put(n, JOINED, block, RIGHT_SLOT)

    def end(self):
        self.ready(THREE)
        for n, q in enumerate(self.quarters):
            self.copies.arrived(self.came[n], self.got[n].at[pl.ds(STRAIGHT, TWO)], self.axis.to_right)

            def one(j, _):
                self.keep(q, j, self.load(self.axis.i, j, q) + self.got[n][STRAIGHT, j].astype(F32) + self.got[n][JOINED, j].astype(F32))

            loop(self.inner, one)


def loop(n, body):
    if n == ONE:
        body(NONE, None)
    else:
        lax.fori_loop(NONE, n, lambda j, _: body(j, None), None)


class Sum:
    def __init__(self, b, copies, p, g, own, bufs):
        self.b, self.copies, self.p, self.g, self.own, self.pairs = b, copies, p, g, own, []
        self.__dict__.update(bufs)

    def pair(self):
        p, b = self.p, self.b
        first, second = b.halves
        x, y = p.along_x, p.along_y
        sent = self.copies.new()
        self.copies.all_sent(sent, self.g.at[p.o], p.other)
        for i, j in ((x.opposite, y.opposite), (x.right, y.right), (x.left, y.left), (x.i, y.i)):
            self.pairs.append((self.copies.go(self.g.at[p.o, i, :, first, :], self.other.at[i, :, first, :], p.other, sent),
                               self.copies.go(self.g.at[p.o, :, j, second, :], self.other.at[:, j, second, :], p.other, sent)))

    def rings(self, inner, quarters, load, keep, prefix, ready):
        p, b = self.p, self.b
        made = []
        for which, axis, qs in zip(range(TWO), (p.along_x, p.along_y), quarters):
            out, got = ([getattr(self, f"{prefix}{kind}{q}") for q in qs] for kind in ("out", "in"))
            made.append(Ring(self.copies, axis, inner, qs, lambda i, j, q, which=which: load(which, i, j, b.at(q)), keep, out, got,
                             lambda k, which=which: ready(k, which)))
        return made

    def first(self):
        b = self.b

        def load(which, i, j, rows):
            x, y = (j, i) if which else (i, j)
            return self.own[x, y, rows, :].astype(F32) + self.other[x, y, rows, :].astype(F32)

        def keep(q, j, value):
            self.half[j, b.at(q), :] = value

        self.now = self.rings(N, ((Q0, Q1), (Q2, Q3)), load, keep, "", lambda k, which: self.pairs and self.pairs[k][which].wait_recv())
        for ring in self.now:
            ring.start()

    def middle(self):
        for ring in self.now:
            ring.middle()

    def second(self):
        b = self.b

        def keep(q, j, value):
            self.block[b.at(q), :] = value

        for ring in self.now:
            ring.end()
        self.now = self.rings(ONE, ((Q2, Q3), (Q0, Q1)), lambda which, i, j, rows: self.half[i, rows, :], keep, "s", lambda k, which: None)
        for ring in self.now:
            ring.start()

    def third(self):
        p, b = self.p, self.b
        if b.deep < b.wide:
            self.block[b.deep * ROW3 : b.wide * ROW3, :] = jnp.zeros(((b.wide - b.deep) * ROW3, LANES), F32)
        for ring in self.now:
            ring.end()
        for z in range(Z):
            for q in range(SIX):
                self.shares[z, q * b.wide : (q + ONE) * b.wide, :] = self.block[pl.ds(z * SIX + q, b.wide, stride=ROW3), :]
            self.low[z] = self.shares[z].astype(BF16)
        sent, self.came = self.copies.new(), self.copies.new()
        self.copies.all_sent(sent, self.got.at[pl.ds(NONE, Z - ONE)], p.other)
        for k, z in enumerate(p.zs):
            self.copies.go(self.low.at[z], self.got.at[k], p.at(z=z), sent, self.came)

    def last(self):
        p, b = self.p, self.b
        total = self.shares[p.z]
        self.copies.arrived(self.came, self.got.at[pl.ds(NONE, Z - ONE)], p.other)
        for k in range(Z - ONE):
            total = total + self.got[k].astype(F32)
        self.exchange_cores(total)

    def exchange_cores(self, total):
        p, b = self.p, self.b
        for core in range(TWO):
            for own, share in b.core_rows(core):
                self.swap[core, own, :] = total[share, :]


def sum_buffers(b):
    low = lambda *shape: pltpu.VMEM((*shape, LANES), BF16)
    wide = lambda *shape: pltpu.VMEM((*shape, LANES), F32)
    o = {}
    for q, rows in enumerate(b.cuts):
        for kind in ("out", "in"):
            o[f"{kind}{q}"], o[f"s{kind}{q}"] = low(THREE, N, rows), low(THREE, ONE, rows)
    o |= {"other": low(N, N, b.rows), "half": wide(N, b.rows), "block": wide(b.space), "shares": wide(Z, b.part), "low": low(Z, b.part)}
    return o | {"got": low(Z, b.part), "swap": wide(TWO, b.own)}


class Gather:
    def __init__(self, b, copies, p, new, full, result, write, bufs):
        self.b, self.copies, self.p, self.new, self.full, self.result, self.write = b, copies, p, new, full, result, write
        self.__dict__.update(bufs)

    def assemble(self):
        p, b = self.p, self.b
        for core in range(TWO):
            for own, share in b.core_rows(core):
                self.share[share, :] = self.new[core, own, :]

    def along_z(self):
        p = self.p
        self.assemble()
        self.wide_z[p.z] = self.share[...].astype(BF16)
        sent, self.came = self.copies.new(), self.copies.new()
        self.copies.all_sent(sent, self.wide_z.at[pl.ds(NONE, Z - ONE)], p.other)
        for z in p.zs:
            self.copies.go(self.wide_z.at[p.z], self.wide_z.at[p.z], p.at(z=z), sent, self.came)

    def first(self):
        p, b, full = self.p, self.b, self.full
        self.copies.arrived(self.came, self.wide_z.at[pl.ds(NONE, Z - ONE)], p.other)
        for z in range(Z):
            share = self.wide_z[z].astype(F32)
            for q in range(SIX):
                self.block[pl.ds(z * SIX + q, b.wide, stride=ROW3), :] = share[q * b.wide : (q + ONE) * b.wide, :]
        full[p.x, p.y] = self.block[: b.rows, :].astype(BF16)
        few = lambda n, rows: full.at[NONE, pl.ds(NONE, n), rows, :]
        self.now = [Spread(self.copies, p.along_y, lambda i, q: full.at[p.x, i, b.at(q), :], (Q0, Q1), lambda n: few(n, b.halves[NONE])),
                    Spread(self.copies, p.along_x, lambda i, q: full.at[i, p.y, b.at(q), :], (Q2, Q3), lambda n: few(n, b.halves[ONE]))]
        for one in self.now:
            one.start()

    def middle(self):
        for one in self.now:
            one.middle()

    def second(self):
        p, b, full = self.p, self.b, self.full
        for one in self.now:
            one.end()
        across = lambda i, q, of=full: of.at[i, :, b.at(q), :]
        along = lambda i, q, of=full: of.at[:, i, b.at(q), :]
        many = lambda n, rows: full.at[pl.ds(NONE, n), :, rows, :]
        self.now = [Spread(self.copies, p.along_x, across, (Q0, Q1), lambda n: many(n, b.halves[NONE])),
                    Spread(self.copies, p.along_y, along, (Q2, Q3), lambda n: many(n, b.halves[ONE]))]
        self.pass_all()
        for one in self.now:
            one.start()
        for one in self.now:
            for q in one.quarters:
                self.pass_on(one.ref, one.axis.i, q)

    def pass_all(self):
        self.passed, self.came_over = self.copies.new(), self.copies.new()
        self.copies.all_sent(self.passed, self.full, self.p.other)

    def pass_on(self, ref, i, q):
        to = ref(i, q, self.result.at[self.p.c])
        self.copies.go(ref(i, q), to, self.p.other, self.passed, self.came_over)
        pltpu.make_async_copy(ref(i, q), to, self.write).start()

    def last_middle(self):
        for one in self.now:
            one.middle()
        for one in self.now:
            for i, q in zip((one.axis.left, one.axis.right), one.quarters):
                self.pass_on(one.ref, i, q)

    def end(self):
        for one in self.now:
            one.end()
            a, b = one.quarters
            for i, q in ((one.axis.left, b), (one.axis.right, a), (one.axis.opposite, a), (one.axis.opposite, b)):
                self.pass_on(one.ref, i, q)

    def finish(self):
        self.copies.arrived(self.came_over, self.full, self.p.other)
        pltpu.make_async_copy(self.full, self.result.at[self.p.c], self.write).wait()


class Spread:
    def __init__(self, copies, axis, ref, quarters, many):
        self.__dict__.update(locals())
        self.sent, self.came = copies.new(), copies.new()
        copies.all_sent(self.sent, many(THREE), axis.to_right)

    def send(self, i, q, device, recv=None):
        return self.copies.go(self.ref(i, q), self.ref(i, q), device, self.sent, recv)

    def start(self):
        at, (a, b) = self.axis, self.quarters
        self.turns = [self.send(at.i, a, at.to_right), self.send(at.i, b, at.to_left)]
        self.send(at.i, b, at.to_right, self.came)
        self.send(at.i, a, at.to_left, self.came)

    def middle(self):
        at = self.axis
        for turn, i, q, device in zip(self.turns, (at.left, at.right), self.quarters, (at.to_right, at.to_left)):
            turn.wait_recv()
            self.send(i, q, device, self.came)

    def end(self):
        self.copies.arrived(self.came, self.many(TWO), self.axis.to_right)


def gather_buffers(b):
    wide = lambda *shape: pltpu.VMEM((*shape, LANES), F32)
    o = {"share": wide(b.part)}
    return o | ({"wide_z": pltpu.VMEM((Z, b.part, LANES), BF16)} if b.deep else {})


HALF = N * N // TWO


class Flow:
    def __init__(self, copies, p, sign, reach, half):
        self.copies, self.p, self.sign, self.reach, self.half = copies, p, sign, reach, half
        self.device = p.at(z=lax.rem(p.z + Z + sign, Z))
        self.n, self.last = NONE, None

    def z(self, steps):
        return lax.rem(self.p.z + Z + self.sign * steps, Z)


def flows(copies, p):
    return [Flow(copies, p, sign, reach, half) for sign, reaches in ((ONE, (4, 3)), (-ONE, (3, 4))) for half, reach in enumerate(reaches)]


class DownSum(Sum):
    def term(self, z, j):
        return self.own[z, j].astype(F32) + self.other[z, j].astype(F32)

    def along_z(self):
        if not hasattr(self, "flows"):
            self.flows = flows(self.copies, self.p)
            for flow, out in zip(self.flows, self.outs.values()):
                flow.sent = self.copies.new()
                self.copies.all_sent(flow.sent, out, flow.device)
        for f, (flow, out, got) in enumerate(zip(self.flows, self.outs.values(), self.gots.values())):
            n = flow.n
            if n == flow.reach:
                continue
            if flow.last:
                flow.last.wait_recv()
            z = flow.z(flow.reach - n)

            def one(j, _):
                term = self.term(z, flow.half * HALF + j)
                out[n, j] = (got[n - ONE, j].astype(F32) + term if n else term).astype(BF16)

            loop(HALF, one)
            flow.last = self.copies.go(out.at[n], got.at[n], flow.device, flow.sent)
            flow.n = n + ONE

    def in_plane(self):
        p = self.p
        for flow in self.flows:
            flow.last.wait_recv()
        for half in range(TWO):
            mine = [(flow.reach - ONE, got) for flow, got in zip(self.flows, self.gots.values()) if flow.half == half]

            def one(j, _):
                at = half * HALF + j
                total = self.term(p.z, at)
                for n, got in mine:
                    total = total + got[n, j].astype(F32)
                self.block[at] = total
                self.low[at] = total.astype(BF16)

            loop(HALF, one)
        sent, self.came = self.copies.new(), self.copies.new()
        self.copies.all_sent(sent, self.got.at[pl.ds(NONE, N * N - ONE)], p.other)
        for k, (x, y) in enumerate(p.plane):
            self.copies.go(self.low.at[x * N + y], self.got.at[k], p.at(x=x, y=y), sent, self.came)

    def last(self):
        p = self.p
        total = self.block[p.x * N + p.y]
        self.copies.arrived(self.came, self.got.at[pl.ds(NONE, N * N - ONE)], p.other)
        for k in range(N * N - ONE):
            total = total + self.got[k].astype(F32)
        self.exchange_cores(total)


class DownGather(Gather):
    def in_plane(self):
        p, b, full = self.p, self.b, self.full
        self.assemble()
        me = p.x * N + p.y
        full[p.z, me] = self.share[...].astype(BF16)
        ref = full.at[p.z, me]
        sent, self.came = self.copies.new(), self.copies.new()
        self.plane = full.at[NONE, pl.ds(NONE, N * N - ONE)]
        self.copies.all_sent(sent, self.plane, p.other)
        for x, y in p.plane:
            self.copies.go(ref, ref, p.at(x=x, y=y), sent, self.came)

    def ref(self, z, half, of=None):
        return (self.full if of is None else of).at[z, pl.ds(half * HALF, HALF)]

    def along_z(self):
        p = self.p
        if not hasattr(self, "flows"):
            self.copies.arrived(self.came, self.plane, p.other)
            self.flows, self.sent = flows(self.copies, p), self.copies.new()
            self.copies.all_sent(self.sent, self.full.at[pl.ds(NONE, Z - ONE)], p.other)
            self.pass_all()
            for half in range(TWO):
                self.pass_on(self.ref, p.z, half)
        for flow in self.flows:
            if flow.last:
                flow.last.wait_recv()
                flow.last = None
                self.pass_on(self.ref, flow.z(-flow.n), flow.half)
            if flow.n < flow.reach:
                ref = self.ref(flow.z(-flow.n), flow.half)
                flow.last = self.copies.go(ref, ref, flow.device, self.sent)
                flow.n += ONE


def down_buffers():
    low = lambda *shape: pltpu.VMEM((*shape, LANES), BF16)
    wide = lambda *shape: pltpu.VMEM((*shape, LANES), F32)
    o = {"own": low(Z, N * N, ROW3), "other": low(Z, N * N, ROW3), "low": low(N * N, ROW3), "got": low(N * N, ROW3), "block": wide(N * N, ROW3)}
    for i, n in enumerate((4, 3, 3, 4)):
        o[f"outs.{i}"], o[f"gots.{i}"] = low(n, HALF, ROW3), low(n, HALF, ROW3)
    return o | {"swap": wide(TWO, DOWN.own)}


DEEP = (("w_gate", 16), ("w_up", 16), ("wq", 6), ("wk", 1), ("wo", 6), ("wv", 1))
SPOT = {"w_gate": (MLP, 0, 0), "w_up": (MLP, 1, 0), "wq": (ATT, 0, 0), "wk": (ATT, 0, 6), "wo": (ATT, 1, 0), "wv": (ATT, 1, 6)}


class Adam:
    def __init__(self, b, copies, p, w, m, v, moments, column32, bufs):
        self.copies = copies
        self.b, self.p, self.w, self.m, self.v, self.moments, self.column32 = b, p, w, m, v, moments, column32
        self.__dict__.update(bufs)

    def fetch(self, sems, n):
        p, b = self.p, self.b
        column = p.x * N + p.y
        self.reads = []
        for name, (batch, _, _) in SPOT.items():
            if batch is b:
                self.reads.append(pltpu.make_async_copy(self.w[name].at[pl.ds(pl.multiple_of(column * 48, 48), 48), :], self.column[name], sems.at[n]))
                n += 1
        if b.flat:
            self.reads.append(pltpu.make_async_copy(self.w["w_down"].at[pl.ds(pl.multiple_of(column * 128, 128), 128), :], self.column["w_down"], sems.at[n]))
            n += 1
        for name, (batch, _, _) in SPOT.items():
            if batch is b:
                self.reads += [pltpu.make_async_copy(src[name], dst[name], sems.at[n + i]) for i, (src, dst) in enumerate(((self.m, self.m_in), (self.v, self.v_in)))]
                n += 2
        if b.flat:
            self.reads += [pltpu.make_async_copy(src["w_down"], dst["w_down"], sems.at[n + i]) for i, (src, dst) in enumerate(((self.m, self.m_in), (self.v, self.v_in)))]
            n += 2
        for read in self.reads:
            read.start()
        return n

    def pack(self):
        p, b = self.p, self.b
        for read in self.reads:
            read.wait()
        if b.deep < b.wide:
            for ref in (self.wp, self.mv):
                ref[...] = jnp.zeros_like(ref)
        for name, tiles in DEEP:
            batch, half, first = SPOT[name]
            if batch is not b:
                continue
            wide = self.column32
            for t in range(tiles):
                wide[t * 48 : (t + 1) * 48, :] = self.column[name][:, t * 128 : (t + 1) * 128].astype(F32)
            for r in range(3):
                to = slice(r * b.wide + first, r * b.wide + first + tiles)
                for core in range(TWO):
                    row = p.z * SIX + core * 3 + r
                    self.wp[half, core, to, :] = wide[pl.ds(row, tiles, stride=ROW3), :] if tiles > 1 else wide[pl.ds(row, 1), :]
                for t in range(tiles):
                    at = slice(r * b.wide + first + t, r * b.wide + first + t + 1)
                    cols = slice(t * 128, (t + 1) * 128)
                    self.mv[half, NONE, at, :] = self.m_in[name][r, :, cols]
                    self.mv[half, ONE, at, :] = self.v_in[name][r, :, cols]
        if b.flat:
            wide = self.column32
            for t in range(2 * b.flat):
                wide[t * ROW8 : (t + 1) * ROW8, :] = self.column["w_down"][:, t * LANES : (t + 1) * LANES].astype(F32)
            at = 3 * b.wide
            for t in range(2 * b.flat):
                half, rows, cols = t // b.flat, slice(at + t % b.flat * 8, at + t % b.flat * 8 + 8), slice(t * 128, (t + 1) * 128)
                for core in range(TWO):
                    self.wp[half, core, rows, :] = wide[pl.ds(pl.multiple_of(t * ROW8 + p.z * SIXTEEN + core * EIGHT, EIGHT), EIGHT), :]
                self.mv[half, NONE, rows, :] = self.m_in["w_down"][:, cols]
                self.mv[half, ONE, rows, :] = self.v_in["w_down"][:, cols]

    def lend(self):
        self.lent = self.copies.go(self.mv.at[self.p.o], self.theirs, self.p.other)

    def step(self, gradient, new):
        p = self.p
        self.lent.wait_recv()
        for core, mv in ((p.c, self.mv.at[p.c]), (p.o, self.theirs)):
            g = gradient[core].astype(BF16).astype(F32)
            m = 0.9 * mv[NONE] + 0.1 * g
            v = 0.95 * mv[ONE] + 0.05 * g * g
            w = self.wp[p.c, core]
            self.done[core, NONE] = m
            self.done[core, ONE] = v
            new[core] = (w - 0.02 * (m * lax.rsqrt(v + 1e-8) + 0.1 * w)).astype(BF16).astype(F32)
        self.back = self.copies.go(self.done.at[p.o], self.returned, p.other)

    def finish(self):
        p = self.p
        self.back.wait_recv()
        for k in range(TWO):
            self.moments[k, p.c] = self.done[p.c, k]
            self.moments[k, p.o] = self.returned[k]


def adam_buffers(b):
    wide = lambda *shape: pltpu.VMEM((*shape, b.own, LANES), F32)
    o = {"wp": wide(TWO, TWO), "mv": wide(TWO, TWO), "theirs": wide(TWO), "done": wide(TWO, TWO), "returned": wide(TWO), "new": wide(TWO)}
    for name, tiles in DEEP:
        if SPOT[name][0] is b:
            o["column." + name] = pltpu.VMEM((48, tiles * 128), BF16)
            o["m_in." + name] = o["v_in." + name] = pltpu.VMEM((3, 1, tiles * 128), F32)
    if b.flat:
        o["column.w_down"] = pltpu.VMEM((128, 768), BF16)
        o["m_in.w_down"] = o["v_in.w_down"] = pltpu.VMEM((8, 768), F32)
    return o


def nest(flat):
    o = {}
    for key, ref in flat.items():
        if "." in key:
            a, b = key.split(".")
            o.setdefault(a, {})[b] = ref
        else:
            o[key] = ref
    return o


COPIES = 152


class Back:
    def __init__(self, bufs, g):
        self.__dict__.update(bufs)
        self.g = g

    def put(self, half, tile, term):
        at = tile * ROW3 if isinstance(tile, int) else pl.multiple_of(tile * ROW3, ROW3)
        self.g[half, :, pl.ds(at, ROW3), :] = term.astype(BF16).reshape(COLUMNS, ROW3, LANES)

    def start(self):
        self.kt[...] = self.k[...].T
        self.dk[...] = jnp.zeros_like(self.dk)
        self.dv[...] = jnp.zeros_like(self.dv)
        self.at[...] = self.o[...].T

    def out(self, part):
        cols = slice(part * D // TWO, (part + ONE) * D // TWO)
        do, term = dot(self.dh[...], self.wo[cols, :], 1, 1).astype(BF16), dot(self.at[...], self.dh[:, cols])
        for n in range(THREE):
            at = slice(n * HEAD, (n + ONE) * HEAD)
            self.do[part * THREE + n] = do[:, at]
            self.put(1, part * THREE + n, term[:, at])

    def turn_to_a(self):
        self.at[...] = self.a[...].T

    def scores(self, i, part, heads=3):
        rows, past = slice(i * BLOCK, (i + 1) * BLOCK), i * BLOCK
        seen = lax.broadcasted_iota(jnp.int32, (BLOCK, BLOCK), 0) <= lax.broadcasted_iota(jnp.int32, (BLOCK, BLOCK), 1)
        spans = ([slice(0, past)] if i else []) + [rows]
        ps, dss = [[] for _ in spans], [[] for _ in spans]
        hs = [part * heads + n for n in range(heads)]
        qs, dos = [self.q[h, rows, :] for h in hs], [self.do[h, rows, :] for h in hs]
        scores = [[dot(self.k[at, :], one, 1, 1) for at in spans] for one in qs]
        dps = [[dot(self.v[at, :], one, 1, 1) for at in spans] for one in dos]
        for n, h in enumerate(hs):
            p = [jnp.exp2(s * POWER - self.lse[h, :, rows]) for s in scores[n]]
            p[-1] = jnp.where(seen, p[-1], 0.0)
            delta = sum((one * dp).sum(0, keepdims=True) for one, dp in zip(p, dps[n]))
            ds = [(one * (dp - delta)).astype(BF16) for one, dp in zip(p, dps[n])]
            dq = sum(dot(self.kt[:, at], one) for at, one in zip(spans, ds))
            dq = (dq * SCALE).T.astype(BF16).astype(F32)
            self.o[rows, h * HEAD : (h + 1) * HEAD] = turn(dq, self.cos[rows, :], -self.sin[rows, :]).astype(BF16)
            for m, one in enumerate(p):
                ps[m].append(one.astype(BF16))
                dss[m].append(ds[m])
        do, q = jnp.concatenate(dos, 0), jnp.concatenate(qs, 0)
        for m, at in enumerate(spans):
            self.dv[at, :] += dot(jnp.concatenate(ps[m], 1), do)
            self.dk[at, :] += dot(jnp.concatenate(dss[m], 1), q)

    def end(self):
        dk = (self.dk[...] * SCALE).astype(BF16).astype(F32)
        both = dot(self.at[...], jnp.concatenate([turn(dk, self.cos[...], -self.sin[...]).astype(BF16), self.dv[...].astype(BF16)], 1))
        for half in range(TWO):
            self.put(half, HEADS, both[:, half * HEAD : (half + ONE) * HEAD])
        for part in range(TWO):
            term = dot(self.at[...], self.o[:, part * D // TWO : (part + ONE) * D // TWO])
            for n in range(THREE):
                self.put(NONE, part * THREE + n, term[:, n * HEAD : (n + ONE) * HEAD])


GIVEN = {"q": ((HEADS, TOKENS, HEAD), BF16), "k": ((TOKENS, HEAD), BF16), "v": ((TOKENS, HEAD), BF16), "o": ((TOKENS, D), BF16), "a": ((TOKENS, D), BF16),
         "dh": ((TOKENS, D), BF16), "lse": ((HEADS, 1, TOKENS), F32), "cos": ((TOKENS, LANES), F32), "sin": ((TOKENS, LANES), F32), "wo": ((D, D), BF16)}
MADE = {"kt": ((HEAD, TOKENS), BF16), "dk": ((TOKENS, HEAD), F32), "dv": ((TOKENS, HEAD), F32), "at": ((D, TOKENS), BF16),
        "do": ((HEADS, TOKENS, HEAD), BF16)}


BATCHES = {"deep": MLP, "down": DOWN, "att": ATT}
SHAPES = {"deep": (N, N, MLP.rows), "down": (Z, N * N, ROW3), "att": (N, N, ATT.rows)}


def exchange(terms, given, weights, m, v):
    scratch = {}
    for i, b in BATCHES.items():
        sums = sum_buffers(b) if b.deep else down_buffers()
        for kind, bufs in (("s", sums), ("g", gather_buffers(b)), ("a", adam_buffers(b)), ("full", {i: pltpu.VMEM((*SHAPES[i], LANES), BF16)})):
            for key, shape in bufs.items():
                scratch[(i, kind, key)] = shape
    for key, shape in (GIVEN | MADE).items():
        scratch[("att", "b", key)] = pltpu.VMEM(*shape)
    scratch[("deep", "s", "own")] = pltpu.VMEM((N, N, MLP.rows, LANES), BF16)
    scratch[("att", "terms", "")] = pltpu.VMEM((TWO, COLUMNS, ATT.rows, LANES), BF16)
    scratch[("all", "column", "")] = pltpu.VMEM((MLP.space, LANES), F32)
    keys = list(scratch)

    def kernel(*refs):
        refs = list(refs)
        take = lambda n: [refs.pop(NONE) for _ in range(n)]
        term = take(len(terms))
        from_hbm = dict(zip(GIVEN, take(len(GIVEN))))
        w, m_in, v_in = (dict(zip(NAMES, take(len(NAMES)))) for _ in range(THREE))
        result, moments = (dict(zip(BATCHES, take(len(BATCHES)))) for _ in range(TWO))
        bufs = dict(zip(keys, take(len(keys))))
        sems, reads, loads, out_sems = refs
        part = lambda i, kind: nest({key[TWO]: ref for key, ref in bufs.items() if key[:TWO] == (i, kind)})
        p = Place()
        copies = Copies(sems)
        ga = bufs[("att", "terms", "")]
        four = ga.reshape(TWO, N, N, ATT.rows, LANES)
        deep = Sum(MLP, copies, p, None, None, part("deep", "s"))
        down = DownSum(DOWN, copies, p, None, None, part("down", "s"))
        att = Sum(ATT, copies, p, four, four.at[p.c], part("att", "s"))
        sums = {"deep": deep, "down": down, "att": att}
        adams = {i: Adam(b, copies, p, w, m_in, v_in, moments[i], bufs[("all", "column", "")], part(i, "a")) for i, b in BATCHES.items()}
        out = {}
        for n, (i, b) in enumerate(BATCHES.items()):
            block = {"block": bufs[(i, "s", "block")]} if b.deep else {}
            kind = Gather if b.deep else DownGather
            out[i] = kind(b, copies, p, adams[i].new, bufs[(i, "full", i)], result[i], out_sems.at[n], part(i, "g") | block)
        back = Back(part("att", "b"), ga)
        pairs = list(zip(term, (deep.own, deep.other, down.own, down.other))) + [(from_hbm[key], getattr(back, key)) for key in GIVEN]
        coming = [pltpu.make_async_copy(src, dst, loads.at[n]) for n, (src, dst) in enumerate(pairs)]
        for one in coming:
            one.start()
        n = NONE
        for a in adams.values():
            n = a.fetch(reads, n)
        greet(p.everyone())
        for one in coming[:TWO]:
            one.wait()
        deep.first()
        for one in coming[TWO:4]:
            one.wait()
        down.along_z()
        for one in coming[4:]:
            one.wait()
        back.start()
        back.out(NONE)
        back.out(ONE)
        back.turn_to_a()
        back.scores(NONE, NONE)
        back.scores(NONE, ONE)
        down.along_z()
        deep.middle()
        back.scores(ONE, NONE)
        back.scores(ONE, ONE)
        back.scores(TWO, NONE)
        down.along_z()
        back.scores(TWO, ONE)
        deep.second()
        back.scores(THREE, NONE)
        down.along_z()
        deep.middle()
        back.scores(THREE, ONE)
        back.end()
        att.pair()
        deep.third()
        down.in_plane()
        for a in adams.values():
            a.pack()
            a.lend()
        new_deep, new_down, new_att = out["deep"], out["down"], out["att"]
        att.first()
        att.middle()
        down.last()
        deep.last()
        for i in ("down", "deep"):
            adams[i].step(sums[i].swap, adams[i].new)
        new_down.in_plane()
        new_deep.along_z()
        att.second()
        att.middle()
        new_down.along_z()
        att.third()
        new_deep.first()
        new_down.along_z()
        new_deep.middle()
        att.last()
        adams["att"].step(att.swap, adams["att"].new)
        new_att.along_z()
        new_deep.second()
        new_down.along_z()
        new_att.first()
        new_deep.last_middle()
        new_down.along_z()
        new_att.middle()
        new_att.second()
        new_down.along_z()
        new_deep.end()
        new_att.last_middle()
        new_att.end()
        for a in adams.values():
            a.finish()
        for one in out.values():
            one.finish()
        copies.finish()
        assert copies.n == COPIES, copies.n

    vm, hbm = pl.BlockSpec(memory_space=pltpu.VMEM), pl.BlockSpec(memory_space=pl.ANY)
    order = lambda t: [t[name] for name in NAMES]
    sems = (COPIES, 21, len(GIVEN) + 4, THREE)
    return pl.pallas_call(
        kernel,
        out_shape=[jax.ShapeDtypeStruct((TWO, *SHAPES[i], LANES), BF16) for i in BATCHES]
        + [jax.ShapeDtypeStruct((TWO, TWO, b.own, LANES), F32) for b in BATCHES.values()],
        in_specs=[hbm] * (len(terms) + len(GIVEN) + THREE * len(NAMES)),
        out_specs=[hbm] * THREE + [vm] * THREE,
        scratch_shapes=[scratch[key] for key in keys] + [pltpu.SemaphoreType.DMA((n,)) for n in sems],
        compiler_params=pltpu.CompilerParams(collective_id=0, has_side_effects=True, vmem_limit_bytes=63 * 2**20),
    )(*terms, *(given[key] for key in GIVEN), *order(weights), *order(m), *order(v))


def lay_out(full, moments):
    names = list(BATCHES)

    def kernel(*refs):
        refs = list(refs)
        take = lambda n: [refs.pop(NONE) for _ in range(n)]
        given, packed = dict(zip(names, take(THREE))), dict(zip(names, take(THREE)))
        outs = dict(zip(NAMES, take(len(NAMES))))
        to = [dict(zip(NAMES, take(len(NAMES)))) for _ in range(TWO)]
        held = dict(zip(names, take(THREE)))
        in_sem, sem = refs

        def go(src, dst):
            pltpu.make_async_copy(src, dst, sem.at[names.index(i)]).start()

        reads = {}
        for n, (i, half) in enumerate((i, half) for half in range(TWO) for i in names):
            reads[i, half] = pltpu.make_async_copy(given[i].at[half], held[i].at[half], in_sem.at[n])
            reads[i, half].start()
        for (i, half), read in reads.items():
            read.wait()
            src = held[i]
            if i == "down":
                for t in range(THREE):
                    for z in range(Z):
                        go(src.at[half, z, :, pl.ds(t * SIXTEEN, SIXTEEN), :],
                           outs["w_down"].at[:, pl.ds(z * SIXTEEN, SIXTEEN), pl.ds((half * THREE + t) * LANES, LANES)])
            for name, tiles in DEEP:
                batch, h, first = SPOT[name]
                if BATCHES[i] is batch and h == half:
                    for t in range(tiles):
                        go(src.at[half, :, pl.ds((first + t) * ROW3, ROW3), :], outs[name].at[:, :, pl.ds(t * LANES, LANES)])
        for k in range(TWO):
            for name, tiles in DEEP:
                batch, half, first = SPOT[name]
                src = packed["deep" if batch is MLP else "att"]
                for r in range(THREE):
                    for t in range(tiles):
                        at = r * batch.wide + first + t
                        to[k][name][r, :, t * LANES : (t + ONE) * LANES] = src[k, half, at : at + ONE, :]
            for t in range(SIX):
                half, n = divmod(t, THREE)
                to[k]["w_down"][:, t * LANES : (t + ONE) * LANES] = packed["down"][k, half, n * EIGHT : (n + ONE) * EIGHT, :]
        for n, i in enumerate(names):
            pltpu.make_async_copy(held[i], held[i], sem.at[n]).wait()

    vm, hbm = pl.BlockSpec(memory_space=pltpu.VMEM), pl.BlockSpec(memory_space=pl.ANY)
    wide = {name: tiles * LANES for name, tiles in DEEP}
    weights = [jax.ShapeDtypeStruct((COLUMNS, ROW3, wide[n]) if n in wide else (COLUMNS, ROW8, D), BF16) for n in NAMES]
    moment = [jax.ShapeDtypeStruct((THREE, ONE, wide[n]) if n in wide else (EIGHT, D), F32) for n in NAMES]
    full = [t.reshape(TWO, COLUMNS, -1, LANES) if i != "down" else t for i, t in zip(names, full)]
    out = pl.pallas_call(
        kernel, out_shape=weights + moment + moment, in_specs=[hbm] * THREE + [vm] * THREE, out_specs=[hbm] * len(NAMES) + [vm] * (TWO * len(NAMES)),
        scratch_shapes=[pltpu.VMEM(t.shape, BF16) for t in full] + [pltpu.SemaphoreType.DMA((n,)) for n in (SIX, THREE)],
        compiler_params=pltpu.CompilerParams(vmem_limit_bytes=63 * 2**20),
    )(*full, *moments)
    new = [t.reshape(ONE, -1, t.shape[-ONE]) for t in out[:7]]
    return new + [t[None] if n == "w_down" else t.transpose(1, 0, 2) for i in (7, 14) for n, t in zip(NAMES, out[i : i + 7])]


def solution(mesh):
    def step(x, dy, *arrays):
        weights, m, v = (dict(zip(NAMES, arrays[i : i + 7], strict=True)) for i in (0, 7, 14))
        weights = {name: w[0] for name, w in weights.items()}
        *terms, q, k, v_, o, a, dh, lse, cos, sin = run_forward(x[0], dy[0], weights)
        given = {"q": q, "k": k, "v": v_, "o": o, "a": a, "dh": dh, "lse": lse, "cos": cos, "sin": sin, "wo": weights["wo"]}
        thin = lambda t: {name: one[0] if name == "w_down" else one.transpose(1, 0, 2) for name, one in t.items()}
        terms = [t.reshape(N, N, MLP.rows, LANES) for t in terms[:2]] + terms[2:]
        out = exchange(terms, given, weights, thin(m), thin(v))
        return tuple(lay_out(out[:3], out[3:]))

    states, all_of, cut = P(("rep", "dp"), None, None), P(None, None, None), P(None, "dp", None)
    return jax.shard_map(
        step,
        mesh=mesh,
        in_specs=(states, states) + (all_of,) * 7 + (cut,) * 14,
        out_specs=(P("rep", None, None),) * 7 + (P("rep", "dp", None),) * 14,
        check_vma=False,
    )
```
